256 devices in a mesh: gx: 16 (over z, core), gy: 8 (over y, x_lo), ma: 2 (over x_hi).
Axes of the slice: x: 4 (x_hi: 2, x_lo: 2; x = x_hi * 2 + x_lo), y: 4, z: 8, core: 2. Of those that a mesh axis runs over, the one named last changes fastest.
Arguments:
- archive: bfloat16 [512, 32, 32, 1024], P('ma', 'gx', None, 'gy')
- obs_index: int32 [65536], P(('gx', 'gy', 'ma')), may hold values from 0 to 4095
- obs_value: float32 [65536], P(('gx', 'gy', 'ma')), may hold values from -6 to 6
- obs_error: float32 [65536], P(('gx', 'gy', 'ma')), may hold values from 0.1 to 1
Outputs:
- increment: float32 [32, 32, 1024], P('gx', 'ma', 'gy')
- weights: float32 [65536], P(('gx', 'gy', 'ma'))
The draws below stay inside these ranges and needn't reach their ends.
Inputs may be any that keep to these rules, and one draw needn't show every extreme that they name: `obs_index`: each entry names a cell of its own block, numbered as in the reference program.
All inputs are finite; a program needn't handle non-finite values.
Results may differ from the reference program's by a relative error of at most 0.0018.
Values may be sent and summed in bfloat16 or wider, within the bound.
A program may use at most 64 MiB of HBM per device.

```python
import math
import jax
import jax.numpy as jnp
from jax import lax

M = 512
RX = 2
RY = 128
NZ = 32
OBS_DEV = 256
TAPER_X = 4
TAPER_Y = 8
ITERS = 2
NX = 32
NY = 1024
NOBS = 65536
N_GY = 8
N_MA = 2


def draw_archive(key, part):
    subkeys = jax.random.split(key, 4)
    background = jax.random.normal(subkeys[0], (1, NX, NZ, NY), jnp.float32) * 0.7
    horizontal = jax.random.normal(subkeys[1], (M, NX, NY), jnp.float32)
    smoothed = horizontal
    for offset in range(1, 6):
        smoothed = smoothed + jnp.roll(horizontal, offset, axis=2)
    smoothed = (smoothed + jnp.roll(smoothed, 1, axis=1)) / math.sqrt(12.0)
    profile = 1.0 + 0.5 * jax.random.normal(subkeys[2], (M, 1, NZ, 1), jnp.float32)
    roughness = 0.6 * jax.random.normal(subkeys[3], (M, NX, NZ, NY), jnp.float32)
    return (background + smoothed[:, :, None, :] * profile + roughness).astype(jnp.bfloat16)


def place_ends(drawn, rng, smallest, top_value):
    longest = drawn.shape.index(max(drawn.shape))
    spots = []
    for shift in (0, 1):
        where = [jax.random.randint(jax.random.fold_in(rng, axis), (), 0, length) for axis, length in enumerate(drawn.shape)]
        where[longest] = (where[longest] + shift) % drawn.shape[longest]
        spots.append(tuple(where))
    return drawn.at[spots[0]].set(smallest).at[spots[1]].set(top_value)


def shard_levels(own_key, extent, shards, smallest, top_value):
    level, own = 1.0, jax.random.fold_in(own_key, 6)
    for axis_at, parts in shards:
        heights = jnp.exp(jax.random.uniform(jax.random.fold_in(own, axis_at), (parts,), jnp.float32, smallest / len(shards), top_value / len(shards)))
        level = level * jnp.repeat(heights, extent[axis_at] // parts).reshape([-1 if axis == axis_at else 1 for axis in range(len(extent))])
    return level


def gaussian(rng, shape, scale, most, shards=(), held_as=jnp.bfloat16):
    level = shard_levels(rng, shape, shards, -0.22, 0.18) if shards else 1.0
    drawn = jax.random.normal(rng, shape, jnp.float32) * scale * level
    return jnp.minimum(jnp.maximum(drawn, -most), most).astype(held_as)


def setup_inputs(seed: int = 0) -> dict:
    keys = jax.random.split(jax.random.key(seed), 5)
    return {
        "archive": draw_archive(jax.random.fold_in(keys[4], 71), 0),
        "obs_index": place_ends(jax.random.randint(keys[1], (NOBS,), 0, RX * (NZ // 2) * RY), jax.random.fold_in(keys[1], 1), 0, (RX * (NZ // 2) * RY) - 1).astype(jnp.int32),
        "obs_value": gaussian(keys[2], (NOBS,), 1.0, 6.0, ((0, 256),), jnp.float32),
        "obs_error": jnp.clip(jnp.exp(math.log(1.0) - 2.3025851 * jax.random.uniform(keys[3], (NOBS,), jnp.float32) ** shard_levels(keys[3], (NOBS,), ((0, 256),), -0.2, 0.2)), 0.1, 1.0),
    }


def taper_weight(distance, half_width):
    ratio = jnp.abs(distance) / half_width
    safe = jnp.maximum(ratio, 1.0)
    inner = (((-0.25 * ratio + 0.5) * ratio + 0.625) * ratio - 5.0 / 3.0) * ratio * ratio + 1.0
    outer = ((((ratio / 12.0 - 0.5) * ratio + 0.625) * ratio + 5.0 / 3.0) * ratio - 5.0) * ratio + 4.0 - 2.0 / (3.0 * safe)
    return jnp.where(ratio <= 1.0, inner, jnp.where(ratio < 2.0, outer, 0.0))

def taper_field(source):
    reach_rows = 2 * TAPER_X
    total = jnp.zeros_like(source)
    for offset in range(-(reach_rows - 1), reach_rows):
        total = total + taper_weight(jnp.float32(offset), float(TAPER_X)) * jnp.roll(source, -offset, axis=1)
    reach = 2 * TAPER_Y
    padded = jnp.pad(total, ((0, 0), (0, 0), (reach, reach)))
    result = jnp.zeros_like(source)
    for offset in range(-reach, reach + 1):
        result = result + taper_weight(jnp.float32(offset), float(TAPER_Y)) * padded[:, :, reach + offset:reach + offset + NY]
    return result

def reference(archive, obs_index, obs_value, obs_error):
    half_levels = NZ // N_MA
    scale = 1.0 / math.sqrt(M - 1.0)

    def row_anomalies(row_index):
        block = lax.dynamic_index_in_dim(archive, row_index, 1, keepdims=False).astype(jnp.float32)
        average = lax.optimization_barrier(jnp.mean(block, axis=0))
        return (((block - average) * scale).astype(jnp.bfloat16), average)
    anomaly_rows, mean_rows = lax.map(row_anomalies, jnp.arange(NX).astype(jnp.int32))
    device = (jnp.arange(NOBS) // OBS_DEV).astype(jnp.int32)
    block_row = device // (N_GY * N_MA)
    block_col = device // N_MA % N_GY
    block_lev = device % N_MA
    global_row = block_row * RX + obs_index // (half_levels * RY)
    global_lev = block_lev * half_levels + obs_index // RY % half_levels
    global_col = block_col * RY + obs_index % RY
    at_obs = anomaly_rows[global_row, :, global_lev, global_col].astype(jnp.float32).T
    mean_obs = mean_rows[global_row, global_lev, global_col]
    column_flat = global_row * NY + global_col

    def spread(vector):
        sources = jnp.zeros((M, NX * NY), jnp.float32).at[:, column_flat].add(at_obs * vector[None, :])
        return taper_field(sources.reshape(M, NX, NY))

    def apply_operator(vector):
        tapered = spread(vector).reshape(M, NX * NY)[:, column_flat]
        return lax.optimization_barrier(jnp.sum(at_obs * tapered, axis=0)) + obs_error * vector
    innovation = obs_value - mean_obs
    weights = jnp.zeros_like(innovation)
    residual = innovation
    direction = innovation
    norm_now = jnp.sum(residual * residual)
    for number in range(ITERS):
        image = apply_operator(direction)
        alpha = norm_now / jnp.sum(direction * image)
        weights = weights + alpha * direction
        residual = residual - alpha * image
        norm_next = jnp.sum(residual * residual)
        direction = residual + norm_next / norm_now * direction
        norm_now = norm_next
    tapered = spread(weights)

    def increment_row(row_index):
        anomalies = lax.dynamic_index_in_dim(anomaly_rows, row_index, 0, keepdims=False).astype(jnp.float32)
        factor = lax.dynamic_index_in_dim(tapered, row_index, 1, keepdims=False)
        return lax.optimization_barrier(jnp.sum(anomalies * factor[:, None, :], axis=0))
    increment = lax.map(increment_row, jnp.arange(NX).astype(jnp.int32))
    return (increment, weights)
```

```python
import functools
import math

import jax
import jax.numpy as jnp
from jax import lax
from jax.experimental import pallas as pl
from jax.experimental.pallas import tpu as pltpu
from jax.sharding import PartitionSpec as P

M = 512
TAPER_X = 4
TAPER_Y = 8
F32 = jnp.float32
BF16 = jnp.bfloat16
MESH = pl.DeviceIdType.MESH

LOADS = 8
CHUNKS = 4
NEAR = (-3, -2, -1, 1, 2, 3)
FAR = 4


def row_weight(distance):
    r = abs(distance) / TAPER_X
    if r <= 1.0:
        return (((-0.25 * r + 0.5) * r + 0.625) * r - 5.0 / 3.0) * r * r + 1.0
    if r < 2.0:
        return (
            ((((r / 12.0 - 0.5) * r + 0.625) * r + 5.0 / 3.0) * r - 5.0) * r
            + 4.0
            - 2.0 / (3.0 * r)
        )
    return 0.0


def taper_weight(distance, half_width):
    ratio = jnp.abs(distance) / half_width
    safe = jnp.maximum(ratio, 1.0)
    inner = (((-0.25 * ratio + 0.5) * ratio + 0.625) * ratio - 5.0 / 3.0) * ratio * ratio + 1.0
    outer = (
        ((((ratio / 12.0 - 0.5) * ratio + 0.625) * ratio + 5.0 / 3.0) * ratio - 5.0) * ratio
        + 4.0
        - 2.0 / (3.0 * safe)
    )
    return jnp.where(ratio <= 1.0, inner, jnp.where(ratio < 2.0, outer, 0.0))


def in_three(x):
    first = x.astype(BF16)
    rest = x - first.astype(F32)
    second = rest.astype(BF16)
    third = (rest - second.astype(F32)).astype(BF16)
    return jnp.concatenate([first, second, third], axis=0)


def sum_of_three(y, rows):
    return (y[2 * rows :] + y[rows : 2 * rows]) + y[:rows]


def kernel(
    n_gx,
    n_gy,
    archive_hbm,
    idx_ref,
    val_ref,
    err_ref,
    inc_ref,
    w_ref,
    arch,
    meta,
    sums,
    part,
    s_ref,
    t_ref,
    near_out,
    near_in,
    far_in,
    f_ref,
    halo_out,
    halo_in,
    wcol,
    pmine,
    ptheirs,
    gsum,
    red1,
    red2,
    load_sem,
    meta_sem,
    sums_sem,
    near_send,
    near_recv,
    far_send,
    far_recv,
    halo_send,
    halo_recv,
    p_sem,
    g_sem,
    red_send,
    red_recv,
):
    members = arch.shape[0]
    levels = arch.shape[2]
    half = levels // 2
    cols = arch.shape[3]
    piece = members // CHUNKS
    gx = lax.axis_index("gx")
    gy = lax.axis_index("gy")
    ma = lax.axis_index("ma")
    other = 1 - ma
    plane = gy * 2 + ma
    n_plane = n_gy * 2

    def row_block(k):
        return {"gx": lax.rem(gx + (k + n_gx), n_gx)}

    def col_block(k):
        return {"gy": lax.rem(gy + (k + n_gy), n_gy)}

    def plane_device(k):
        at = lax.rem(plane + k, n_plane)
        return {"gy": at // 2, "ma": lax.rem(at, 2)}

    load = members // LOADS
    loads = []
    for k in range(LOADS):
        copy = pltpu.make_async_copy(
            archive_hbm.at[pl.ds(k * load, load)], arch.at[pl.ds(k * load, load)], load_sem.at[k]
        )
        copy.start()
        loads.append(copy)

    barrier = pltpu.get_barrier_semaphore()
    for k in range(1, n_gx):
        pl.semaphore_signal(barrier, inc=1, device_id=row_block(k), device_id_type=MESH)
    for k in range(1, n_plane):
        pl.semaphore_signal(barrier, inc=1, device_id=plane_device(k), device_id_type=MESH)

    meta[ma, 0:2, :] = idx_ref[...].astype(F32)
    meta[ma, 2:4, :] = val_ref[...]
    meta[ma, 4:6, :] = err_ref[...]
    meta[ma, 6:8, :] = jnp.zeros((2, cols), F32)

    total = tuple(jnp.zeros((levels, cols), F32) for _ in range(2))
    for k in range(LOADS):
        loads[k].wait()

        def add(m, carry):
            return tuple(carry[x] + arch[m, x].astype(F32) for x in range(2))

        total = lax.fori_loop(k * load, (k + 1) * load, add, total, unroll=8)
    for x in range(2):
        sums[ma, x * levels : (x + 1) * levels, :] = total[x]

    pl.semaphore_wait(barrier, n_gx - 1 + n_plane - 1)

    def to_partner(ref, sem):
        return pltpu.make_async_remote_copy(
            src_ref=ref.at[ma],
            dst_ref=ref.at[ma],
            send_sem=sem.at[0],
            recv_sem=sem.at[1],
            device_id={"ma": other},
            device_id_type=MESH,
        )

    meta_copy = to_partner(meta, meta_sem)
    meta_copy.start()
    sums_copy = to_partner(sums, sums_sem)
    sums_copy.start()

    source = lax.broadcasted_iota(jnp.int32, (cols, cols), 0)
    target = lax.broadcasted_iota(jnp.int32, (cols, cols), 1)
    for k in range(3):
        weight = taper_weight((source - target + (k - 1) * cols).astype(F32), float(TAPER_Y))
        if k == 0:
            weight = jnp.where(gy > 0, weight, 0.0)
        if k == 2:
            weight = jnp.where(gy < n_gy - 1, weight, 0.0)
        high = weight.astype(BF16)
        low = (weight - high.astype(F32)).astype(BF16)
        wcol[k * 2 * cols : (k * 2 + 1) * cols, :] = high
        wcol[(k * 2 + 1) * cols : (k * 2 + 2) * cols, :] = low

    meta_copy.wait()

    def in_a_row(first):
        rows = [meta[h, first + i : first + i + 1, :] for h in range(2) for i in range(2)]
        return jnp.concatenate(rows, axis=1)

    index = in_a_row(0).astype(jnp.int32)
    target_value = in_a_row(2)
    noise = in_a_row(4)
    n_obs = index.shape[1]
    owner = lax.broadcasted_iota(jnp.int32, (1, n_obs), 1) // (n_obs // 2)
    obs_line = (index >> 11) * levels + owner * half + ((index >> 7) & (half - 1))
    obs_col = index & (cols - 1)
    line_hot = (
        lax.broadcasted_iota(jnp.int32, (2 * levels, n_obs), 0) == obs_line
    ).astype(F32)
    col_hot = (
        (lax.broadcasted_iota(jnp.int32, (cols, n_obs), 0) == obs_col).astype(F32).astype(BF16)
    )

    def gather(grid):
        rows = 2 * levels
        spread = jnp.dot(in_three(grid), col_hot, preferred_element_type=F32)
        return jnp.sum(sum_of_three(spread, rows) * line_hot, axis=0, keepdims=True)

    def scatter(vector):
        rows = 2 * levels
        spread = lax.dot_general(
            in_three(line_hot * vector),
            col_hot,
            (((1,), (1,)), ((), ())),
            preferred_element_type=F32,
        )
        return sum_of_three(spread, rows)

    sums_copy.wait()
    average = (sums[0] + sums[1]) * (1.0 / M)
    innovation = target_value - gather(average)
    scale = 1.0 / math.sqrt(M - 1.0)

    def send_sources(phase, q):
        copies = []
        for n, k in enumerate(NEAR):
            copies.append(
                pltpu.make_async_remote_copy(
                    src_ref=near_out.at[phase, q],
                    dst_ref=near_in.at[phase, q, len(NEAR) - 1 - n],
                    send_sem=near_send.at[phase, q, n],
                    recv_sem=near_recv.at[phase, q, len(NEAR) - 1 - n],
                    device_id=row_block(k),
                    device_id_type=MESH,
                )
            )
        for side in range(2):
            copies.append(
                pltpu.make_async_remote_copy(
                    src_ref=near_out.at[phase, q, 1 - side],
                    dst_ref=far_in.at[phase, q, side],
                    send_sem=far_send.at[phase, q, side],
                    recv_sem=far_recv.at[phase, q, side],
                    device_id=row_block(FAR if side == 0 else -FAR),
                    device_id_type=MESH,
                )
            )
        for copy in copies:
            copy.start()
        return copies

    def form_sources(phase, q, grid):
        value = [grid[x * levels : (x + 1) * levels] for x in range(2)]
        mean = [average[x * levels : (x + 1) * levels] for x in range(2)]

        def one(i, carry):
            m = q * piece + i
            for x in range(2):
                if phase == 0:
                    anomaly = ((arch[m, x].astype(F32) - mean[x]) * scale).astype(BF16)
                    arch[m, x] = anomaly
                else:
                    anomaly = arch[m, x]
                product = anomaly.astype(F32) * value[x]
                part[x, pl.ds(pl.multiple_of(i * 8, 8), 8), :] = (
                    product[0:8] + product[8:16]
                ) + (product[16:24] + product[24:32])
            return carry

        lax.fori_loop(0, piece, one, 0, unroll=4)
        for x in range(2):
            for g in range(piece // 8):
                rows = [part[x, pl.ds(g * 64 + k, 8, stride=8), :] for k in range(8)]
                s_ref[phase, x, q * piece + g * 8 : q * piece + g * 8 + 8, :] = (
                    (rows[0] + rows[1]) + (rows[2] + rows[3])
                ) + ((rows[4] + rows[5]) + (rows[6] + rows[7]))
            near_out[phase, q, x] = s_ref[phase, x, q * piece : (q + 1) * piece, :].astype(BF16)

    def filter_rows(phase, q, copies):
        for copy in copies:
            copy.wait_recv()
        for i in range(2):
            out = None
            for r in range(2):
                terms = [(row_weight(r - i), s_ref[phase, r, q * piece : (q + 1) * piece, :])]
                for n, k in enumerate(NEAR):
                    terms.append((row_weight(2 * k + r - i), near_in[phase, q, n, r].astype(F32)))
                for weight, row in terms:
                    if weight:
                        out = row * weight if out is None else out + row * weight
            if i == 0:
                out = out + far_in[phase, q, 0].astype(F32) * row_weight(-2 * FAR + 1)
            else:
                out = out + far_in[phase, q, 1].astype(F32) * row_weight(2 * FAR - 1)
            f_ref[phase, q, i] = out
            halo_out[phase, q, i] = out.astype(BF16)
        sends = []
        for side in range(2):
            copy = pltpu.make_async_remote_copy(
                src_ref=halo_out.at[phase, q],
                dst_ref=halo_in.at[phase, q, side],
                send_sem=halo_send.at[phase, q, side],
                recv_sem=halo_recv.at[phase, q, side],
                device_id=col_block(1 if side == 0 else -1),
                device_id_type=MESH,
            )
            copy.start()
            sends.append(copy)
        return sends

    def filter_cols(phase, q, copies):
        for copy in copies:
            copy.wait_recv()
        rows = 2 * piece
        field = f_ref[phase, q].reshape(rows, cols)
        high = field.astype(BF16)
        low = (field - high.astype(F32)).astype(BF16)
        left = halo_in[phase, q, 0].reshape(rows, cols)
        right = halo_in[phase, q, 1].reshape(rows, cols)
        result = jnp.dot(
            jnp.concatenate([left, left, high, high, right, right], axis=1),
            wcol[...],
            preferred_element_type=F32,
        ) + jnp.dot(low, wcol[2 * cols : 3 * cols, :], preferred_element_type=F32)
        for x in range(2):
            t_ref[phase, x, q * piece : (q + 1) * piece, :] = result[
                x * piece : (x + 1) * piece
            ]

    def member_sum(phase, q, carry):
        def one(i, carry):
            m = q * piece + i
            return tuple(
                carry[x] + arch[m, x].astype(F32) * t_ref[phase, x, pl.ds(m, 1), :]
                for x in range(2)
            )

        return lax.fori_loop(0, piece, one, carry, unroll=4)

    def spread(phase, grid, before_last):
        sent = []
        for q in range(CHUNKS):
            form_sources(phase, q, grid)
            sent.append(send_sources(phase, q))
        halos = []
        carry = tuple(jnp.zeros((levels, cols), F32) for _ in range(2))
        for q in range(CHUNKS):
            halos.append(filter_rows(phase, q, sent[q]))
            if q == 0:
                before_last()
            else:
                filter_cols(phase, q - 1, halos[q - 1])
                carry = member_sum(phase, q - 1, carry)
        filter_cols(phase, CHUNKS - 1, halos[CHUNKS - 1])
        carry = member_sum(phase, CHUNKS - 1, carry)
        for x in range(2):
            for h in range(2):
                pmine[phase, h, x] = carry[x][h * half : (h + 1) * half]
        copy = pltpu.make_async_remote_copy(
            src_ref=pmine.at[phase, other],
            dst_ref=ptheirs.at[phase],
            send_sem=p_sem.at[phase, 0],
            recv_sem=p_sem.at[phase, 1],
            device_id={"ma": other},
            device_id_type=MESH,
        )
        copy.start()
        pending = [c for group in sent + halos for c in group]
        return jnp.concatenate(carry, axis=0), pending, copy

    def per_column(x):
        return jnp.sum(x, axis=0, keepdims=True)

    def folded(vector):
        width = cols
        return sum(vector[:, k * width : (k + 1) * width] for k in range(n_obs // width)) * 0.5

    def reduce_first(which, rows):
        red1[which, gx, 0:1, :] = rows[0]
        red1[which, gx, 1:2, :] = rows[1]
        copies = []
        for k in range(1, n_gx):
            copy = pltpu.make_async_remote_copy(
                src_ref=red1.at[which, gx],
                dst_ref=red1.at[which, gx],
                send_sem=red_send.at[which, 0, k],
                recv_sem=red_recv.at[which, 0, k],
                device_id=row_block(k),
                device_id_type=MESH,
            )
            copy.start()
            copies.append(copy)
        return copies

    def reduce_second(which, waits):
        for copy in waits:
            copy.wait_recv()
        red2[which, plane] = jnp.sum(red1[which], axis=0)
        copies = []
        for k in range(1, n_plane):
            copy = pltpu.make_async_remote_copy(
                src_ref=red2.at[which, plane],
                dst_ref=red2.at[which, plane],
                send_sem=red_send.at[which, 1, k],
                recv_sem=red_recv.at[which, 1, k],
                device_id=plane_device(k),
                device_id_type=MESH,
            )
            copy.start()
            copies.append(copy)
        return copies

    def reduce_last(which, waits):
        for copy in waits:
            copy.wait_recv()
        both = jnp.sum(jnp.sum(red2[which], axis=0), axis=1, keepdims=True)
        return both[0:1], both[1:2]

    grid_b, pending_b, p_copy_b = spread(0, scatter(innovation), lambda: None)
    gsum[ma] = gather(grid_b)
    g_copy = pltpu.make_async_remote_copy(
        src_ref=gsum.at[ma],
        dst_ref=gsum.at[ma],
        send_sem=g_sem.at[0],
        recv_sem=g_sem.at[1],
        device_id={"ma": other},
        device_id_type=MESH,
    )
    g_copy.start()
    first = reduce_first(
        0,
        (
            folded(innovation * innovation),
            per_column(
                sum(s_ref[0, x] * t_ref[0, x] for x in range(2))
            ) + folded(noise * innovation * innovation),
        ),
    )
    g_copy.wait()
    image = gsum[0] + gsum[1] + noise * innovation

    state = {}

    def meanwhile():
        state["second"] = reduce_second(0, first)

    grid_g, pending_g, p_copy_g = spread(1, scatter(image), meanwhile)
    norm_now, product = reduce_last(0, state["second"])
    alpha = norm_now / product
    residual = innovation - alpha * image
    along = per_column(
        sum(
            (s_ref[0, x] - alpha * s_ref[1, x]) * (t_ref[0, x] - alpha * t_ref[1, x])
            for x in range(2)
        )
    )
    last_first = reduce_first(
        1, (folded(residual * residual), along + folded(noise * residual * residual))
    )
    last_second = reduce_second(1, last_first)
    norm_next, product = reduce_last(1, last_second)
    ratio = norm_next / norm_now
    alpha_next = norm_next / (product - ratio * norm_next / alpha)
    weights = alpha * innovation + alpha_next * (residual + ratio * innovation)
    chosen = jnp.where(ma == 0, weights[:, : n_obs // 2], weights[:, n_obs // 2 :])
    w_ref[0:1, :] = chosen[:, :cols]
    w_ref[1:2, :] = chosen[:, cols:]

    p_copy_b.wait()
    p_copy_g.wait()
    first_weight = (alpha + alpha_next * (1.0 + ratio))[None]
    second_weight = (alpha * alpha_next)[None]
    inc_ref[...] = first_weight * (pmine[0, ma] + ptheirs[0]) - second_weight * (
        pmine[1, ma] + ptheirs[1]
    )

    for copy in pending_b + pending_g + first + state["second"] + last_first + last_second:
        copy.wait_send()


def shards(n_gx, n_gy, archive, obs_index, obs_value, obs_error):
    members, rows, levels, cols = archive.shape
    half = levels // 2
    n_own = obs_index.shape[0]
    piece = members // CHUNKS
    shape = (n_own // cols, cols)
    dma = pltpu.SemaphoreType.DMA
    vmem = pl.BlockSpec(memory_space=pltpu.VMEM)
    increment, weights = pl.pallas_call(
        functools.partial(kernel, n_gx, n_gy),
        out_shape=(
            jax.ShapeDtypeStruct((rows, half, cols), F32),
            jax.ShapeDtypeStruct(shape, F32),
        ),
        in_specs=[pl.BlockSpec(memory_space=pl.ANY), vmem, vmem, vmem],
        out_specs=(vmem, vmem),
        scratch_shapes=[
            pltpu.VMEM((members, rows, levels, cols), BF16),
            pltpu.VMEM((2, 8, cols), F32),
            pltpu.VMEM((2, rows * levels, cols), F32),
            pltpu.VMEM((rows, piece * 8, cols), F32),
            pltpu.VMEM((2, rows, members, cols), F32),
            pltpu.VMEM((2, rows, members, cols), F32),
            pltpu.VMEM((2, CHUNKS, rows, piece, cols), BF16),
            pltpu.VMEM((2, CHUNKS, len(NEAR), rows, piece, cols), BF16),
            pltpu.VMEM((2, CHUNKS, 2, piece, cols), BF16),
            pltpu.VMEM((2, CHUNKS, rows, piece, cols), F32),
            pltpu.VMEM((2, CHUNKS, rows, piece, cols), BF16),
            pltpu.VMEM((2, CHUNKS, 2, rows, piece, cols), BF16),
            pltpu.VMEM((6 * cols, cols), BF16),
            pltpu.VMEM((2, 2, rows, half, cols), F32),
            pltpu.VMEM((2, rows, half, cols), F32),
            pltpu.VMEM((2, 1, 2 * n_own), F32),
            pltpu.VMEM((2, n_gx, 2, cols), F32),
            pltpu.VMEM((2, 2 * n_gy, 2, cols), F32),
            dma((LOADS,)),
            dma((2,)),
            dma((2,)),
            dma((2, CHUNKS, len(NEAR))),
            dma((2, CHUNKS, len(NEAR))),
            dma((2, CHUNKS, 2)),
            dma((2, CHUNKS, 2)),
            dma((2, CHUNKS, 2)),
            dma((2, CHUNKS, 2)),
            dma((2, 2)),
            dma((2,)),
            dma((2, 2, max(n_gx, 2 * n_gy))),
            dma((2, 2, max(n_gx, 2 * n_gy))),
        ],
        compiler_params=pltpu.CompilerParams(
            collective_id=0, has_side_effects=True, vmem_limit_bytes=40 * 1024 * 1024
        ),
        name="analysis",
    )(archive, obs_index.reshape(shape), obs_value.reshape(shape), obs_error.reshape(shape))
    return increment, weights.reshape(n_own)


def solution(mesh):
    n_gx, n_gy = mesh.shape["gx"], mesh.shape["gy"]
    own = P(("gx", "gy", "ma"))
    return jax.shard_map(
        functools.partial(shards, n_gx, n_gy),
        mesh=mesh,
        in_specs=(P("ma", "gx", None, "gy"), own, own, own),
        out_specs=(P("gx", "ma", "gy"), own),
        check_vma=False,
    )
```

```python
import functools
import math

import jax
import jax.numpy as jnp
from jax import lax
from jax.experimental import pallas as pl
from jax.experimental.pallas import tpu as pltpu
from jax.sharding import PartitionSpec as P

M = 512
TAPER_X = 4
TAPER_Y = 8
F32 = jnp.float32
BF16 = jnp.bfloat16
MESH = pl.DeviceIdType.MESH

LOADS = 8
CHUNKS = 4
STRIP = 16
BOTH, BEFORE, AFTER, BESIDE, ONE = range(5)


def row_weight(distance):
    r = abs(distance) / TAPER_X
    if r <= 1.0:
        return (((-0.25 * r + 0.5) * r + 0.625) * r - 5.0 / 3.0) * r * r + 1.0
    if r < 2.0:
        return (
            ((((r / 12.0 - 0.5) * r + 0.625) * r + 5.0 / 3.0) * r - 5.0) * r
            + 4.0
            - 2.0 / (3.0 * r)
        )
    return 0.0


def taper_weight(distance, half_width):
    ratio = jnp.abs(distance) / half_width
    safe = jnp.maximum(ratio, 1.0)
    inner = (((-0.25 * ratio + 0.5) * ratio + 0.625) * ratio - 5.0 / 3.0) * ratio * ratio + 1.0
    outer = (
        ((((ratio / 12.0 - 0.5) * ratio + 0.625) * ratio + 5.0 / 3.0) * ratio - 5.0) * ratio
        + 4.0
        - 2.0 / (3.0 * safe)
    )
    return jnp.where(ratio <= 1.0, inner, jnp.where(ratio < 2.0, outer, 0.0))


def in_three(x):
    first = x.astype(BF16)
    rest = x - first.astype(F32)
    second = rest.astype(BF16)
    third = (rest - second.astype(F32)).astype(BF16)
    return jnp.concatenate([first, second, third], axis=0)


def sum_of_three(y, rows):
    return (y[2 * rows :] + y[rows : 2 * rows]) + y[:rows]


def kernel(
    n_gx,
    n_gy,
    archive_hbm,
    idx_hbm,
    val_hbm,
    err_hbm,
    inc_ref,
    w_ref,
    arch,
    idx_ref,
    val_ref,
    err_ref,
    meta,
    sums,
    part,
    s_ref,
    f_ref,
    h_ref,
    t_ref,
    out_ref,
    block_in,
    row_in,
    fwd_in,
    strip_out,
    strip_in,
    wcol,
    pmine,
    ptheirs,
    gsum,
    red1,
    red2,
    load_sem,
    meta_sem,
    sums_sem,
    block_send,
    block_recv,
    fwd_send,
    fwd_recv,
    strip_send,
    strip_recv,
    p_sem,
    g_sem,
    red_send,
    red_recv,
):
    members = arch.shape[0]
    levels = arch.shape[2]
    half = levels // 2
    cols = arch.shape[3]
    piece = members // CHUNKS
    gx = lax.axis_index("gx")
    gy = lax.axis_index("gy")
    ma = lax.axis_index("ma")
    core = lax.rem(gx, 2)
    other = 1 - ma
    plane = gy * 2 + ma
    n_plane = n_gy * 2

    def row_block(k):
        return {"gx": lax.rem(gx + (k + n_gx), n_gx)}

    def col_block(k):
        return {"gy": lax.rem(gy + (k + n_gy), n_gy)}

    def plane_device(k):
        at = lax.rem(plane + k, n_plane)
        return {"gy": at // 2, "ma": lax.rem(at, 2)}

    def remote(src, dst, send_sem, recv_sem, device):
        copy = pltpu.make_async_remote_copy(
            src_ref=src,
            dst_ref=dst,
            send_sem=send_sem,
            recv_sem=recv_sem,
            device_id=device,
            device_id_type=MESH,
        )
        copy.start()
        return copy

    barrier = pltpu.get_barrier_semaphore()
    for k in range(1, n_gx):
        pl.semaphore_signal(barrier, inc=1, device_id=row_block(k), device_id_type=MESH)
    for k in range(1, n_plane):
        pl.semaphore_signal(barrier, inc=1, device_id=plane_device(k), device_id_type=MESH)

    load = members // LOADS
    loads = []
    for k in range(LOADS):
        copy = pltpu.make_async_copy(
            archive_hbm.at[pl.ds(k * load, load)], arch.at[pl.ds(k * load, load)], load_sem.at[k]
        )
        copy.start()
        loads.append(copy)
    small = []
    for k, (src, dst) in enumerate(
        ((idx_hbm, idx_ref), (val_hbm, val_ref), (err_hbm, err_ref))
    ):
        copy = pltpu.make_async_copy(src, dst, load_sem.at[LOADS + k])
        copy.start()
        small.append(copy)

    source = lax.broadcasted_iota(jnp.int32, (cols, cols), 0)
    target = lax.broadcasted_iota(jnp.int32, (cols, cols), 1)

    def col_weight(shift):
        return taper_weight((source - target + shift).astype(F32), float(TAPER_Y))

    beside = jnp.where(gy > 0, col_weight(-cols), 0.0) + jnp.where(
        gy < n_gy - 1, col_weight(cols), 0.0
    )
    for k, weight in enumerate((col_weight(0), beside)):
        high = weight.astype(BF16)
        low = (weight - high.astype(F32)).astype(BF16)
        wcol[2 * k * cols : (2 * k + 1) * cols, :] = high
        wcol[(2 * k + 1) * cols : (2 * k + 2) * cols, :] = low
        if k == 0:
            wcol[4 * cols : 5 * cols, :] = high

    total = tuple(jnp.zeros((levels, cols), F32) for _ in range(2))
    for k in range(LOADS):
        loads[k].wait()

        def add(m, carry):
            return tuple(carry[x] + arch[m, x].astype(F32) for x in range(2))

        total = lax.fori_loop(k * load, (k + 1) * load, add, total, unroll=8)
    for x in range(2):
        sums[ma, x * levels : (x + 1) * levels, :] = total[x]
    for copy in small:
        copy.wait()
    meta[ma, 0:2, :] = idx_ref[...].astype(F32)
    meta[ma, 2:4, :] = val_ref[...]
    meta[ma, 4:6, :] = err_ref[...]
    meta[ma, 6:8, :] = jnp.zeros((2, cols), F32)

    pl.semaphore_wait(barrier, n_gx - 1 + n_plane - 1)

    partner = {"ma": other}
    meta_copy = remote(meta.at[ma], meta.at[ma], meta_sem.at[0], meta_sem.at[1], partner)
    sums_copy = remote(sums.at[ma], sums.at[ma], sums_sem.at[0], sums_sem.at[1], partner)

    meta_copy.wait()

    def in_a_row(first):
        rows = [meta[h, first + i : first + i + 1, :] for h in range(2) for i in range(2)]
        return jnp.concatenate(rows, axis=1)

    index = in_a_row(0).astype(jnp.int32)
    target_value = in_a_row(2)
    noise = in_a_row(4)
    n_obs = index.shape[1]
    owner = lax.broadcasted_iota(jnp.int32, (1, n_obs), 1) // (n_obs // 2)
    obs_line = (index >> 11) * levels + owner * half + ((index >> 7) & (half - 1))
    obs_col = index & (cols - 1)
    line_hot = (
        lax.broadcasted_iota(jnp.int32, (2 * levels, n_obs), 0) == obs_line
    ).astype(F32)
    col_hot = (
        (lax.broadcasted_iota(jnp.int32, (cols, n_obs), 0) == obs_col).astype(F32).astype(BF16)
    )

    def gather(grid):
        rows = 2 * levels
        spread = jnp.dot(in_three(grid), col_hot, preferred_element_type=F32)
        return jnp.sum(sum_of_three(spread, rows) * line_hot, axis=0, keepdims=True)

    def scatter(vector):
        rows = 2 * levels
        spread = lax.dot_general(
            in_three(line_hot * vector),
            col_hot,
            (((1,), (1,)), ((), ())),
            preferred_element_type=F32,
        )
        return sum_of_three(spread, rows)

    sums_copy.wait()
    average = (sums[0] + sums[1]) * (1.0 / M)
    innovation = target_value - gather(average)
    scale = 1.0 / math.sqrt(M - 1.0)

    def send_sources(phase, q):
        away = 8 * core - 4
        whole = out_ref.at[phase, q]

        def to(src, slot, dst, device):
            return remote(
                src, dst, block_send.at[phase, q, slot], block_recv.at[phase, q, slot], device
            )

        return {
            BOTH: to(whole, BOTH, block_in.at[phase, q, BOTH], row_block(away)),
            ONE: to(
                out_ref.at[phase, q, 1 - core], ONE, row_in.at[phase, q], row_block(-away)
            ),
            BEFORE: to(whole, BEFORE, block_in.at[phase, q, BEFORE], row_block(2)),
            AFTER: to(whole, AFTER, block_in.at[phase, q, AFTER], row_block(-2)),
            BESIDE: to(whole, BESIDE, block_in.at[phase, q, BESIDE], row_block(1 - 2 * core)),
        }

    def pass_on(phase, q, copies):
        passed = []
        for slot in (BEFORE, AFTER, BOTH):
            copies[slot].wait_recv()
            passed.append(
                remote(
                    block_in.at[phase, q, slot],
                    fwd_in.at[phase, q, slot],
                    fwd_send.at[phase, q, slot],
                    fwd_recv.at[phase, q, slot],
                    row_block(1 - 2 * core),
                )
            )
        return passed

    strip_rows = 2 * piece * STRIP // cols
    lane = lax.broadcasted_iota(jnp.int32, (strip_rows, cols), 1)

    def send_strips(phase, kind, q, field):
        last = first = jnp.zeros((strip_rows, cols), F32)
        for j in range(cols // STRIP):
            group = field[j * strip_rows : (j + 1) * strip_rows]
            mine = lane // STRIP == j
            last = jnp.where(mine, pltpu.roll(group, ((j + 1) * STRIP) % cols, 1), last)
            first = jnp.where(mine, pltpu.roll(group, j * STRIP, 1), first)
        copies = []
        for side, strip in enumerate((last, first)):
            strip_out[phase, kind, q, side] = strip.astype(BF16)
            copies.append(
                remote(
                    strip_out.at[phase, kind, q, side],
                    strip_in.at[phase, kind, q, side],
                    strip_send.at[phase, kind, q, side],
                    strip_recv.at[phase, kind, q, side],
                    col_block(1 - 2 * side),
                )
            )
        return copies

    def filter_cols(phase, kind, q, field, copies):
        for copy in copies:
            copy.wait_recv()
        left = strip_in[phase, kind, q, 0].astype(F32)
        right = strip_in[phase, kind, q, 1].astype(F32)
        strips = []
        for j in range(cols // STRIP):
            strips.append(
                jnp.where(
                    lane < cols // 2,
                    pltpu.roll(right, (cols - j * STRIP) % cols, 1),
                    pltpu.roll(left, cols - (j + 1) * STRIP, 1),
                )
            )
        strips = jnp.concatenate(strips, axis=0).astype(BF16)
        high = field.astype(BF16)
        low = (field - high.astype(F32)).astype(BF16)
        return jnp.dot(
            jnp.concatenate([high, high, strips, strips, low], axis=1),
            wcol[...],
            preferred_element_type=F32,
        )

    def form_sources(phase, q, grid):
        value = [grid[x * levels : (x + 1) * levels] for x in range(2)]
        mean = [average[x * levels : (x + 1) * levels] for x in range(2)]

        def one(i, carry):
            m = q * piece + i
            for x in range(2):
                if phase == 0:
                    anomaly = ((arch[m, x].astype(F32) - mean[x]) * scale).astype(BF16)
                    arch[m, x] = anomaly
                else:
                    anomaly = arch[m, x]
                product = anomaly.astype(F32) * value[x]
                part[x, pl.ds(pl.multiple_of(i * 8, 8), 8), :] = (
                    product[0:8] + product[8:16]
                ) + (product[16:24] + product[24:32])
            return carry

        lax.fori_loop(0, piece, one, 0, unroll=4)
        for x in range(2):
            for g in range(piece // 8):
                rows = [part[x, pl.ds(g * 64 + k, 8, stride=8), :] for k in range(8)]
                s_ref[phase, q, x * piece + g * 8 : x * piece + g * 8 + 8, :] = (
                    (rows[0] + rows[1]) + (rows[2] + rows[3])
                ) + ((rows[4] + rows[5]) + (rows[6] + rows[7]))
            out_ref[phase, q, x] = s_ref[phase, q, x * piece : (x + 1) * piece, :].astype(BF16)

    def filter_rows(phase, q, copies, passed):
        copies[BESIDE].wait_recv()
        copies[ONE].wait_recv()
        for copy in passed:
            copy.wait_recv()

        def weight(k, r, i):
            both = [row_weight(2 * at + r - i) for at in k]
            return both[0] if both[0] == both[1] else jnp.where(core == 0, both[0], both[1])

        blocks = [
            ((0, 0), lambda r: s_ref[phase, q, r * piece : (r + 1) * piece, :]),
            ((-2, -2), lambda r: block_in[phase, q, BEFORE, r].astype(F32)),
            ((2, 2), lambda r: block_in[phase, q, AFTER, r].astype(F32)),
            ((1, -1), lambda r: block_in[phase, q, BESIDE, r].astype(F32)),
            ((-1, -3), lambda r: fwd_in[phase, q, BEFORE, r].astype(F32)),
            ((3, 1), lambda r: fwd_in[phase, q, AFTER, r].astype(F32)),
            ((-3, 3), lambda r: fwd_in[phase, q, BOTH, r].astype(F32)),
        ]
        farthest = row_weight(7)
        far = [
            block_in[phase, q, BOTH, core].astype(F32) * farthest,
            row_in[phase, q].astype(F32) * farthest,
        ]
        outs = [jnp.where(core == 1, far[0], far[1]), jnp.where(core == 1, far[1], far[0])]
        for k, block in blocks:
            for r in range(2):
                row = block(r)
                for i in range(2):
                    outs[i] = outs[i] + row * weight(k, r, i)
        for i in range(2):
            f_ref[phase, q, i * piece : (i + 1) * piece, :] = outs[i]
        return send_strips(phase, 1, q, jnp.concatenate(outs, axis=0))

    def member_sum(phase, q, carry):
        def one(i, carry):
            m = q * piece + i
            return tuple(
                carry[x]
                + arch[m, x].astype(F32) * t_ref[q, pl.ds(x * piece + i, 1), :]
                for x in range(2)
            )

        return lax.fori_loop(0, piece, one, carry, unroll=4)

    def spread(phase, grid, meanwhile, rows_done):
        pending = []
        sent, own_strips, passed, strips = [], [], [], []
        for q in range(CHUNKS):
            form_sources(phase, q, grid)
            sent.append(send_sources(phase, q))
            own_strips.append(send_strips(phase, 0, q, s_ref[phase, q]))
        meanwhile()
        carry = tuple(jnp.zeros((levels, cols), F32) for _ in range(2))

        def finish(q, carry):
            t_ref[q] = filter_cols(phase, 1, q, f_ref[phase, q], strips[q])
            return member_sum(phase, q, carry)

        for q in range(CHUNKS + 1):
            if q < CHUNKS:
                h_ref[phase, q] = filter_cols(phase, 0, q, s_ref[phase, q], own_strips[q])
                passed.append(pass_on(phase, q, sent[q]))
            if q >= 1:
                strips.append(filter_rows(phase, q - 1, sent[q - 1], passed[q - 1]))
            if q >= 3 and q < CHUNKS:
                carry = finish(q - 3, carry)
        rows_done()
        for q in range(max(CHUNKS - 3, 0), CHUNKS):
            carry = finish(q, carry)
        for x in range(2):
            for h in range(2):
                pmine[phase, h, x] = carry[x][h * half : (h + 1) * half]
        pending = [c for group in sent for c in group.values()]
        pending += [c for group in own_strips + passed + strips for c in group]
        return jnp.concatenate(carry, axis=0), pending

    def send_increment(phase):
        return remote(
            pmine.at[phase, other], ptheirs.at[phase], p_sem.at[phase, 0], p_sem.at[phase, 1], partner
        )

    def per_column(x):
        return jnp.sum(x, axis=0, keepdims=True)

    def folded(vector):
        return (
            sum(vector[:, k * cols : (k + 1) * cols] for k in range(n_obs // cols)) * 0.5
        )

    def reduce_first(which, rows):
        red1[which, gx, 0:1, :] = rows[0]
        red1[which, gx, 1:2, :] = rows[1]
        mine = red1.at[which, gx]
        return [
            remote(mine, mine, red_send.at[which, 0, k], red_recv.at[which, 0, k], row_block(k))
            for k in range(1, n_gx)
        ]

    def reduce_second(which, waits):
        for copy in waits:
            copy.wait_recv()
        red2[which, plane] = jnp.sum(red1[which], axis=0)
        mine = red2.at[which, plane]
        return [
            remote(mine, mine, red_send.at[which, 1, k], red_recv.at[which, 1, k], plane_device(k))
            for k in range(1, n_plane)
        ]

    def reduce_last(which, waits):
        for copy in waits:
            copy.wait_recv()
        both = jnp.sum(jnp.sum(red2[which], axis=0), axis=1, keepdims=True)
        return both[0:1], both[1:2]

    state = {}

    def nothing():
        pass

    grid_b, pending_b = spread(0, scatter(innovation), nothing, nothing)
    gsum[ma] = gather(grid_b)
    g_copy = remote(gsum.at[ma], gsum.at[ma], g_sem.at[0], g_sem.at[1], partner)
    p_copy_b = send_increment(0)
    along = per_column(sum(f_ref[0, q] * h_ref[0, q] for q in range(CHUNKS)))
    first = reduce_first(
        0,
        (
            folded(innovation * innovation),
            along + folded(noise * innovation * innovation),
        ),
    )
    g_copy.wait()
    image = gsum[0] + gsum[1] + noise * innovation

    def meanwhile():
        state["second"] = reduce_second(0, first)

    def rows_done():
        norm_now, product = reduce_last(0, state["second"])
        alpha = norm_now / product
        residual = innovation - alpha * image
        along = per_column(
            sum(
                (f_ref[0, q] - alpha * f_ref[1, q]) * (h_ref[0, q] - alpha * h_ref[1, q])
                for q in range(CHUNKS)
            )
        )
        state["last_first"] = reduce_first(
            1, (folded(residual * residual), along + folded(noise * residual * residual))
        )
        state["step"] = norm_now, alpha, residual

    grid_g, pending_g = spread(1, scatter(image), meanwhile, rows_done)
    p_copy_g = send_increment(1)
    norm_now, alpha, residual = state["step"]
    last_second = reduce_second(1, state["last_first"])
    norm_next, product = reduce_last(1, last_second)
    ratio = norm_next / norm_now
    alpha_next = norm_next / (product - ratio * norm_next / alpha)
    weights = alpha * innovation + alpha_next * (residual + ratio * innovation)
    chosen = jnp.where(ma == 0, weights[:, : n_obs // 2], weights[:, n_obs // 2 :])
    w_ref[0:1, :] = chosen[:, :cols]
    w_ref[1:2, :] = chosen[:, cols:]

    p_copy_b.wait()
    p_copy_g.wait()
    first_weight = (alpha + alpha_next * (1.0 + ratio))[None]
    second_weight = (alpha * alpha_next)[None]
    inc_ref[...] = first_weight * (pmine[0, ma] + ptheirs[0]) - second_weight * (
        pmine[1, ma] + ptheirs[1]
    )

    for copy in (
        pending_b
        + pending_g
        + first
        + state["second"]
        + state["last_first"]
        + last_second
    ):
        copy.wait_send()


def shards(n_gx, n_gy, archive, obs_index, obs_value, obs_error):
    members, rows, levels, cols = archive.shape
    half = levels // 2
    n_own = obs_index.shape[0]
    piece = members // CHUNKS
    strip_rows = rows * piece * STRIP // cols
    shape = (n_own // cols, cols)
    dma = pltpu.SemaphoreType.DMA
    vmem = pl.BlockSpec(memory_space=pltpu.VMEM)
    hbm = pl.BlockSpec(memory_space=pl.ANY)
    increment, weights = pl.pallas_call(
        functools.partial(kernel, n_gx, n_gy),
        out_shape=(
            jax.ShapeDtypeStruct((rows, half, cols), F32),
            jax.ShapeDtypeStruct(shape, F32),
        ),
        in_specs=[hbm, hbm, hbm, hbm],
        out_specs=(vmem, vmem),
        scratch_shapes=[
            pltpu.VMEM((members, rows, levels, cols), BF16),
            pltpu.VMEM(shape, jnp.int32),
            pltpu.VMEM(shape, F32),
            pltpu.VMEM(shape, F32),
            pltpu.VMEM((2, 8, cols), F32),
            pltpu.VMEM((2, rows * levels, cols), F32),
            pltpu.VMEM((rows, piece * 8, cols), F32),
            pltpu.VMEM((2, CHUNKS, rows * piece, cols), F32),
            pltpu.VMEM((2, CHUNKS, rows * piece, cols), F32),
            pltpu.VMEM((2, CHUNKS, rows * piece, cols), F32),
            pltpu.VMEM((CHUNKS, rows * piece, cols), F32),
            pltpu.VMEM((2, CHUNKS, rows, piece, cols), BF16),
            pltpu.VMEM((2, CHUNKS, 4, rows, piece, cols), BF16),
            pltpu.VMEM((2, CHUNKS, piece, cols), BF16),
            pltpu.VMEM((2, CHUNKS, 3, rows, piece, cols), BF16),
            pltpu.VMEM((2, 2, CHUNKS, 2, strip_rows, cols), BF16),
            pltpu.VMEM((2, 2, CHUNKS, 2, strip_rows, cols), BF16),
            pltpu.VMEM((5 * cols, cols), BF16),
            pltpu.VMEM((2, 2, rows, half, cols), F32),
            pltpu.VMEM((2, rows, half, cols), F32),
            pltpu.VMEM((2, 1, 2 * n_own), F32),
            pltpu.VMEM((2, n_gx, 2, cols), F32),
            pltpu.VMEM((2, 2 * n_gy, 2, cols), F32),
            dma((LOADS + 3,)),
            dma((2,)),
            dma((2,)),
            dma((2, CHUNKS, 5)),
            dma((2, CHUNKS, 5)),
            dma((2, CHUNKS, 3)),
            dma((2, CHUNKS, 3)),
            dma((2, 2, CHUNKS, 2)),
            dma((2, 2, CHUNKS, 2)),
            dma((2, 2)),
            dma((2,)),
            dma((2, 2, max(n_gx, 2 * n_gy))),
            dma((2, 2, max(n_gx, 2 * n_gy))),
        ],
        compiler_params=pltpu.CompilerParams(
            collective_id=0, has_side_effects=True, vmem_limit_bytes=60 * 1024 * 1024
        ),
        name="analysis",
    )(archive, obs_index.reshape(shape), obs_value.reshape(shape), obs_error.reshape(shape))
    return increment, weights.reshape(n_own)


def solution(mesh):
    n_gx, n_gy = mesh.shape["gx"], mesh.shape["gy"]
    own = P(("gx", "gy", "ma"))
    return jax.shard_map(
        functools.partial(shards, n_gx, n_gy),
        mesh=mesh,
        in_specs=(P("ma", "gx", None, "gy"), own, own, own),
        out_specs=(P("gx", "ma", "gy"), own),
        check_vma=False,
    )
```

```python
import functools
import math

import jax
import jax.numpy as jnp
from jax import lax
from jax.experimental import pallas as pl
from jax.experimental.pallas import tpu as pltpu
from jax.sharding import PartitionSpec as P

M = 512
TAPER_X = 4
TAPER_Y = 8
F32 = jnp.float32
BF16 = jnp.bfloat16
MESH = pl.DeviceIdType.MESH

LOADS = 8
ROWS_FIRST = (0, 1)
COLS_FIRST = (2, 3)
CHUNKS = 4
STRIP = 16
BOTH, BEFORE, AFTER, BESIDE, ONE = range(5)


def row_weight(distance):
    r = abs(distance) / TAPER_X
    if r <= 1.0:
        return (((-0.25 * r + 0.5) * r + 0.625) * r - 5.0 / 3.0) * r * r + 1.0
    if r < 2.0:
        return (
            ((((r / 12.0 - 0.5) * r + 0.625) * r + 5.0 / 3.0) * r - 5.0) * r
            + 4.0
            - 2.0 / (3.0 * r)
        )
    return 0.0


def taper_weight(distance, half_width):
    ratio = jnp.abs(distance) / half_width
    safe = jnp.maximum(ratio, 1.0)
    inner = (((-0.25 * ratio + 0.5) * ratio + 0.625) * ratio - 5.0 / 3.0) * ratio * ratio + 1.0
    outer = (
        ((((ratio / 12.0 - 0.5) * ratio + 0.625) * ratio + 5.0 / 3.0) * ratio - 5.0) * ratio
        + 4.0
        - 2.0 / (3.0 * safe)
    )
    return jnp.where(ratio <= 1.0, inner, jnp.where(ratio < 2.0, outer, 0.0))


def in_three(x):
    first = x.astype(BF16)
    rest = x - first.astype(F32)
    second = rest.astype(BF16)
    third = (rest - second.astype(F32)).astype(BF16)
    return jnp.concatenate([first, second, third], axis=0)


def sum_of_three(y, rows):
    return (y[2 * rows :] + y[rows : 2 * rows]) + y[:rows]


def kernel(
    n_gx,
    n_gy,
    archive_hbm,
    idx_hbm,
    val_hbm,
    err_hbm,
    inc_ref,
    w_ref,
    arch,
    idx_ref,
    val_ref,
    err_ref,
    meta,
    sums,
    part,
    s_ref,
    f_ref,
    h_ref,
    t_ref,
    out_ref,
    block_in,
    row_in,
    fwd_in,
    strip_out,
    strip_in,
    wcol,
    pmine,
    ptheirs,
    gsum,
    red1,
    red2,
    load_sem,
    meta_sem,
    sums_sem,
    block_send,
    block_recv,
    fwd_send,
    fwd_recv,
    strip_send,
    strip_recv,
    p_sem,
    g_sem,
    red_send,
    red_recv,
):
    members = arch.shape[0]
    levels = arch.shape[2]
    half = levels // 2
    cols = arch.shape[3]
    piece = members // CHUNKS
    gx = lax.axis_index("gx")
    gy = lax.axis_index("gy")
    ma = lax.axis_index("ma")
    core = lax.rem(gx, 2)
    other = 1 - ma
    plane = gy * 2 + ma
    n_plane = n_gy * 2

    def row_block(k):
        return {"gx": lax.rem(gx + (k + n_gx), n_gx)}

    def col_block(k):
        return {"gy": lax.rem(gy + (k + n_gy), n_gy)}

    def plane_device(k):
        at = lax.rem(plane + k, n_plane)
        return {"gy": at // 2, "ma": lax.rem(at, 2)}

    def remote(src, dst, send_sem, recv_sem, device):
        copy = pltpu.make_async_remote_copy(
            src_ref=src,
            dst_ref=dst,
            send_sem=send_sem,
            recv_sem=recv_sem,
            device_id=device,
            device_id_type=MESH,
        )
        copy.start()
        return copy

    barrier = pltpu.get_barrier_semaphore()
    for k in range(1, n_gx):
        pl.semaphore_signal(barrier, inc=1, device_id=row_block(k), device_id_type=MESH)
    for k in range(1, n_plane):
        pl.semaphore_signal(barrier, inc=1, device_id=plane_device(k), device_id_type=MESH)

    load = members // LOADS
    loads = []
    for k in range(LOADS):
        copy = pltpu.make_async_copy(
            archive_hbm.at[pl.ds(k * load, load)], arch.at[pl.ds(k * load, load)], load_sem.at[k]
        )
        copy.start()
        loads.append(copy)
    small = []
    for k, (src, dst) in enumerate(
        ((idx_hbm, idx_ref), (val_hbm, val_ref), (err_hbm, err_ref))
    ):
        copy = pltpu.make_async_copy(src, dst, load_sem.at[LOADS + k])
        copy.start()
        small.append(copy)

    source = lax.broadcasted_iota(jnp.int32, (cols, cols), 0)
    target = lax.broadcasted_iota(jnp.int32, (cols, cols), 1)

    def col_weight(shift):
        return taper_weight((source - target + shift).astype(F32), float(TAPER_Y))

    beside = jnp.where(gy > 0, col_weight(-cols), 0.0) + jnp.where(
        gy < n_gy - 1, col_weight(cols), 0.0
    )
    for k, weight in enumerate((col_weight(0), beside)):
        high = weight.astype(BF16)
        low = (weight - high.astype(F32)).astype(BF16)
        wcol[2 * k * cols : (2 * k + 1) * cols, :] = high
        wcol[(2 * k + 1) * cols : (2 * k + 2) * cols, :] = low
        if k == 0:
            wcol[4 * cols : 5 * cols, :] = high

    total = tuple(jnp.zeros((levels, cols), F32) for _ in range(2))
    for k in range(LOADS):
        loads[k].wait()

        def add(m, carry):
            return tuple(carry[x] + arch[m, x].astype(F32) for x in range(2))

        total = lax.fori_loop(k * load, (k + 1) * load, add, total, unroll=8)
    for x in range(2):
        sums[ma, x * levels : (x + 1) * levels, :] = total[x]
    for copy in small:
        copy.wait()
    meta[ma, 0:2, :] = idx_ref[...].astype(F32)
    meta[ma, 2:4, :] = val_ref[...]
    meta[ma, 4:6, :] = err_ref[...]
    meta[ma, 6:8, :] = jnp.zeros((2, cols), F32)

    pl.semaphore_wait(barrier, n_gx - 1 + n_plane - 1)

    partner = {"ma": other}
    meta_copy = remote(meta.at[ma], meta.at[ma], meta_sem.at[0], meta_sem.at[1], partner)
    sums_copy = remote(sums.at[ma], sums.at[ma], sums_sem.at[0], sums_sem.at[1], partner)

    meta_copy.wait()

    def in_a_row(first):
        rows = [meta[h, first + i : first + i + 1, :] for h in range(2) for i in range(2)]
        return jnp.concatenate(rows, axis=1)

    index = in_a_row(0).astype(jnp.int32)
    target_value = in_a_row(2)
    noise = in_a_row(4)
    n_obs = index.shape[1]
    owner = lax.broadcasted_iota(jnp.int32, (1, n_obs), 1) // (n_obs // 2)
    obs_line = (index >> 11) * levels + owner * half + ((index >> 7) & (half - 1))
    obs_col = index & (cols - 1)
    line_hot = (
        lax.broadcasted_iota(jnp.int32, (2 * levels, n_obs), 0) == obs_line
    ).astype(F32)
    col_hot = (
        (lax.broadcasted_iota(jnp.int32, (cols, n_obs), 0) == obs_col).astype(F32).astype(BF16)
    )

    def gather(grid):
        rows = 2 * levels
        spread = jnp.dot(in_three(grid), col_hot, preferred_element_type=F32)
        return jnp.sum(sum_of_three(spread, rows) * line_hot, axis=0, keepdims=True)

    def scatter(vector):
        rows = 2 * levels
        spread = lax.dot_general(
            in_three(line_hot * vector),
            col_hot,
            (((1,), (1,)), ((), ())),
            preferred_element_type=F32,
        )
        return sum_of_three(spread, rows)

    sums_copy.wait()
    average = (sums[0] + sums[1]) * (1.0 / M)
    innovation = target_value - gather(average)
    scale = 1.0 / math.sqrt(M - 1.0)

    def send_sources(phase, q, field):
        for x in range(2):
            out_ref[phase, q, x] = field[x * piece : (x + 1) * piece].astype(BF16)
        away = 8 * core - 4
        whole = out_ref.at[phase, q]

        def to(src, slot, dst, device):
            return remote(
                src, dst, block_send.at[phase, q, slot], block_recv.at[phase, q, slot], device
            )

        return {
            BOTH: to(whole, BOTH, block_in.at[phase, q, BOTH], row_block(away)),
            ONE: to(
                out_ref.at[phase, q, 1 - core], ONE, row_in.at[phase, q], row_block(-away)
            ),
            BEFORE: to(whole, BEFORE, block_in.at[phase, q, BEFORE], row_block(2)),
            AFTER: to(whole, AFTER, block_in.at[phase, q, AFTER], row_block(-2)),
            BESIDE: to(whole, BESIDE, block_in.at[phase, q, BESIDE], row_block(1 - 2 * core)),
        }

    def pass_on(phase, q, copies):
        passed = []
        for slot in (BEFORE, AFTER, BOTH):
            copies[slot].wait_recv()
            passed.append(
                remote(
                    block_in.at[phase, q, slot],
                    fwd_in.at[phase, q, slot],
                    fwd_send.at[phase, q, slot],
                    fwd_recv.at[phase, q, slot],
                    row_block(1 - 2 * core),
                )
            )
        return passed

    strip_rows = 2 * piece * STRIP // cols
    lane = lax.broadcasted_iota(jnp.int32, (strip_rows, cols), 1)

    def send_strips(phase, kind, q, field):
        last = first = jnp.zeros((strip_rows, cols), F32)
        for j in range(cols // STRIP):
            group = field[j * strip_rows : (j + 1) * strip_rows]
            mine = lane // STRIP == j
            last = jnp.where(mine, pltpu.roll(group, ((j + 1) * STRIP) % cols, 1), last)
            first = jnp.where(mine, pltpu.roll(group, j * STRIP, 1), first)
        copies = []
        for side, strip in enumerate((last, first)):
            strip_out[phase, kind, q, side] = strip.astype(BF16)
            copies.append(
                remote(
                    strip_out.at[phase, kind, q, side],
                    strip_in.at[phase, kind, q, side],
                    strip_send.at[phase, kind, q, side],
                    strip_recv.at[phase, kind, q, side],
                    col_block(1 - 2 * side),
                )
            )
        return copies

    def filter_cols(phase, kind, q, field, copies):
        for copy in copies:
            copy.wait_recv()
        left = strip_in[phase, kind, q, 0].astype(F32)
        right = strip_in[phase, kind, q, 1].astype(F32)
        strips = []
        for j in range(cols // STRIP):
            strips.append(
                jnp.where(
                    lane < cols // 2,
                    pltpu.roll(right, (cols - j * STRIP) % cols, 1),
                    pltpu.roll(left, cols - (j + 1) * STRIP, 1),
                )
            )
        strips = jnp.concatenate(strips, axis=0).astype(BF16)
        high = field.astype(BF16)
        low = (field - high.astype(F32)).astype(BF16)
        return jnp.dot(
            jnp.concatenate([high, high, strips, strips, low], axis=1),
            wcol[...],
            preferred_element_type=F32,
        )

    def form_sources(phase, q, grid):
        value = [grid[x * levels : (x + 1) * levels] for x in range(2)]
        mean = [average[x * levels : (x + 1) * levels] for x in range(2)]

        def one(i, carry):
            m = q * piece + i
            for x in range(2):
                if phase == 0:
                    anomaly = ((arch[m, x].astype(F32) - mean[x]) * scale).astype(BF16)
                    arch[m, x] = anomaly
                else:
                    anomaly = arch[m, x]
                product = anomaly.astype(F32) * value[x]
                part[x, pl.ds(pl.multiple_of(i * 8, 8), 8), :] = (
                    product[0:8] + product[8:16]
                ) + (product[16:24] + product[24:32])
            return carry

        lax.fori_loop(0, piece, one, 0, unroll=4)
        for x in range(2):
            for g in range(piece // 8):
                rows = [part[x, pl.ds(g * 64 + k, 8, stride=8), :] for k in range(8)]
                s_ref[phase, q, x * piece + g * 8 : x * piece + g * 8 + 8, :] = (
                    (rows[0] + rows[1]) + (rows[2] + rows[3])
                ) + ((rows[4] + rows[5]) + (rows[6] + rows[7]))

    def filter_rows(phase, q, own, copies, passed):
        copies[BESIDE].wait_recv()
        copies[ONE].wait_recv()
        for copy in passed:
            copy.wait_recv()

        def weight(k, r, i):
            both = [row_weight(2 * at + r - i) for at in k]
            return both[0] if both[0] == both[1] else jnp.where(core == 0, both[0], both[1])

        blocks = [
            ((0, 0), lambda r: own[phase, q, r * piece : (r + 1) * piece, :]),
            ((-2, -2), lambda r: block_in[phase, q, BEFORE, r].astype(F32)),
            ((2, 2), lambda r: block_in[phase, q, AFTER, r].astype(F32)),
            ((1, -1), lambda r: block_in[phase, q, BESIDE, r].astype(F32)),
            ((-1, -3), lambda r: fwd_in[phase, q, BEFORE, r].astype(F32)),
            ((3, 1), lambda r: fwd_in[phase, q, AFTER, r].astype(F32)),
            ((-3, 3), lambda r: fwd_in[phase, q, BOTH, r].astype(F32)),
        ]
        farthest = row_weight(7)
        far = [
            block_in[phase, q, BOTH, core].astype(F32) * farthest,
            row_in[phase, q].astype(F32) * farthest,
        ]
        outs = [jnp.where(core == 1, far[0], far[1]), jnp.where(core == 1, far[1], far[0])]
        for k, block in blocks:
            for r in range(2):
                row = block(r)
                for i in range(2):
                    outs[i] = outs[i] + row * weight(k, r, i)
        return jnp.concatenate(outs, axis=0)

    def member_sum(phase, q, carry):
        def one(i, carry):
            m = q * piece + i
            return tuple(
                carry[x]
                + arch[m, x].astype(F32) * t_ref[phase, q, pl.ds(x * piece + i, 1), :]
                for x in range(2)
            )

        return lax.fori_loop(0, piece, one, carry, unroll=4)

    def spread(phase, grid, meanwhile, rows_done):
        sent, own_strips, passed, strips = {}, {}, {}, {}
        for pair in zip(ROWS_FIRST, COLS_FIRST):
            for q in pair:
                form_sources(phase, q, grid)
                if q in ROWS_FIRST:
                    sent[q] = send_sources(phase, q, s_ref[phase, q])
                own_strips[q] = send_strips(phase, 0, q, s_ref[phase, q])
        meanwhile()
        for q in COLS_FIRST:
            h_ref[phase, q] = filter_cols(phase, 0, q, s_ref[phase, q], own_strips[q])
            sent[q] = send_sources(phase, q, h_ref[phase, q])
        for q in ROWS_FIRST:
            h_ref[phase, q] = filter_cols(phase, 0, q, s_ref[phase, q], own_strips[q])

        def rows_of(q):
            if q in ROWS_FIRST:
                f_ref[phase, q] = filter_rows(phase, q, s_ref, sent[q], passed[q])
                strips[q] = send_strips(phase, 1, q, f_ref[phase, q])
            else:
                t_ref[phase, q] = filter_rows(phase, q, h_ref, sent[q], passed[q])

        def finish(q, carry):
            if q in ROWS_FIRST:
                t_ref[phase, q] = filter_cols(phase, 1, q, f_ref[phase, q], strips[q])
            return member_sum(phase, q, carry)

        carry = tuple(jnp.zeros((levels, cols), F32) for _ in range(2))
        for q in range(CHUNKS):
            passed[q] = pass_on(phase, q, sent[q])
            if q >= 1:
                rows_of(q - 1)
        carry = finish(0, carry)
        carry = finish(2, carry)
        rows_of(CHUNKS - 1)
        rows_done()
        carry = finish(1, carry)
        carry = finish(3, carry)
        for x in range(2):
            for h in range(2):
                pmine[phase, h, x] = carry[x][h * half : (h + 1) * half]
        pending = [c for group in sent.values() for c in group.values()]
        for groups in (own_strips, passed, strips):
            pending += [c for group in groups.values() for c in group]
        return jnp.concatenate(carry, axis=0), pending

    def dotted(left, right):
        terms = [left(f_ref, q) * right(h_ref, q) for q in ROWS_FIRST]
        terms += [left(s_ref, q) * right(t_ref, q) for q in COLS_FIRST]
        return jnp.sum(sum(terms), axis=0, keepdims=True)

    def send_increment(phase):
        return remote(
            pmine.at[phase, other], ptheirs.at[phase], p_sem.at[phase, 0], p_sem.at[phase, 1], partner
        )

    def folded(vector):
        return (
            sum(vector[:, k * cols : (k + 1) * cols] for k in range(n_obs // cols)) * 0.5
        )

    def reduce_first(which, rows):
        red1[which, gx, 0:1, :] = rows[0]
        red1[which, gx, 1:2, :] = rows[1]
        mine = red1.at[which, gx]
        return [
            remote(mine, mine, red_send.at[which, 0, k], red_recv.at[which, 0, k], row_block(k))
            for k in range(1, n_gx)
        ]

    def reduce_second(which, waits):
        for copy in waits:
            copy.wait_recv()
        red2[which, plane] = jnp.sum(red1[which], axis=0)
        mine = red2.at[which, plane]
        return [
            remote(mine, mine, red_send.at[which, 1, k], red_recv.at[which, 1, k], plane_device(k))
            for k in range(1, n_plane)
        ]

    def reduce_last(which, waits):
        for copy in waits:
            copy.wait_recv()
        both = jnp.sum(jnp.sum(red2[which], axis=0), axis=1, keepdims=True)
        return both[0:1], both[1:2]

    state = {}

    def nothing():
        pass

    grid_b, pending_b = spread(0, scatter(innovation), nothing, nothing)
    gsum[ma] = gather(grid_b)
    g_copy = remote(gsum.at[ma], gsum.at[ma], g_sem.at[0], g_sem.at[1], partner)
    p_copy_b = send_increment(0)
    along = dotted(lambda ref, q: ref[0, q], lambda ref, q: ref[0, q])
    first = reduce_first(
        0,
        (
            folded(innovation * innovation),
            along + folded(noise * innovation * innovation),
        ),
    )
    g_copy.wait()
    image = gsum[0] + gsum[1] + noise * innovation

    def meanwhile():
        state["second"] = reduce_second(0, first)

    def rows_done():
        norm_now, product = reduce_last(0, state["second"])
        alpha = norm_now / product
        residual = innovation - alpha * image

        def of_residual(ref, q):
            return ref[0, q] - alpha * ref[1, q]

        along = dotted(of_residual, of_residual)
        state["last_first"] = reduce_first(
            1, (folded(residual * residual), along + folded(noise * residual * residual))
        )
        state["step"] = norm_now, alpha, residual

    grid_g, pending_g = spread(1, scatter(image), meanwhile, rows_done)
    p_copy_g = send_increment(1)
    norm_now, alpha, residual = state["step"]
    last_second = reduce_second(1, state["last_first"])
    for copy in pending_b + pending_g + first + state["second"] + state["last_first"]:
        copy.wait_send()
    p_copy_b.wait()
    norm_next, product = reduce_last(1, last_second)
    ratio = norm_next / norm_now
    alpha_next = norm_next / (product - ratio * norm_next / alpha)
    weights = alpha * innovation + alpha_next * (residual + ratio * innovation)
    chosen = jnp.where(ma == 0, weights[:, : n_obs // 2], weights[:, n_obs // 2 :])
    w_ref[0:1, :] = chosen[:, :cols]
    w_ref[1:2, :] = chosen[:, cols:]

    p_copy_g.wait()
    first_weight = (alpha + alpha_next * (1.0 + ratio))[None]
    second_weight = (alpha * alpha_next)[None]
    inc_ref[...] = first_weight * (pmine[0, ma] + ptheirs[0]) - second_weight * (
        pmine[1, ma] + ptheirs[1]
    )

    for copy in last_second:
        copy.wait_send()


def shards(n_gx, n_gy, archive, obs_index, obs_value, obs_error):
    members, rows, levels, cols = archive.shape
    half = levels // 2
    n_own = obs_index.shape[0]
    piece = members // CHUNKS
    strip_rows = rows * piece * STRIP // cols
    shape = (n_own // cols, cols)
    dma = pltpu.SemaphoreType.DMA
    vmem = pl.BlockSpec(memory_space=pltpu.VMEM)
    hbm = pl.BlockSpec(memory_space=pltpu.HBM)
    increment, weights = pl.pallas_call(
        functools.partial(kernel, n_gx, n_gy),
        out_shape=(
            pltpu.VMEM((rows, half, cols), F32),
            pltpu.VMEM(shape, F32),
        ),
        in_specs=[hbm, hbm, hbm, hbm],
        out_specs=(vmem, vmem),
        scratch_shapes=[
            pltpu.VMEM((members, rows, levels, cols), BF16),
            pltpu.VMEM(shape, jnp.int32),
            pltpu.VMEM(shape, F32),
            pltpu.VMEM(shape, F32),
            pltpu.VMEM((2, 8, cols), F32),
            pltpu.VMEM((2, rows * levels, cols), F32),
            pltpu.VMEM((rows, piece * 8, cols), F32),
            pltpu.VMEM((2, CHUNKS, rows * piece, cols), F32),
            pltpu.VMEM((2, CHUNKS, rows * piece, cols), F32),
            pltpu.VMEM((2, CHUNKS, rows * piece, cols), F32),
            pltpu.VMEM((2, CHUNKS, rows * piece, cols), F32),
            pltpu.VMEM((2, CHUNKS, rows, piece, cols), BF16),
            pltpu.VMEM((2, CHUNKS, 4, rows, piece, cols), BF16),
            pltpu.VMEM((2, CHUNKS, piece, cols), BF16),
            pltpu.VMEM((2, CHUNKS, 3, rows, piece, cols), BF16),
            pltpu.VMEM((2, 2, CHUNKS, 2, strip_rows, cols), BF16),
            pltpu.VMEM((2, 2, CHUNKS, 2, strip_rows, cols), BF16),
            pltpu.VMEM((5 * cols, cols), BF16),
            pltpu.VMEM((2, 2, rows, half, cols), F32),
            pltpu.VMEM((2, rows, half, cols), F32),
            pltpu.VMEM((2, 1, 2 * n_own), F32),
            pltpu.VMEM((2, n_gx, 2, cols), F32),
            pltpu.VMEM((2, 2 * n_gy, 2, cols), F32),
            dma((LOADS + 3,)),
            dma((2,)),
            dma((2,)),
            dma((2, CHUNKS, 5)),
            dma((2, CHUNKS, 5)),
            dma((2, CHUNKS, 3)),
            dma((2, CHUNKS, 3)),
            dma((2, 2, CHUNKS, 2)),
            dma((2, 2, CHUNKS, 2)),
            dma((2, 2)),
            dma((2,)),
            dma((2, 2, max(n_gx, 2 * n_gy))),
            dma((2, 2, max(n_gx, 2 * n_gy))),
        ],
        compiler_params=pltpu.CompilerParams(
            collective_id=0, has_side_effects=True, vmem_limit_bytes=56 * 1024 * 1024
        ),
        name="analysis",
    )(archive, obs_index.reshape(shape), obs_value.reshape(shape), obs_error.reshape(shape))
    return increment, weights.reshape(n_own)


def solution(mesh):
    n_gx, n_gy = mesh.shape["gx"], mesh.shape["gy"]
    own = P(("gx", "gy", "ma"))
    return jax.shard_map(
        functools.partial(shards, n_gx, n_gy),
        mesh=mesh,
        in_specs=(P("ma", "gx", None, "gy"), own, own, own),
        out_specs=(P("gx", "ma", "gy"), own),
        check_vma=False,
    )
```

```python
import functools
import math

import jax
import jax.numpy as jnp
from jax import lax
from jax.experimental import pallas as pl
from jax.experimental.pallas import tpu as pltpu
from jax.sharding import PartitionSpec as P

M = 512
TAPER_X = 4
TAPER_Y = 8
F32 = jnp.float32
BF16 = jnp.bfloat16
MESH = pl.DeviceIdType.MESH

LOADS = 8
CHUNKS = 4
ORDER = (0, 2, 1, 3)
STRIP = 16
SOURCE, FILTERED = 0, 1


def course(kind, q):
    return (1 if q < CHUNKS // 2 else -1) * (1 if kind == SOURCE else -1)


def row_weight(distance):
    r = abs(distance) / TAPER_X
    if r <= 1.0:
        return (((-0.25 * r + 0.5) * r + 0.625) * r - 5.0 / 3.0) * r * r + 1.0
    if r < 2.0:
        return (
            ((((r / 12.0 - 0.5) * r + 0.625) * r + 5.0 / 3.0) * r - 5.0) * r
            + 4.0
            - 2.0 / (3.0 * r)
        )
    return 0.0


def taper_weight(distance, half_width):
    ratio = jnp.abs(distance) / half_width
    safe = jnp.maximum(ratio, 1.0)
    inner = (((-0.25 * ratio + 0.5) * ratio + 0.625) * ratio - 5.0 / 3.0) * ratio * ratio + 1.0
    outer = (
        ((((ratio / 12.0 - 0.5) * ratio + 0.625) * ratio + 5.0 / 3.0) * ratio - 5.0) * ratio
        + 4.0
        - 2.0 / (3.0 * safe)
    )
    return jnp.where(ratio <= 1.0, inner, jnp.where(ratio < 2.0, outer, 0.0))


def in_three(x):
    first = x.astype(BF16)
    rest = x - first.astype(F32)
    second = rest.astype(BF16)
    third = (rest - second.astype(F32)).astype(BF16)
    return jnp.concatenate([first, second, third], axis=0)


def sum_of_three(y, rows):
    return (y[2 * rows :] + y[rows : 2 * rows]) + y[:rows]


def kernel(
    n_gx,
    n_gy,
    archive_hbm,
    idx_hbm,
    val_hbm,
    err_hbm,
    inc_ref,
    w_ref,
    arch,
    idx_ref,
    pair_ref,
    meta,
    sums,
    part,
    s_ref,
    f_ref,
    h_ref,
    t_ref,
    out_ref,
    side_in,
    beside_in,
    sent_ref,
    strip_out,
    strip_in,
    wcol,
    pmine,
    ptheirs,
    gsum,
    red1,
    red2,
    load_sem,
    meta_sem,
    sums_sem,
    block_send,
    block_recv,
    fwd_recv,
    beside_recv,
    strip_send,
    strip_recv,
    p_sem,
    g_sem,
    red_send,
    red_recv,
):
    members = arch.shape[0]
    levels = arch.shape[2]
    half = levels // 2
    cols = arch.shape[3]
    piece = members // CHUNKS
    gx = lax.axis_index("gx")
    gy = lax.axis_index("gy")
    ma = lax.axis_index("ma")
    core = lax.rem(gx, 2)
    other = 1 - ma
    sent_rows = sent_ref.at[0 : 15 * CHUNKS]
    plane = gy * 2 + ma
    n_plane = n_gy * 2

    def row_block(k):
        return {"gx": lax.rem(gx + (k + n_gx), n_gx)}

    def col_block(k):
        return {"gy": lax.rem(gy + (k + n_gy), n_gy)}

    def plane_device(k):
        at = lax.rem(plane + k, n_plane)
        return {"gy": at // 2, "ma": lax.rem(at, 2)}

    def remote(src, dst, send_sem, recv_sem, device):
        copy = pltpu.make_async_remote_copy(
            src_ref=src,
            dst_ref=dst,
            send_sem=send_sem,
            recv_sem=recv_sem,
            device_id=device,
            device_id_type=MESH,
        )
        copy.start()
        return copy

    def wait_for(ref, sem):
        pltpu.make_async_copy(ref, ref, sem).wait()

    load = members // LOADS
    loads = []
    for k in range(LOADS):
        copy = pltpu.make_async_copy(
            archive_hbm.at[pl.ds(k * load, load)], arch.at[pl.ds(k * load, load)], load_sem.at[k]
        )
        copy.start()
        loads.append(copy)
    pltpu.make_async_copy(idx_hbm, idx_ref, load_sem.at[LOADS]).start()
    pltpu.make_async_copy(val_hbm, pair_ref.at[0], load_sem.at[LOADS + 1]).start()
    pltpu.make_async_copy(err_hbm, pair_ref.at[1], load_sem.at[LOADS + 1]).start()

    barrier = pltpu.get_barrier_semaphore()
    for k in range(1, n_gx):
        pl.semaphore_signal(barrier, inc=1, device_id=row_block(k), device_id_type=MESH)
    for k in range(1, n_plane):
        pl.semaphore_signal(barrier, inc=1, device_id=plane_device(k), device_id_type=MESH)

    source = lax.broadcasted_iota(jnp.int32, (cols, cols), 0)
    target = lax.broadcasted_iota(jnp.int32, (cols, cols), 1)

    def col_weight(shift):
        return taper_weight((source - target + shift).astype(F32), float(TAPER_Y))

    beside = jnp.where(gy > 0, col_weight(-cols), 0.0) + jnp.where(
        gy < n_gy - 1, col_weight(cols), 0.0
    )
    for k, weight in enumerate((col_weight(0), beside)):
        high = weight.astype(BF16)
        low = (weight - high.astype(F32)).astype(BF16)
        wcol[2 * k * cols : (2 * k + 1) * cols, :] = high
        wcol[(2 * k + 1) * cols : (2 * k + 2) * cols, :] = low
        if k == 0:
            wcol[4 * cols : 5 * cols, :] = high

    total = tuple(jnp.zeros((levels, cols), F32) for _ in range(2))
    for k in range(LOADS):
        loads[k].wait()

        def add(m, carry):
            return tuple(carry[x] + arch[m, x].astype(F32) for x in range(2))

        total = lax.fori_loop(k * load, (k + 1) * load, add, total, unroll=8)
    for x in range(2):
        sums[ma, x * levels : (x + 1) * levels, :] = total[x]
    wait_for(idx_ref, load_sem.at[LOADS])
    wait_for(pair_ref, load_sem.at[LOADS + 1])
    meta[ma, 0:2, :] = idx_ref[...].astype(F32)
    meta[ma, 2:4, :] = pair_ref[0]
    meta[ma, 4:6, :] = pair_ref[1]
    meta[ma, 6:8, :] = jnp.zeros((2, cols), F32)

    pl.semaphore_wait(barrier, n_gx - 1 + n_plane - 1)

    partner = {"ma": other}
    meta_copy = remote(meta.at[ma], meta.at[ma], meta_sem.at[0], meta_sem.at[1], partner)
    sums_copy = remote(sums.at[ma], sums.at[ma], sums_sem.at[0], sums_sem.at[1], partner)

    meta_copy.wait()

    def in_a_row(first):
        rows = [meta[h, first + i : first + i + 1, :] for h in range(2) for i in range(2)]
        return jnp.concatenate(rows, axis=1)

    index = in_a_row(0).astype(jnp.int32)
    target_value = in_a_row(2)
    noise = in_a_row(4)
    n_obs = index.shape[1]
    owner = lax.broadcasted_iota(jnp.int32, (1, n_obs), 1) // (n_obs // 2)
    obs_line = (index >> 11) * levels + owner * half + ((index >> 7) & (half - 1))
    obs_col = index & (cols - 1)
    line_hot = (
        lax.broadcasted_iota(jnp.int32, (2 * levels, n_obs), 0) == obs_line
    ).astype(F32)
    col_hot = (
        (lax.broadcasted_iota(jnp.int32, (cols, n_obs), 0) == obs_col).astype(F32).astype(BF16)
    )

    def gather(grid):
        rows = 2 * levels
        spread = jnp.dot(in_three(grid), col_hot, preferred_element_type=F32)
        return jnp.sum(sum_of_three(spread, rows) * line_hot, axis=0, keepdims=True)

    def scatter(vector):
        rows = 2 * levels
        spread = lax.dot_general(
            in_three(line_hot * vector),
            col_hot,
            (((1,), (1,)), ((), ())),
            preferred_element_type=F32,
        )
        return sum_of_three(spread, rows)

    sums_copy.wait()
    average = (sums[0] + sums[1]) * (1.0 / M)
    innovation = target_value - gather(average)
    scale = 1.0 / math.sqrt(M - 1.0)

    beside_me = row_block(1 - 2 * core)

    def big(way):
        return core == (1 if way > 0 else 0)

    def send_block(phase, kind, q, field):
        way = course(kind, q)
        row = 1 if way > 0 else 0
        for x in range(2):
            out_ref[phase, kind, q, x] = field[x * piece : (x + 1) * piece].astype(BF16)
        block = out_ref.at[phase, kind, q]
        here = side_in.at[phase, kind, q]
        sems = block_send.at[phase], block_recv.at[phase, kind, q]

        @pl.when(big(way))
        def _():
            remote(block, here.at[2:4], *sems, row_block(4 * way))

        @pl.when(jnp.logical_not(big(way)))
        def _():
            remote(block.at[row], here.at[2], *sems, row_block(4 * way))

        remote(block, here.at[0:2], *sems, row_block(2 * way))

    def either(way, size_if_big, size_if_not, sem):
        @pl.when(big(way))
        def _():
            wait_for(size_if_big, sem)

        @pl.when(jnp.logical_not(big(way)))
        def _():
            wait_for(size_if_not, sem)

    def pass_on(phase, kind, q):
        way = course(kind, q)
        here = side_in.at[phase, kind, q]
        sem = block_recv.at[phase, kind, q]
        either(way, here.at[0:4], here.at[0:3], sem)
        sems = block_send.at[phase], fwd_recv.at[phase, kind, q]

        @pl.when(big(way))
        def _():
            remote(here.at[0:4], here.at[4:8], *sems, beside_me)

        @pl.when(jnp.logical_not(big(way)))
        def _():
            remote(here.at[0:2], here.at[4:6], *sems, beside_me)

    def weight(k, r, i):
        both = [row_weight(2 * at + r - i) for at in k]
        return both[0] if both[0] == both[1] else jnp.where(core == 0, both[0], both[1])

    def weighed(terms):
        outs = [None, None]
        for k, rows in terms:
            for r in range(2):
                for i in range(2):
                    if any(row_weight(2 * at + r - i) for at in k):
                        term = rows[r] * weight(k, r, i)
                        outs[i] = term if outs[i] is None else outs[i] + term
        return outs

    def halves(field):
        return [field[:piece], field[piece:]]

    def far_row(phase, kind, q):
        way = course(kind, q)
        at = 2 + jnp.where(big(way), 1 if way > 0 else 0, 0)
        value = side_in[phase, kind, q, at].astype(F32) * row_weight(7)
        return value, 0 if way > 0 else 1

    def from_side(phase, kind, q, extra=()):
        way = course(kind, q)
        here = side_in.at[phase, kind, q]
        either(way, here.at[4:6], here.at[4:8], fwd_recv.at[phase, kind, q])
        rows = [here[k].astype(F32) for k in (0, 1, 4, 5)]
        rows += [jnp.where(big(way), 0.0, here[k].astype(F32)) for k in (6, 7)]
        outs = weighed(
            [
                ((-2 * way,) * 2, rows[0:2]),
                ((1 - 2 * way, -1 - 2 * way), rows[2:4]),
                ((-3 * way,) * 2, rows[4:6]),
                *extra,
            ]
        )
        value, i = far_row(phase, kind, q)
        outs[i] = outs[i] + value
        return jnp.concatenate(outs, axis=0)

    strip_rows = 2 * piece * STRIP // cols
    lane = lax.broadcasted_iota(jnp.int32, (strip_rows, cols), 1)

    def send_strips(phase, kind, q, field):
        last = first = jnp.zeros((strip_rows, cols), F32)
        for j in range(cols // STRIP):
            group = field[j * strip_rows : (j + 1) * strip_rows]
            mine = lane // STRIP == j
            last = jnp.where(mine, pltpu.roll(group, ((j + 1) * STRIP) % cols, 1), last)
            first = jnp.where(mine, pltpu.roll(group, j * STRIP, 1), first)
        for side, strip in enumerate((last, first)):
            strip_out[phase, kind, q, side] = strip.astype(BF16)
            remote(
                strip_out.at[phase, kind, q, side],
                strip_in.at[phase, kind, q, side],
                strip_send.at[phase],
                strip_recv.at[phase, kind, q],
                col_block(1 - 2 * side),
            )

    def filter_cols(phase, kind, q, field):
        wait_for(strip_in.at[phase, kind, q], strip_recv.at[phase, kind, q])
        left = strip_in[phase, kind, q, 0].astype(F32)
        right = strip_in[phase, kind, q, 1].astype(F32)
        strips = []
        for j in range(cols // STRIP):
            strips.append(
                jnp.where(
                    lane < cols // 2,
                    pltpu.roll(right, (cols - j * STRIP) % cols, 1),
                    pltpu.roll(left, cols - (j + 1) * STRIP, 1),
                )
            )
        strips = jnp.concatenate(strips, axis=0).astype(BF16)
        high = field.astype(BF16)
        low = (field - high.astype(F32)).astype(BF16)
        return jnp.dot(
            jnp.concatenate([high, high, strips, strips, low], axis=1),
            wcol[...],
            preferred_element_type=F32,
        )

    def form_sources(phase, q, grid):
        value = [grid[x * levels : (x + 1) * levels] for x in range(2)]
        mean = [average[x * levels : (x + 1) * levels] for x in range(2)]

        def one(i, carry):
            m = q * piece + i
            for x in range(2):
                if phase == 0:
                    anomaly = ((arch[m, x].astype(F32) - mean[x]) * scale).astype(BF16)
                    arch[m, x] = anomaly
                else:
                    anomaly = arch[m, x]
                product = anomaly.astype(F32) * value[x]
                part[x, pl.ds(pl.multiple_of(i * 8, 8), 8), :] = (
                    product[0:8] + product[8:16]
                ) + (product[16:24] + product[24:32])
            return carry

        lax.fori_loop(0, piece, one, 0, unroll=4)
        for x in range(2):
            for g in range(piece // 8):
                rows = [part[x, pl.ds(g * 64 + k, 8, stride=8), :] for k in range(8)]
                s_ref[q, x * piece + g * 8 : x * piece + g * 8 + 8, :] = (
                    (rows[0] + rows[1]) + (rows[2] + rows[3])
                ) + ((rows[4] + rows[5]) + (rows[6] + rows[7]))

    def member_sum(pieces, carry):
        def one(i, carry):
            for q in pieces:
                carry = tuple(
                    carry[x]
                    + arch[q * piece + i, x].astype(F32) * t_ref[q, pl.ds(x * piece + i, 1), :]
                    for x in range(2)
                )
            return carry

        return lax.fori_loop(0, piece, one, carry, unroll=4)

    def spread(phase, grid, meanwhile, half_in, near_end):
        for q in ORDER:
            form_sources(phase, q, grid)
            send_strips(phase, SOURCE, q, s_ref[q])
            send_block(phase, SOURCE, q, s_ref[q])
        meanwhile()
        for q in ORDER:
            h_ref[phase, q] = filter_cols(phase, SOURCE, q, s_ref[q])
            send_block(phase, FILTERED, q, h_ref[phase, q])
            remote(
                out_ref.at[phase, FILTERED, q],
                beside_in.at[phase, q],
                block_send.at[phase],
                beside_recv.at[phase, q],
                beside_me,
            )
        for q in ORDER:
            pass_on(phase, SOURCE, q)
        for q in ORDER:
            wait_for(beside_in.at[phase, q], beside_recv.at[phase, q])
        half_in()
        for q in ORDER:
            f_ref[q] = from_side(phase, SOURCE, q)
            send_strips(phase, FILTERED, q, f_ref[q])

        def finish(pieces, carry):
            for q in pieces:
                rest = from_side(
                    phase,
                    FILTERED,
                    q,
                    (
                        ((0, 0), halves(h_ref[phase, q])),
                        ((1, -1), [beside_in[phase, q, r].astype(F32) for r in range(2)]),
                    ),
                )
                t_ref[q] = filter_cols(phase, FILTERED, q, f_ref[q]) + rest
            return member_sum(pieces, carry)

        carry = tuple(jnp.zeros((levels, cols), F32) for _ in range(2))
        for q in ORDER:
            pass_on(phase, FILTERED, q)
        carry = finish(ORDER[:2], carry)
        near_end()
        carry = finish(ORDER[2:], carry)
        for x in range(2):
            for h in range(2):
                pmine[phase, h, x] = carry[x][h * half : (h + 1) * half]
        return jnp.concatenate(carry, axis=0)

    def dotted(phase, factor):
        total = None
        for q in ORDER:
            way = course(SOURCE, q)
            here = side_in.at[phase, SOURCE, q]
            own = halves(s_ref[q])
            near = [here[r].astype(F32) * 2.0 for r in range(2)]
            far = [jnp.where(big(way), here[2 + r].astype(F32) * 2.0, 0.0) for r in range(2)]
            mine = weighed([((0, 0), own), ((-2 * way,) * 2, near)])
            value, i = far_row(phase, SOURCE, q)
            mine[i] = mine[i] + value * 2.0
            theirs = weighed(
                [
                    ((-1, 1), own),
                    ((-2 * way - 1, -2 * way + 1), near),
                    ((-3 * way,) * 2, far),
                ]
            )
            field = halves(h_ref[phase, q])
            for i in range(2):
                beside = beside_in[phase, q, i].astype(F32)
                if factor is None:
                    term = mine[i] * field[i] + theirs[i] * beside
                else:
                    term = (mine[i] * factor) * (field[i] * factor) + (theirs[i] * factor) * (
                        beside * factor
                    )
                total = term if total is None else total + term
        return jnp.sum(total, axis=0, keepdims=True)

    def send_increment(phase):
        return remote(
            pmine.at[phase, other], ptheirs.at[phase], p_sem.at[2], p_sem.at[phase], partner
        )

    def folded(vector):
        return (
            sum(vector[:, k * cols : (k + 1) * cols] for k in range(n_obs // cols)) * 0.5
        )

    def reduce_first(which, rows):
        red1[which, gx, 0:1, :] = rows[0]
        red1[which, gx, 1:2, :] = rows[1]
        mine = red1.at[which, gx]
        for k in range(1, n_gx):
            remote(mine, mine, red_send.at[which, 0], red_recv.at[which, 0], row_block(k))

    def reduce_second(which):
        wait_for(red1.at[which, 0 : n_gx - 1], red_recv.at[which, 0])
        red2[which, plane] = jnp.sum(red1[which], axis=0)
        mine = red2.at[which, plane]
        for k in range(1, n_plane):
            remote(mine, mine, red_send.at[which, 1], red_recv.at[which, 1], plane_device(k))

    def reduce_last(which):
        wait_for(red2.at[which, 0 : n_plane - 1], red_recv.at[which, 1])
        both = jnp.sum(jnp.sum(red2[which], axis=0), axis=1, keepdims=True)
        return both[0:1], both[1:2]

    def nothing():
        pass

    grid_b = spread(0, scatter(innovation), nothing, nothing, nothing)
    gsum[ma] = gather(grid_b)
    g_copy = remote(gsum.at[ma], gsum.at[ma], g_sem.at[0], g_sem.at[1], partner)
    send_increment(0)
    reduce_first(
        0,
        (
            folded(innovation * innovation),
            dotted(0, None) + folded(noise * innovation * innovation),
        ),
    )
    g_copy.wait()
    image = gsum[0] + gsum[1] + noise * innovation

    state = {}

    def meanwhile():
        reduce_second(0)

    def half_in():
        norm_now, product = reduce_last(0)
        alpha = norm_now / product
        scaled = alpha * image
        residual = innovation - scaled
        change = folded(scaled * (noise * scaled - 2.0 * image))
        reduce_first(1, (folded(residual * residual), dotted(1, alpha) + change))
        state["step"] = norm_now, product, alpha, residual

    def near_end():
        reduce_second(1)

    spread(1, scatter(image), meanwhile, half_in, near_end)
    send_increment(1)
    for phase in range(2):
        wait_for(sent_rows, block_send.at[phase])
        wait_for(strip_in.at[phase], strip_send.at[phase])
        wait_for(red1.at[phase, 0 : n_gx - 1], red_send.at[phase, 0])
    wait_for(red2.at[0, 0 : n_plane - 1], red_send.at[0, 1])
    wait_for(ptheirs.at[0], p_sem.at[0])

    norm_now, product, alpha, residual = state["step"]
    norm_next, change = reduce_last(1)
    product = product + change
    ratio = norm_next / norm_now
    alpha_next = norm_next / (product - ratio * norm_next / alpha)
    weights = alpha * innovation + alpha_next * (residual + ratio * innovation)
    chosen = jnp.where(ma == 0, weights[:, : n_obs // 2], weights[:, n_obs // 2 :])
    w_ref[0:1, :] = chosen[:, :cols]
    w_ref[1:2, :] = chosen[:, cols:]

    wait_for(ptheirs.at[1], p_sem.at[1])
    first_weight = (alpha + alpha_next * (1.0 + ratio))[None]
    second_weight = (alpha * alpha_next)[None]
    inc_ref[...] = first_weight * (pmine[0, ma] + ptheirs[0]) - second_weight * (
        pmine[1, ma] + ptheirs[1]
    )

    wait_for(ptheirs, p_sem.at[2])
    wait_for(red2.at[1, 0 : n_plane - 1], red_send.at[1, 1])


def shards(n_gx, n_gy, archive, obs_index, obs_value, obs_error):
    members, rows, levels, cols = archive.shape
    half = levels // 2
    n_own = obs_index.shape[0]
    piece = members // CHUNKS
    strip_rows = rows * piece * STRIP // cols
    shape = (n_own // cols, cols)
    dma = pltpu.SemaphoreType.DMA
    vmem = pl.BlockSpec(memory_space=pltpu.VMEM)
    hbm = pl.BlockSpec(memory_space=pltpu.HBM)
    increment, weights = pl.pallas_call(
        functools.partial(kernel, n_gx, n_gy),
        out_shape=(
            pltpu.VMEM((rows, half, cols), F32),
            pltpu.VMEM(shape, F32),
        ),
        in_specs=[hbm, hbm, hbm, hbm],
        out_specs=(vmem, vmem),
        scratch_shapes=[
            pltpu.VMEM((members, rows, levels, cols), BF16),
            pltpu.VMEM(shape, jnp.int32),
            pltpu.VMEM((2, *shape), F32),
            pltpu.VMEM((2, 8, cols), F32),
            pltpu.VMEM((2, rows * levels, cols), F32),
            pltpu.VMEM((rows, piece * 8, cols), F32),
            pltpu.VMEM((CHUNKS, rows * piece, cols), F32),
            pltpu.VMEM((CHUNKS, rows * piece, cols), F32),
            pltpu.VMEM((2, CHUNKS, rows * piece, cols), F32),
            pltpu.VMEM((CHUNKS, rows * piece, cols), F32),
            pltpu.VMEM((2, 2, CHUNKS, rows, piece, cols), BF16),
            pltpu.VMEM((2, 2, CHUNKS, 8, piece, cols), BF16),
            pltpu.VMEM((2, CHUNKS, rows, piece, cols), BF16),
            pltpu.VMEM((15 * CHUNKS, piece, cols), BF16),
            pltpu.VMEM((2, 2, CHUNKS, 2, strip_rows, cols), BF16),
            pltpu.VMEM((2, 2, CHUNKS, 2, strip_rows, cols), BF16),
            pltpu.VMEM((5 * cols, cols), BF16),
            pltpu.VMEM((2, 2, rows, half, cols), F32),
            pltpu.VMEM((2, rows, half, cols), F32),
            pltpu.VMEM((2, 1, 2 * n_own), F32),
            pltpu.VMEM((2, n_gx, 2, cols), F32),
            pltpu.VMEM((2, 2 * n_gy, 2, cols), F32),
            dma((LOADS + 2,)),
            dma((2,)),
            dma((2,)),
            dma((2,)),
            dma((2, 2, CHUNKS)),
            dma((2, 2, CHUNKS)),
            dma((2, CHUNKS)),
            dma((2,)),
            dma((2, 2, CHUNKS)),
            dma((3,)),
            dma((2,)),
            dma((2, 2)),
            dma((2, 2)),
        ],
        compiler_params=pltpu.CompilerParams(
            collective_id=0, has_side_effects=True, vmem_limit_bytes=56 * 1024 * 1024
        ),
        name="analysis",
    )(archive, obs_index.reshape(shape), obs_value.reshape(shape), obs_error.reshape(shape))
    return increment, weights.reshape(n_own)


def solution(mesh):
    n_gx, n_gy = mesh.shape["gx"], mesh.shape["gy"]
    own = P(("gx", "gy", "ma"))
    return jax.shard_map(
        functools.partial(shards, n_gx, n_gy),
        mesh=mesh,
        in_specs=(P("ma", "gx", None, "gy"), own, own, own),
        out_specs=(P("gx", "ma", "gy"), own),
        check_vma=False,
    )
```

```python
import functools
import math

import jax
import jax.numpy as jnp
from jax import lax
from jax.experimental import pallas as pl
from jax.experimental.pallas import tpu as pltpu
from jax.sharding import PartitionSpec as P

M = 512
TAPER_X = 4
TAPER_Y = 8
F32 = jnp.float32
BF16 = jnp.bfloat16
MESH = pl.DeviceIdType.MESH

LOADS = 8
CHUNKS = 4
ORDER = (0, 2, 1, 3)
STRIP = 16
SOURCE, FILTERED = 0, 1


def course(kind, q):
    return (1 if q < CHUNKS // 2 else -1) * (1 if kind == SOURCE else -1)


def row_weight(distance):
    r = abs(distance) / TAPER_X
    if r <= 1.0:
        return (((-0.25 * r + 0.5) * r + 0.625) * r - 5.0 / 3.0) * r * r + 1.0
    if r < 2.0:
        return (
            ((((r / 12.0 - 0.5) * r + 0.625) * r + 5.0 / 3.0) * r - 5.0) * r
            + 4.0
            - 2.0 / (3.0 * r)
        )
    return 0.0


def taper_weight(distance, half_width):
    ratio = jnp.abs(distance) / half_width
    safe = jnp.maximum(ratio, 1.0)
    inner = (((-0.25 * ratio + 0.5) * ratio + 0.625) * ratio - 5.0 / 3.0) * ratio * ratio + 1.0
    outer = (
        ((((ratio / 12.0 - 0.5) * ratio + 0.625) * ratio + 5.0 / 3.0) * ratio - 5.0) * ratio
        + 4.0
        - 2.0 / (3.0 * safe)
    )
    return jnp.where(ratio <= 1.0, inner, jnp.where(ratio < 2.0, outer, 0.0))


def in_three(x):
    first = x.astype(BF16)
    rest = x - first.astype(F32)
    second = rest.astype(BF16)
    third = (rest - second.astype(F32)).astype(BF16)
    return jnp.concatenate([first, second, third], axis=0)


def sum_of_three(y, rows):
    return (y[2 * rows :] + y[rows : 2 * rows]) + y[:rows]


def kernel(
    n_gx,
    n_gy,
    archive_hbm,
    idx_hbm,
    val_hbm,
    err_hbm,
    inc_ref,
    w_ref,
    arch,
    idx_ref,
    pair_ref,
    meta,
    sums,
    part,
    s_ref,
    f_ref,
    h_ref,
    t_ref,
    out_ref,
    side_in,
    beside_in,
    sent_ref,
    strip_out,
    strip_in,
    wcol,
    pmine,
    ptheirs,
    gsum,
    red1,
    red2,
    count_ref,
    load_sem,
    meta_sem,
    sums_sem,
    block_send,
    block_recv,
    fwd_recv,
    beside_recv,
    strip_send,
    strip_recv,
    p_sem,
    g_sem,
    red_send,
    red_recv,
):
    members = arch.shape[0]
    levels = arch.shape[2]
    half = levels // 2
    cols = arch.shape[3]
    piece = members // CHUNKS
    gx = lax.axis_index("gx")
    gy = lax.axis_index("gy")
    ma = lax.axis_index("ma")
    core = lax.rem(gx, 2)
    other = 1 - ma
    sent_rows = sent_ref.at[0 : 15 * CHUNKS]
    plane = gy * 2 + ma
    n_plane = n_gy * 2

    def row_block(k):
        return {"gx": lax.rem(gx + (k + n_gx), n_gx)}

    def col_block(k):
        return {"gy": lax.rem(gy + (k + n_gy), n_gy)}

    def plane_device(k):
        at = lax.rem(plane + k, n_plane)
        return {"gy": at // 2, "ma": lax.rem(at, 2)}

    def remote(src, dst, send_sem, recv_sem, device):
        copy = pltpu.make_async_remote_copy(
            src_ref=src,
            dst_ref=dst,
            send_sem=send_sem,
            recv_sem=recv_sem,
            device_id=device,
            device_id_type=MESH,
        )
        copy.start()
        return copy

    def wait_for(ref, sem):
        pltpu.make_async_copy(ref, ref, sem).wait()

    load = members // LOADS
    loads = []
    for k in range(LOADS):
        copy = pltpu.make_async_copy(
            archive_hbm.at[pl.ds(k * load, load)], arch.at[pl.ds(k * load, load)], load_sem.at[k]
        )
        copy.start()
        loads.append(copy)
    pltpu.make_async_copy(idx_hbm, idx_ref, load_sem.at[LOADS]).start()
    pltpu.make_async_copy(val_hbm, pair_ref.at[0], load_sem.at[LOADS + 1]).start()
    pltpu.make_async_copy(err_hbm, pair_ref.at[1], load_sem.at[LOADS + 1]).start()

    barrier = pltpu.get_barrier_semaphore()
    for k in range(1, n_gx):
        pl.semaphore_signal(barrier, inc=1, device_id=row_block(k), device_id_type=MESH)
    for k in range(1, n_plane):
        pl.semaphore_signal(barrier, inc=1, device_id=plane_device(k), device_id_type=MESH)
        across = {**plane_device(k), **row_block(1 - 2 * core)}
        pl.semaphore_signal(barrier, inc=1, device_id=across, device_id_type=MESH)

    source = lax.broadcasted_iota(jnp.int32, (cols, cols), 0)
    target = lax.broadcasted_iota(jnp.int32, (cols, cols), 1)

    def col_weight(shift):
        return taper_weight((source - target + shift).astype(F32), float(TAPER_Y))

    beside = jnp.where(gy > 0, col_weight(-cols), 0.0) + jnp.where(
        gy < n_gy - 1, col_weight(cols), 0.0
    )
    for k, weight in enumerate((col_weight(0), beside)):
        high = weight.astype(BF16)
        low = (weight - high.astype(F32)).astype(BF16)
        wcol[2 * k * cols : (2 * k + 1) * cols, :] = high
        wcol[(2 * k + 1) * cols : (2 * k + 2) * cols, :] = low
        if k == 0:
            wcol[4 * cols : 5 * cols, :] = high

    total = tuple(jnp.zeros((levels, cols), F32) for _ in range(2))
    for k in range(LOADS):
        loads[k].wait()

        def add(m, carry):
            return tuple(carry[x] + arch[m, x].astype(F32) for x in range(2))

        total = lax.fori_loop(k * load, (k + 1) * load, add, total, unroll=8)
    for x in range(2):
        sums[ma, x * levels : (x + 1) * levels, :] = total[x]
    wait_for(idx_ref, load_sem.at[LOADS])
    wait_for(pair_ref, load_sem.at[LOADS + 1])
    meta[ma, 0:2, :] = idx_ref[...].astype(F32)
    meta[ma, 2:4, :] = pair_ref[0]
    meta[ma, 4:6, :] = pair_ref[1]
    meta[ma, 6:8, :] = jnp.zeros((2, cols), F32)

    pl.semaphore_wait(barrier, n_gx - 1 + 2 * (n_plane - 1))

    partner = {"ma": other}
    meta_copy = remote(meta.at[ma], meta.at[ma], meta_sem.at[0], meta_sem.at[1], partner)
    sums_copy = remote(sums.at[ma], sums.at[ma], sums_sem.at[0], sums_sem.at[1], partner)

    meta_copy.wait()

    def in_a_row(first):
        rows = [meta[h, first + i : first + i + 1, :] for h in range(2) for i in range(2)]
        return jnp.concatenate(rows, axis=1)

    index = in_a_row(0).astype(jnp.int32)
    target_value = in_a_row(2)
    noise = in_a_row(4)
    n_obs = index.shape[1]
    owner = lax.broadcasted_iota(jnp.int32, (1, n_obs), 1) // (n_obs // 2)
    obs_line = (index >> 11) * levels + owner * half + ((index >> 7) & (half - 1))
    obs_col = index & (cols - 1)
    line_hot = (
        lax.broadcasted_iota(jnp.int32, (2 * levels, n_obs), 0) == obs_line
    ).astype(F32)
    col_hot = (
        (lax.broadcasted_iota(jnp.int32, (cols, n_obs), 0) == obs_col).astype(F32).astype(BF16)
    )

    def gather(grid):
        rows = 2 * levels
        spread = jnp.dot(in_three(grid), col_hot, preferred_element_type=F32)
        return jnp.sum(sum_of_three(spread, rows) * line_hot, axis=0, keepdims=True)

    def scatter(vector):
        rows = 2 * levels
        spread = lax.dot_general(
            in_three(line_hot * vector),
            col_hot,
            (((1,), (1,)), ((), ())),
            preferred_element_type=F32,
        )
        return sum_of_three(spread, rows)

    sums_copy.wait()
    average = (sums[0] + sums[1]) * (1.0 / M)
    innovation = target_value - gather(average)
    scale = 1.0 / math.sqrt(M - 1.0)

    beside_me = row_block(1 - 2 * core)

    def big(way):
        return core == (1 if way > 0 else 0)

    def send_block(phase, kind, q, field):
        way = course(kind, q)
        row = 1 if way > 0 else 0
        for x in range(2):
            out_ref[phase, kind, q, x] = field[x * piece : (x + 1) * piece].astype(BF16)
        block = out_ref.at[phase, kind, q]
        here = side_in.at[phase, kind, q]
        sems = block_send.at[phase], block_recv.at[phase, kind, q]

        @pl.when(big(way))
        def _():
            remote(block, here.at[2:4], *sems, row_block(4 * way))

        @pl.when(jnp.logical_not(big(way)))
        def _():
            remote(block.at[row], here.at[2], *sems, row_block(4 * way))

        remote(block, here.at[0:2], *sems, row_block(2 * way))

    def either(way, size_if_big, size_if_not, sem):
        @pl.when(big(way))
        def _():
            wait_for(size_if_big, sem)

        @pl.when(jnp.logical_not(big(way)))
        def _():
            wait_for(size_if_not, sem)

    def pass_on(phase, kind, q):
        way = course(kind, q)
        here = side_in.at[phase, kind, q]
        sem = block_recv.at[phase, kind, q]
        either(way, here.at[0:4], here.at[0:3], sem)
        sems = block_send.at[phase], fwd_recv.at[phase, kind, q]

        @pl.when(big(way))
        def _():
            remote(here.at[0:4], here.at[4:8], *sems, beside_me)

        @pl.when(jnp.logical_not(big(way)))
        def _():
            remote(here.at[0:2], here.at[4:6], *sems, beside_me)

    def weight(k, r, i):
        both = [row_weight(2 * at + r - i) for at in k]
        return both[0] if both[0] == both[1] else jnp.where(core == 0, both[0], both[1])

    def weighed(terms):
        outs = [None, None]
        for k, rows in terms:
            for r in range(2):
                for i in range(2):
                    if any(row_weight(2 * at + r - i) for at in k):
                        term = rows[r] * weight(k, r, i)
                        outs[i] = term if outs[i] is None else outs[i] + term
        return outs

    def halves(field):
        return [field[:piece], field[piece:]]

    def far_row(phase, kind, q):
        way = course(kind, q)
        at = 2 + jnp.where(big(way), 1 if way > 0 else 0, 0)
        value = side_in[phase, kind, q, at].astype(F32) * row_weight(7)
        return value, 0 if way > 0 else 1

    def passed_in(phase, kind, q):
        here = side_in.at[phase, kind, q]
        either(course(kind, q), here.at[4:6], here.at[4:8], fwd_recv.at[phase, kind, q])

    def from_side(phase, kind, q, extra=()):
        way = course(kind, q)
        here = side_in.at[phase, kind, q]
        rows = [here[k].astype(F32) for k in (0, 1, 4, 5)]
        rows += [jnp.where(big(way), 0.0, here[k].astype(F32)) for k in (6, 7)]
        outs = weighed(
            [
                ((-2 * way,) * 2, rows[0:2]),
                ((1 - 2 * way, -1 - 2 * way), rows[2:4]),
                ((-3 * way,) * 2, rows[4:6]),
                *extra,
            ]
        )
        value, i = far_row(phase, kind, q)
        outs[i] = outs[i] + value
        return jnp.concatenate(outs, axis=0)

    strip_rows = 2 * piece * STRIP // cols
    lane = lax.broadcasted_iota(jnp.int32, (strip_rows, cols), 1)

    def send_strips(phase, kind, q, field):
        last = first = jnp.zeros((strip_rows, cols), F32)
        for j in range(cols // STRIP):
            group = field[j * strip_rows : (j + 1) * strip_rows]
            mine = lane // STRIP == j
            last = jnp.where(mine, pltpu.roll(group, ((j + 1) * STRIP) % cols, 1), last)
            first = jnp.where(mine, pltpu.roll(group, j * STRIP, 1), first)
        for side, strip in enumerate((last, first)):
            strip_out[phase, kind, q, side] = strip.astype(BF16)
            remote(
                strip_out.at[phase, kind, q, side],
                strip_in.at[phase, kind, q, side],
                strip_send.at[phase],
                strip_recv.at[phase, kind, q],
                col_block(1 - 2 * side),
            )

    def strips_in(phase, kind, q):
        wait_for(strip_in.at[phase, kind, q], strip_recv.at[phase, kind, q])

    def filter_cols(phase, kind, q, field):
        left = strip_in[phase, kind, q, 0].astype(F32)
        right = strip_in[phase, kind, q, 1].astype(F32)
        strips = []
        for j in range(cols // STRIP):
            strips.append(
                jnp.where(
                    lane < cols // 2,
                    pltpu.roll(right, (cols - j * STRIP) % cols, 1),
                    pltpu.roll(left, cols - (j + 1) * STRIP, 1),
                )
            )
        strips = jnp.concatenate(strips, axis=0).astype(BF16)
        high = field.astype(BF16)
        low = (field - high.astype(F32)).astype(BF16)
        return jnp.dot(
            jnp.concatenate([high, high, strips, strips, low], axis=1),
            wcol[...],
            preferred_element_type=F32,
        )

    def form_sources(phase, q, grid):
        value = [grid[x * levels : (x + 1) * levels] for x in range(2)]
        mean = [average[x * levels : (x + 1) * levels] for x in range(2)]

        def one(i, carry):
            m = q * piece + i
            for x in range(2):
                if phase == 0:
                    anomaly = ((arch[m, x].astype(F32) - mean[x]) * scale).astype(BF16)
                    arch[m, x] = anomaly
                else:
                    anomaly = arch[m, x]
                product = anomaly.astype(F32) * value[x]
                part[x, pl.ds(pl.multiple_of(i * 8, 8), 8), :] = (
                    product[0:8] + product[8:16]
                ) + (product[16:24] + product[24:32])
            return carry

        lax.fori_loop(0, piece, one, 0, unroll=8)
        for x in range(2):
            for g in range(piece // 8):
                rows = [part[x, pl.ds(g * 64 + k, 8, stride=8), :] for k in range(8)]
                s_ref[q, x * piece + g * 8 : x * piece + g * 8 + 8, :] = (
                    (rows[0] + rows[1]) + (rows[2] + rows[3])
                ) + ((rows[4] + rows[5]) + (rows[6] + rows[7]))

    def member_sum(pieces, carry):
        def one(i, carry):
            for q in pieces:
                carry = tuple(
                    carry[x]
                    + arch[q * piece + i, x].astype(F32) * t_ref[q, pl.ds(x * piece + i, 1), :]
                    for x in range(2)
                )
            return carry

        return lax.fori_loop(0, piece, one, carry, unroll=8)

    def spread(phase, grid, before_last, half_in, near_end):
        for q in ORDER:
            form_sources(phase, q, grid)
            send_strips(phase, SOURCE, q, s_ref[q])
            send_block(phase, SOURCE, q, s_ref[q])
        def filter_own(pieces):
            for q in pieces:
                strips_in(phase, SOURCE, q)
                h_ref[phase, q] = filter_cols(phase, SOURCE, q, s_ref[q])
                send_block(phase, FILTERED, q, h_ref[phase, q])
                remote(
                    out_ref.at[phase, FILTERED, q],
                    beside_in.at[phase, q],
                    block_send.at[phase],
                    beside_recv.at[phase, q],
                    beside_me,
                )

        def filter_one_side(pieces):
            for q in pieces:
                passed_in(phase, SOURCE, q)
                f_ref[q] = from_side(phase, SOURCE, q)
                send_strips(phase, FILTERED, q, f_ref[q])

        early, late = ORDER[:2], ORDER[2:]
        filter_own(early)
        if phase == 0:
            for q in early:
                pass_on(phase, SOURCE, q)
            filter_own(late[:1])
            filter_one_side(early)
            filter_own(late[1:])
        else:
            filter_own(late)
            for q in early:
                pass_on(phase, SOURCE, q)
        for q in ORDER:
            wait_for(beside_in.at[phase, q], beside_recv.at[phase, q])
        before_last()
        for q in late:
            pass_on(phase, SOURCE, q)
        half_in()
        if phase == 1:
            filter_one_side(early)
        filter_one_side(late)

        def finish(pieces, carry):
            for q in pieces:
                passed_in(phase, FILTERED, q)
                strips_in(phase, FILTERED, q)
            filtered = [filter_cols(phase, FILTERED, q, f_ref[q]) for q in pieces]
            for q, of_one_side in zip(pieces, filtered):
                rest = from_side(
                    phase,
                    FILTERED,
                    q,
                    (
                        ((0, 0), halves(h_ref[phase, q])),
                        ((1, -1), [beside_in[phase, q, r].astype(F32) for r in range(2)]),
                    ),
                )
                t_ref[q] = of_one_side + rest
            return member_sum(pieces, carry)

        carry = tuple(jnp.zeros((levels, cols), F32) for _ in range(2))
        if phase == 0:
            for pieces in (early, late):
                for q in pieces:
                    pass_on(phase, FILTERED, q)
                carry = finish(pieces, carry)
        else:
            for q in ORDER:
                pass_on(phase, FILTERED, q)
            carry = finish(early, carry)
            near_end()
            carry = finish(late, carry)
        for x in range(2):
            for h in range(2):
                pmine[phase, h, x] = carry[x][h * half : (h + 1) * half]
        return jnp.concatenate(carry, axis=0)

    def dotted(phase, factor, pieces):
        total = None
        for q in pieces:
            way = course(SOURCE, q)
            here = side_in.at[phase, SOURCE, q]
            own = halves(s_ref[q])
            near = [here[r].astype(F32) * 2.0 for r in range(2)]
            far = [jnp.where(big(way), here[2 + r].astype(F32) * 2.0, 0.0) for r in range(2)]
            mine = weighed([((0, 0), own), ((-2 * way,) * 2, near)])
            value, i = far_row(phase, SOURCE, q)
            mine[i] = mine[i] + value * 2.0
            theirs = weighed(
                [
                    ((-1, 1), own),
                    ((-2 * way - 1, -2 * way + 1), near),
                    ((-3 * way,) * 2, far),
                ]
            )
            field = halves(h_ref[phase, q])
            for i in range(2):
                beside = beside_in[phase, q, i].astype(F32)
                if factor is None:
                    term = mine[i] * field[i] + theirs[i] * beside
                else:
                    term = (mine[i] * factor) * (field[i] * factor) + (theirs[i] * factor) * (
                        beside * factor
                    )
                total = term if total is None else total + term
        return jnp.sum(total, axis=0, keepdims=True)

    def send_increment(phase):
        return remote(
            pmine.at[phase, other], ptheirs.at[phase], p_sem.at[2], p_sem.at[phase], partner
        )

    def folded(vector):
        return (
            sum(vector[:, k * cols : (k + 1) * cols] for k in range(n_obs // cols)) * 0.5
        )

    n_z = n_gx // 2
    hub = core == 1

    def reduce_first(which, rows):
        red1[which, gx, 0:1, :] = rows[0]
        red1[which, gx, 1:2, :] = rows[1]
        mine = red1.at[which, gx]
        sems = red_send.at[which, 0], red_recv.at[which, 0]
        for k in range(1, n_z):
            remote(mine, mine, *sems, {"gx": 2 * lax.rem(gx // 2 + k, n_z) + 1})

        @pl.when(jnp.logical_not(hub))
        def _():
            remote(mine, mine, *sems, {"gx": gx + 1})

    def reduce_second(which):
        @pl.when(hub)
        def _():
            wait_for(red1.at[which, 0 : n_gx - 1], red_recv.at[which, 0])
            red2[which, plane] = jnp.sum(red1[which], axis=0)
            mine = red2.at[which, plane]
            sems = red_send.at[which, 1], red_recv.at[which, 1]
            for k in range(1, n_plane):
                remote(mine, mine, *sems, {**plane_device(k), "gx": gx - 1})
            for k in range(1, n_plane):
                remote(mine, mine, *sems, plane_device(k))
            remote(mine, mine, *sems, {"gx": gx - 1})

    def reduce_last(which):
        @pl.when(hub)
        def _():
            wait_for(red2.at[which, 0 : n_plane - 1], red_recv.at[which, 1])

        @pl.when(jnp.logical_not(hub))
        def _():
            wait_for(red2.at[which, 0:n_plane], red_recv.at[which, 1])

        both = jnp.sum(jnp.sum(red2[which], axis=0), axis=1, keepdims=True)
        return both[0:1], both[1:2]

    def reduce_sent(which):
        @pl.when(hub)
        def _():
            wait_for(count_ref.at[0 : n_z - 1], red_send.at[which, 0])
            wait_for(count_ref.at[0 : 2 * n_plane - 1], red_send.at[which, 1])

        @pl.when(jnp.logical_not(hub))
        def _():
            wait_for(count_ref.at[0:n_z], red_send.at[which, 0])

    def first_half_in():
        product = folded(noise * innovation * innovation) + dotted(0, None, ORDER)
        reduce_first(0, (folded(innovation * innovation), product))

    grid_b = spread(0, scatter(innovation), lambda: None, first_half_in, lambda: None)
    gsum[ma] = gather(grid_b)
    g_copy = remote(gsum.at[ma], gsum.at[ma], g_sem.at[0], g_sem.at[1], partner)
    send_increment(0)
    reduce_second(0)
    g_copy.wait()
    image = gsum[0] + gsum[1] + noise * innovation

    state = {}

    def before_last():
        norm_now, product = reduce_last(0)
        alpha = norm_now / product
        scaled = alpha * image
        residual = innovation - scaled
        change = folded(scaled * (noise * scaled - 2.0 * image)) + dotted(1, alpha, ORDER[:2])
        state["step"] = norm_now, product, alpha, residual
        state["sums"] = folded(residual * residual), change

    def half_in():
        norm, change = state["sums"]
        reduce_first(1, (norm, change + dotted(1, state["step"][2], ORDER[2:])))

    spread(1, scatter(image), before_last, half_in, lambda: reduce_second(1))
    send_increment(1)
    for phase in range(2):
        wait_for(sent_rows, block_send.at[phase])
        wait_for(strip_in.at[phase], strip_send.at[phase])
    reduce_sent(0)
    wait_for(ptheirs.at[0], p_sem.at[0])

    norm_now, product, alpha, residual = state["step"]
    norm_next, change = reduce_last(1)
    product = product + change
    ratio = norm_next / norm_now
    alpha_next = norm_next / (product - ratio * norm_next / alpha)
    weights = alpha * innovation + alpha_next * (residual + ratio * innovation)
    chosen = jnp.where(ma == 0, weights[:, : n_obs // 2], weights[:, n_obs // 2 :])
    w_ref[0:1, :] = chosen[:, :cols]
    w_ref[1:2, :] = chosen[:, cols:]

    wait_for(ptheirs.at[1], p_sem.at[1])
    first_weight = (alpha + alpha_next * (1.0 + ratio))[None]
    second_weight = (alpha * alpha_next)[None]
    inc_ref[...] = first_weight * (pmine[0, ma] + ptheirs[0]) - second_weight * (
        pmine[1, ma] + ptheirs[1]
    )

    wait_for(ptheirs, p_sem.at[2])
    reduce_sent(1)


def shards(n_gx, n_gy, archive, obs_index, obs_value, obs_error):
    members, rows, levels, cols = archive.shape
    half = levels // 2
    n_own = obs_index.shape[0]
    piece = members // CHUNKS
    strip_rows = rows * piece * STRIP // cols
    shape = (n_own // cols, cols)
    dma = pltpu.SemaphoreType.DMA
    vmem = pl.BlockSpec(memory_space=pltpu.VMEM)
    hbm = pl.BlockSpec(memory_space=pltpu.HBM)
    increment, weights = pl.pallas_call(
        functools.partial(kernel, n_gx, n_gy),
        out_shape=(
            pltpu.VMEM((rows, half, cols), F32),
            pltpu.VMEM(shape, F32),
        ),
        in_specs=[hbm, hbm, hbm, hbm],
        out_specs=(vmem, vmem),
        scratch_shapes=[
            pltpu.VMEM((members, rows, levels, cols), BF16),
            pltpu.VMEM(shape, jnp.int32),
            pltpu.VMEM((2, *shape), F32),
            pltpu.VMEM((2, 8, cols), F32),
            pltpu.VMEM((2, rows * levels, cols), F32),
            pltpu.VMEM((rows, piece * 8, cols), F32),
            pltpu.VMEM((CHUNKS, rows * piece, cols), F32),
            pltpu.VMEM((CHUNKS, rows * piece, cols), F32),
            pltpu.VMEM((2, CHUNKS, rows * piece, cols), F32),
            pltpu.VMEM((CHUNKS, rows * piece, cols), F32),
            pltpu.VMEM((2, 2, CHUNKS, rows, piece, cols), BF16),
            pltpu.VMEM((2, 2, CHUNKS, 8, piece, cols), BF16),
            pltpu.VMEM((2, CHUNKS, rows, piece, cols), BF16),
            pltpu.VMEM((15 * CHUNKS, piece, cols), BF16),
            pltpu.VMEM((2, 2, CHUNKS, 2, strip_rows, cols), BF16),
            pltpu.VMEM((2, 2, CHUNKS, 2, strip_rows, cols), BF16),
            pltpu.VMEM((5 * cols, cols), BF16),
            pltpu.VMEM((2, 2, rows, half, cols), F32),
            pltpu.VMEM((2, rows, half, cols), F32),
            pltpu.VMEM((2, 1, 2 * n_own), F32),
            pltpu.VMEM((2, n_gx, 2, cols), F32),
            pltpu.VMEM((2, 2 * n_gy, 2, cols), F32),
            pltpu.VMEM((4 * n_gy, 2, cols), F32),
            dma((LOADS + 2,)),
            dma((2,)),
            dma((2,)),
            dma((2,)),
            dma((2, 2, CHUNKS)),
            dma((2, 2, CHUNKS)),
            dma((2, CHUNKS)),
            dma((2,)),
            dma((2, 2, CHUNKS)),
            dma((3,)),
            dma((2,)),
            dma((2, 2)),
            dma((2, 2)),
        ],
        compiler_params=pltpu.CompilerParams(
            collective_id=0, has_side_effects=True, vmem_limit_bytes=56 * 1024 * 1024
        ),
        name="analysis",
    )(archive, obs_index.reshape(shape), obs_value.reshape(shape), obs_error.reshape(shape))
    return increment, weights.reshape(n_own)


def solution(mesh):
    n_gx, n_gy = mesh.shape["gx"], mesh.shape["gy"]
    own = P(("gx", "gy", "ma"))
    return jax.shard_map(
        functools.partial(shards, n_gx, n_gy),
        mesh=mesh,
        in_specs=(P("ma", "gx", None, "gy"), own, own, own),
        out_specs=(P("gx", "ma", "gy"), own),
        check_vma=False,
    )
```

```python
import functools
import math

import jax
import jax.numpy as jnp
from jax import lax
from jax.experimental import pallas as pl
from jax.experimental.pallas import tpu as pltpu
from jax.sharding import PartitionSpec as P

M = 512
TAPER_X = 4
TAPER_Y = 8
F32 = jnp.float32
BF16 = jnp.bfloat16
MESH = pl.DeviceIdType.MESH

LOADS = 8
CHUNKS = 4
PAIRS = CHUNKS // 2
STRIP = 16
SOURCE, FILTERED = 0, 1


def course(kind, q):
    return (1 if q % 2 == 0 else -1) * (1 if kind == SOURCE else -1)


def row_weight(distance):
    r = abs(distance) / TAPER_X
    if r <= 1.0:
        return (((-0.25 * r + 0.5) * r + 0.625) * r - 5.0 / 3.0) * r * r + 1.0
    if r < 2.0:
        return (
            ((((r / 12.0 - 0.5) * r + 0.625) * r + 5.0 / 3.0) * r - 5.0) * r
            + 4.0
            - 2.0 / (3.0 * r)
        )
    return 0.0


def taper_weight(distance, half_width):
    ratio = jnp.abs(distance) / half_width
    safe = jnp.maximum(ratio, 1.0)
    inner = (((-0.25 * ratio + 0.5) * ratio + 0.625) * ratio - 5.0 / 3.0) * ratio * ratio + 1.0
    outer = (
        ((((ratio / 12.0 - 0.5) * ratio + 0.625) * ratio + 5.0 / 3.0) * ratio - 5.0) * ratio
        + 4.0
        - 2.0 / (3.0 * safe)
    )
    return jnp.where(ratio <= 1.0, inner, jnp.where(ratio < 2.0, outer, 0.0))


def in_three(x):
    first = x.astype(BF16)
    rest = x - first.astype(F32)
    second = rest.astype(BF16)
    third = (rest - second.astype(F32)).astype(BF16)
    return jnp.concatenate([first, second, third], axis=0)


def sum_of_three(y, rows):
    return (y[2 * rows :] + y[rows : 2 * rows]) + y[:rows]


def kernel(
    n_gx,
    n_gy,
    archive_hbm,
    idx_hbm,
    val_hbm,
    err_hbm,
    inc_ref,
    w_ref,
    arch,
    idx_ref,
    pair_ref,
    meta,
    sums,
    part,
    s_ref,
    f_ref,
    h_ref,
    t_ref,
    out_ref,
    side_in,
    beside_in,
    count_rows,
    strip_out,
    strip_in,
    wcol,
    pmine,
    ptheirs,
    gsum,
    red1,
    red2,
    count_ref,
    load_sem,
    meta_sem,
    sums_sem,
    block_send,
    block_recv,
    fwd_recv,
    beside_recv,
    strip_send,
    strip_recv,
    p_sem,
    g_sem,
    red_send,
    red_recv,
):
    members = arch.shape[0]
    levels = arch.shape[2]
    half = levels // 2
    cols = arch.shape[3]
    piece = members // CHUNKS
    gx = lax.axis_index("gx")
    gy = lax.axis_index("gy")
    ma = lax.axis_index("ma")
    core = lax.rem(gx, 2)
    other = 1 - ma
    sent_rows = count_rows.at[0 : 15 * CHUNKS]
    plane = gy * 2 + ma
    n_plane = n_gy * 2

    def row_block(k):
        return {"gx": lax.rem(gx + (k + n_gx), n_gx)}

    def col_block(k):
        return {"gy": lax.rem(gy + (k + n_gy), n_gy)}

    def plane_device(k):
        at = lax.rem(plane + k, n_plane)
        return {"gy": at // 2, "ma": lax.rem(at, 2)}

    def remote(src, dst, send_sem, recv_sem, device):
        copy = pltpu.make_async_remote_copy(
            src_ref=src,
            dst_ref=dst,
            send_sem=send_sem,
            recv_sem=recv_sem,
            device_id=device,
            device_id_type=MESH,
        )
        copy.start()
        return copy

    def wait_for(ref, sem):
        pltpu.make_async_copy(ref, ref, sem).wait()

    load = members // LOADS
    loads = []
    for k in range(LOADS):
        copy = pltpu.make_async_copy(
            archive_hbm.at[pl.ds(k * load, load)], arch.at[pl.ds(k * load, load)], load_sem.at[k]
        )
        copy.start()
        loads.append(copy)
    pltpu.make_async_copy(idx_hbm, idx_ref, load_sem.at[LOADS]).start()
    pltpu.make_async_copy(val_hbm, pair_ref.at[0], load_sem.at[LOADS + 1]).start()
    pltpu.make_async_copy(err_hbm, pair_ref.at[1], load_sem.at[LOADS + 1]).start()

    barrier = pltpu.get_barrier_semaphore()
    def far_first(count):
        return sorted(range(1, count), key=lambda k: -min(k, count - k))

    for k in far_first(n_gx):
        pl.semaphore_signal(barrier, inc=1, device_id=row_block(k), device_id_type=MESH)
    for k in far_first(n_plane):
        across = {**plane_device(k), **row_block(1 - 2 * core)}
        for device in (plane_device(k), across):
            pl.semaphore_signal(barrier, inc=1, device_id=device, device_id_type=MESH)

    total = tuple(jnp.zeros((levels, cols), F32) for _ in range(2))
    for k in range(LOADS):
        loads[k].wait()

        def add(m, carry):
            return tuple(carry[x] + arch[m, x].astype(F32) for x in range(2))

        total = lax.fori_loop(k * load, (k + 1) * load, add, total, unroll=8)
    for x in range(2):
        sums[ma, x * levels : (x + 1) * levels, :] = total[x]
    wait_for(idx_ref, load_sem.at[LOADS])
    wait_for(pair_ref, load_sem.at[LOADS + 1])
    meta[ma, 0:2, :] = idx_ref[...].astype(F32)
    meta[ma, 2:4, :] = pair_ref[0]
    meta[ma, 4:6, :] = pair_ref[1]
    meta[ma, 6:8, :] = jnp.zeros((2, cols), F32)

    pl.semaphore_wait(barrier, n_gx - 1 + 2 * (n_plane - 1))

    partner = {"ma": other}
    meta_copy = remote(meta.at[ma], meta.at[ma], meta_sem.at[0], meta_sem.at[1], partner)
    sums_copy = remote(sums.at[ma], sums.at[ma], sums_sem.at[0], sums_sem.at[1], partner)

    source = lax.broadcasted_iota(jnp.int32, (cols, cols), 0)
    target = lax.broadcasted_iota(jnp.int32, (cols, cols), 1)

    def col_weight(shift):
        return taper_weight((source - target + shift).astype(F32), float(TAPER_Y))

    beside = jnp.where(gy > 0, col_weight(-cols), 0.0) + jnp.where(
        gy < n_gy - 1, col_weight(cols), 0.0
    )
    for k, weight in enumerate((col_weight(0), beside)):
        high = weight.astype(BF16)
        low = (weight - high.astype(F32)).astype(BF16)
        wcol[2 * k * cols : (2 * k + 1) * cols, :] = high
        wcol[(2 * k + 1) * cols : (2 * k + 2) * cols, :] = low
        if k == 0:
            wcol[4 * cols : 5 * cols, :] = high

    meta_copy.wait()

    def in_a_row(first):
        rows = [meta[h, first + i : first + i + 1, :] for h in range(2) for i in range(2)]
        return jnp.concatenate(rows, axis=1)

    index = in_a_row(0).astype(jnp.int32)
    target_value = in_a_row(2)
    noise = in_a_row(4)
    n_obs = index.shape[1]
    owner = lax.broadcasted_iota(jnp.int32, (1, n_obs), 1) // (n_obs // 2)
    obs_line = (index >> 11) * levels + owner * half + ((index >> 7) & (half - 1))
    obs_col = index & (cols - 1)
    line_hot = (
        lax.broadcasted_iota(jnp.int32, (2 * levels, n_obs), 0) == obs_line
    ).astype(F32)
    col_hot = (
        (lax.broadcasted_iota(jnp.int32, (cols, n_obs), 0) == obs_col).astype(F32).astype(BF16)
    )

    def gather(grid):
        rows = 2 * levels
        spread = jnp.dot(in_three(grid), col_hot, preferred_element_type=F32)
        return jnp.sum(sum_of_three(spread, rows) * line_hot, axis=0, keepdims=True)

    def scatter(vector):
        rows = 2 * levels
        spread = lax.dot_general(
            in_three(line_hot * vector),
            col_hot,
            (((1,), (1,)), ((), ())),
            preferred_element_type=F32,
        )
        return sum_of_three(spread, rows)

    sums_copy.wait()
    average = (sums[0] + sums[1]) * (1.0 / M)
    innovation = target_value - gather(average)
    scale = 1.0 / math.sqrt(M - 1.0)

    beside_me = row_block(1 - 2 * core)

    def big(way):
        return core == (1 if way > 0 else 0)

    def send_block(phase, kind, q, field):
        way = course(kind, q)
        row = 1 if way > 0 else 0
        for x in range(2):
            out_ref[phase, kind, q, x] = field[x * piece : (x + 1) * piece].astype(BF16)
        block = out_ref.at[phase, kind, q]
        here = side_in.at[phase, kind, q]
        sems = block_send.at[phase], block_recv.at[phase, kind, q // 2]

        @pl.when(big(way))
        def _():
            remote(block, here.at[2:4], *sems, row_block(4 * way))

        @pl.when(jnp.logical_not(big(way)))
        def _():
            remote(block.at[row], here.at[2], *sems, row_block(4 * way))

        remote(block, here.at[0:2], *sems, row_block(2 * way))

    def pass_on(phase, kind, pair):
        wait_for(count_rows.at[0:7], block_recv.at[phase, kind, pair])
        sems = block_send.at[phase], fwd_recv.at[phase, kind, pair]
        for q in (2 * pair, 2 * pair + 1):
            way = course(kind, q)
            here = side_in.at[phase, kind, q]

            @pl.when(big(way))
            def _(here=here):
                remote(here.at[0:4], here.at[4:8], *sems, beside_me)

            @pl.when(jnp.logical_not(big(way)))
            def _(here=here):
                remote(here.at[0:2], here.at[4:6], *sems, beside_me)

    def passed_in(phase, kind, pair):
        wait_for(count_rows.at[0:6], fwd_recv.at[phase, kind, pair])

    def come_beside(phase):
        for pair in range(PAIRS):
            both = beside_in.at[phase, 2 * pair : 2 * pair + 2]
            wait_for(both, beside_recv.at[phase, pair])

    def weight(k, r, i):
        both = [row_weight(2 * at + r - i) for at in k]
        return both[0] if both[0] == both[1] else jnp.where(core == 0, both[0], both[1])

    def weighed(terms):
        outs = [None, None]
        for k, rows in terms:
            for r in range(2):
                for i in range(2):
                    if any(row_weight(2 * at + r - i) for at in k):
                        term = rows[r] * weight(k, r, i)
                        outs[i] = term if outs[i] is None else outs[i] + term
        return outs

    def halves(field):
        return [field[:piece], field[piece:]]

    def far_row(phase, kind, q):
        way = course(kind, q)
        at = 2 + jnp.where(big(way), 1 if way > 0 else 0, 0)
        value = side_in[phase, kind, q, at].astype(F32) * row_weight(7)
        return value, 0 if way > 0 else 1

    def from_side(phase, kind, q, extra=()):
        way = course(kind, q)
        here = side_in.at[phase, kind, q]
        rows = [here[k].astype(F32) for k in (0, 1, 4, 5)]
        rows += [jnp.where(big(way), 0.0, here[k].astype(F32)) for k in (6, 7)]
        outs = weighed(
            [
                ((-2 * way,) * 2, rows[0:2]),
                ((1 - 2 * way, -1 - 2 * way), rows[2:4]),
                ((-3 * way,) * 2, rows[4:6]),
                *extra,
            ]
        )
        value, i = far_row(phase, kind, q)
        outs[i] = outs[i] + value
        return jnp.concatenate(outs, axis=0)

    strip_rows = 2 * piece * STRIP // cols
    lane = lax.broadcasted_iota(jnp.int32, (strip_rows, cols), 1)

    def send_strips(phase, kind, q, field):
        last = first = jnp.zeros((strip_rows, cols), F32)
        for j in range(cols // STRIP):
            group = field[j * strip_rows : (j + 1) * strip_rows]
            mine = lane // STRIP == j
            last = jnp.where(mine, pltpu.roll(group, ((j + 1) * STRIP) % cols, 1), last)
            first = jnp.where(mine, pltpu.roll(group, j * STRIP, 1), first)
        for side, strip in enumerate((last, first)):
            strip_out[phase, kind, q, side] = strip.astype(BF16)
            remote(
                strip_out.at[phase, kind, q, side],
                strip_in.at[phase, kind, q, side],
                strip_send.at[phase],
                strip_recv.at[phase, q if kind == SOURCE else CHUNKS + q // 2],
                col_block(1 - 2 * side),
            )

    def filter_cols(phase, kind, q, field):
        left = strip_in[phase, kind, q, 0].astype(F32)
        right = strip_in[phase, kind, q, 1].astype(F32)
        strips = []
        for j in range(cols // STRIP):
            strips.append(
                jnp.where(
                    lane < cols // 2,
                    pltpu.roll(right, (cols - j * STRIP) % cols, 1),
                    pltpu.roll(left, cols - (j + 1) * STRIP, 1),
                )
            )
        strips = jnp.concatenate(strips, axis=0).astype(BF16)
        high = field.astype(BF16)
        low = (field - high.astype(F32)).astype(BF16)
        return jnp.dot(
            jnp.concatenate([high, high, strips, strips, low], axis=1),
            wcol[...],
            preferred_element_type=F32,
        )

    def form_sources(phase, q, grid):
        value = [grid[x * levels : (x + 1) * levels] for x in range(2)]
        mean = [average[x * levels : (x + 1) * levels] for x in range(2)]

        def one(i, carry):
            m = q * piece + i
            for x in range(2):
                if phase == 0:
                    anomaly = ((arch[m, x].astype(F32) - mean[x]) * scale).astype(BF16)
                    arch[m, x] = anomaly
                else:
                    anomaly = arch[m, x]
                product = anomaly.astype(F32) * value[x]
                part[x, pl.ds(pl.multiple_of(i * 8, 8), 8), :] = (
                    product[0:8] + product[8:16]
                ) + (product[16:24] + product[24:32])
            return carry

        lax.fori_loop(0, piece, one, 0, unroll=8)
        for x in range(2):
            for g in range(piece // 8):
                rows = [part[x, pl.ds(g * 64 + k, 8, stride=8), :] for k in range(8)]
                s_ref[q, x * piece + g * 8 : x * piece + g * 8 + 8, :] = (
                    (rows[0] + rows[1]) + (rows[2] + rows[3])
                ) + ((rows[4] + rows[5]) + (rows[6] + rows[7]))

    def member_sum(pieces, carry):
        def one(i, carry):
            for q in pieces:
                carry = tuple(
                    carry[x]
                    + arch[q * piece + i, x].astype(F32) * t_ref[q, pl.ds(x * piece + i, 1), :]
                    for x in range(2)
                )
            return carry

        return lax.fori_loop(0, piece, one, carry, unroll=8)

    def spread(phase, grid, before_last, half_in, near_end):
        for q in range(CHUNKS):
            form_sources(phase, q, grid)
            send_strips(phase, SOURCE, q, s_ref[q])
            send_block(phase, SOURCE, q, s_ref[q])

        def filter_own(*pieces):
            for q in pieces:
                wait_for(strip_in.at[phase, SOURCE, q], strip_recv.at[phase, q])
                h_ref[phase, q] = filter_cols(phase, SOURCE, q, s_ref[q])
                send_block(phase, FILTERED, q, h_ref[phase, q])
                remote(
                    out_ref.at[phase, FILTERED, q],
                    beside_in.at[phase, q],
                    block_send.at[phase],
                    beside_recv.at[phase, q // 2],
                    beside_me,
                )

        def filter_one_side(pair):
            passed_in(phase, SOURCE, pair)
            for q in (2 * pair, 2 * pair + 1):
                f_ref[q] = from_side(phase, SOURCE, q)
                send_strips(phase, FILTERED, q, f_ref[q])

        def finish(pair, carry):
            pieces = (2 * pair, 2 * pair + 1)
            passed_in(phase, FILTERED, pair)
            both = strip_in.at[phase, FILTERED, pieces[0] : pieces[1] + 1]
            wait_for(both, strip_recv.at[phase, CHUNKS + pair])
            filtered = [filter_cols(phase, FILTERED, q, f_ref[q]) for q in pieces]
            for q, of_one_side in zip(pieces, filtered):
                rest = from_side(
                    phase,
                    FILTERED,
                    q,
                    (
                        ((0, 0), halves(h_ref[phase, q])),
                        ((1, -1), [beside_in[phase, q, r].astype(F32) for r in range(2)]),
                    ),
                )
                t_ref[q] = of_one_side + rest
            return member_sum(pieces, carry)

        filter_own(0, 1)
        if phase == 0:
            pass_on(phase, SOURCE, 0)
            filter_own(2)
            filter_one_side(0)
            filter_own(3)
        else:
            filter_own(2, 3)
            pass_on(phase, SOURCE, 0)
        come_beside(phase)
        before_last()
        pass_on(phase, SOURCE, 1)
        half_in()
        if phase == 1:
            filter_one_side(0)
        filter_one_side(1)

        carry = tuple(jnp.zeros((levels, cols), F32) for _ in range(2))
        if phase == 0:
            for pair in range(PAIRS):
                pass_on(phase, FILTERED, pair)
                carry = finish(pair, carry)
        else:
            for pair in range(PAIRS):
                pass_on(phase, FILTERED, pair)
            carry = finish(0, carry)
            near_end()
            carry = finish(1, carry)
        for x in range(2):
            for h in range(2):
                pmine[phase, h, x] = carry[x][h * half : (h + 1) * half]
        return jnp.concatenate(carry, axis=0)

    def dotted(phase, factor, pieces):
        total = None
        for q in pieces:
            way = course(SOURCE, q)
            here = side_in.at[phase, SOURCE, q]
            own = halves(s_ref[q])
            near = [here[r].astype(F32) * 2.0 for r in range(2)]
            far = [jnp.where(big(way), here[2 + r].astype(F32) * 2.0, 0.0) for r in range(2)]
            mine = weighed([((0, 0), own), ((-2 * way,) * 2, near)])
            value, i = far_row(phase, SOURCE, q)
            mine[i] = mine[i] + value * 2.0
            theirs = weighed(
                [
                    ((-1, 1), own),
                    ((-2 * way - 1, -2 * way + 1), near),
                    ((-3 * way,) * 2, far),
                ]
            )
            field = halves(h_ref[phase, q])
            for i in range(2):
                beside = beside_in[phase, q, i].astype(F32)
                if factor is None:
                    term = mine[i] * field[i] + theirs[i] * beside
                else:
                    term = (mine[i] * factor) * (field[i] * factor) + (theirs[i] * factor) * (
                        beside * factor
                    )
                total = term if total is None else total + term
        return jnp.sum(total, axis=0, keepdims=True)

    def send_increment(phase):
        return remote(
            pmine.at[phase, other], ptheirs.at[phase], p_sem.at[2], p_sem.at[phase], partner
        )

    def folded(vector):
        return (
            sum(vector[:, k * cols : (k + 1) * cols] for k in range(n_obs // cols)) * 0.5
        )

    n_z = n_gx // 2
    hub = core == 1

    def reduce_first(which, rows):
        red1[which, gx, 0:1, :] = rows[0]
        red1[which, gx, 1:2, :] = rows[1]
        mine = red1.at[which, gx]
        sems = red_send.at[which, 0], red_recv.at[which, 0]
        for k in range(1, n_z):
            remote(mine, mine, *sems, {"gx": 2 * lax.rem(gx // 2 + k, n_z) + 1})

        @pl.when(jnp.logical_not(hub))
        def _():
            remote(mine, mine, *sems, {"gx": gx + 1})

    def reduce_second(which):
        @pl.when(hub)
        def _():
            wait_for(red1.at[which, 0 : n_gx - 1], red_recv.at[which, 0])
            red2[which, plane] = jnp.sum(red1[which], axis=0)
            mine = red2.at[which, plane]
            sems = red_send.at[which, 1], red_recv.at[which, 1]
            for k in range(1, n_plane):
                remote(mine, mine, *sems, {**plane_device(k), "gx": gx - 1})
            for k in range(1, n_plane):
                remote(mine, mine, *sems, plane_device(k))
            remote(mine, mine, *sems, {"gx": gx - 1})

    def reduce_last(which):
        @pl.when(hub)
        def _():
            wait_for(red2.at[which, 0 : n_plane - 1], red_recv.at[which, 1])

        @pl.when(jnp.logical_not(hub))
        def _():
            wait_for(red2.at[which, 0:n_plane], red_recv.at[which, 1])

        both = jnp.sum(jnp.sum(red2[which], axis=0), axis=1, keepdims=True)
        return both[0:1], both[1:2]

    def reduce_sent(which):
        @pl.when(hub)
        def _():
            wait_for(count_ref.at[0 : n_z - 1], red_send.at[which, 0])
            wait_for(count_ref.at[0 : 2 * n_plane - 1], red_send.at[which, 1])

        @pl.when(jnp.logical_not(hub))
        def _():
            wait_for(count_ref.at[0:n_z], red_send.at[which, 0])

    def first_half_in():
        product = folded(noise * innovation * innovation) + dotted(0, None, range(CHUNKS))
        reduce_first(0, (folded(innovation * innovation), product))

    grid_b = spread(0, scatter(innovation), lambda: None, first_half_in, lambda: None)
    gsum[ma] = gather(grid_b)
    g_copy = remote(gsum.at[ma], gsum.at[ma], g_sem.at[0], g_sem.at[1], partner)
    send_increment(0)
    reduce_second(0)
    g_copy.wait()
    image = gsum[0] + gsum[1] + noise * innovation

    state = {}

    def before_last():
        norm_now, product = reduce_last(0)
        alpha = norm_now / product
        scaled = alpha * image
        residual = innovation - scaled
        change = folded(scaled * (noise * scaled - 2.0 * image)) + dotted(1, alpha, (0, 1))
        state["step"] = norm_now, product, alpha, residual
        state["sums"] = folded(residual * residual), change

    def half_in():
        norm, change = state["sums"]
        reduce_first(1, (norm, change + dotted(1, state["step"][2], (2, 3))))

    spread(1, scatter(image), before_last, half_in, lambda: reduce_second(1))
    send_increment(1)
    for phase in range(2):
        wait_for(sent_rows, block_send.at[phase])
        wait_for(strip_in.at[phase], strip_send.at[phase])
    reduce_sent(0)
    wait_for(ptheirs.at[0], p_sem.at[0])

    norm_now, product, alpha, residual = state["step"]
    norm_next, change = reduce_last(1)
    product = product + change
    ratio = norm_next / norm_now
    alpha_next = norm_next / (product - ratio * norm_next / alpha)
    weights = alpha * innovation + alpha_next * (residual + ratio * innovation)
    chosen = jnp.where(ma == 0, weights[:, : n_obs // 2], weights[:, n_obs // 2 :])
    w_ref[0:1, :] = chosen[:, :cols]
    w_ref[1:2, :] = chosen[:, cols:]

    wait_for(ptheirs.at[1], p_sem.at[1])
    first_weight = (alpha + alpha_next * (1.0 + ratio))[None]
    second_weight = (alpha * alpha_next)[None]
    inc_ref[...] = first_weight * (pmine[0, ma] + ptheirs[0]) - second_weight * (
        pmine[1, ma] + ptheirs[1]
    )

    wait_for(ptheirs, p_sem.at[2])
    reduce_sent(1)


def shards(n_gx, n_gy, archive, obs_index, obs_value, obs_error):
    members, rows, levels, cols = archive.shape
    half = levels // 2
    n_own = obs_index.shape[0]
    piece = members // CHUNKS
    strip_rows = rows * piece * STRIP // cols
    shape = (n_own // cols, cols)
    dma = pltpu.SemaphoreType.DMA
    vmem = pl.BlockSpec(memory_space=pltpu.VMEM)
    hbm = pl.BlockSpec(memory_space=pltpu.HBM)
    increment, weights = pl.pallas_call(
        functools.partial(kernel, n_gx, n_gy),
        out_shape=(
            pltpu.VMEM((rows, half, cols), F32),
            pltpu.VMEM(shape, F32),
        ),
        in_specs=[hbm, hbm, hbm, hbm],
        out_specs=(vmem, vmem),
        scratch_shapes=[
            pltpu.VMEM((members, rows, levels, cols), BF16),
            pltpu.VMEM(shape, jnp.int32),
            pltpu.VMEM((2, *shape), F32),
            pltpu.VMEM((2, 8, cols), F32),
            pltpu.VMEM((2, rows * levels, cols), F32),
            pltpu.VMEM((rows, piece * 8, cols), F32),
            pltpu.VMEM((CHUNKS, rows * piece, cols), F32),
            pltpu.VMEM((CHUNKS, rows * piece, cols), F32),
            pltpu.VMEM((2, CHUNKS, rows * piece, cols), F32),
            pltpu.VMEM((CHUNKS, rows * piece, cols), F32),
            pltpu.VMEM((2, 2, CHUNKS, rows, piece, cols), BF16),
            pltpu.VMEM((2, 2, CHUNKS, 8, piece, cols), BF16),
            pltpu.VMEM((2, CHUNKS, rows, piece, cols), BF16),
            pltpu.VMEM((15 * CHUNKS, piece, cols), BF16),
            pltpu.VMEM((2, 2, CHUNKS, 2, strip_rows, cols), BF16),
            pltpu.VMEM((2, 2, CHUNKS, 2, strip_rows, cols), BF16),
            pltpu.VMEM((5 * cols, cols), BF16),
            pltpu.VMEM((2, 2, rows, half, cols), F32),
            pltpu.VMEM((2, rows, half, cols), F32),
            pltpu.VMEM((2, 1, 2 * n_own), F32),
            pltpu.VMEM((2, n_gx, 2, cols), F32),
            pltpu.VMEM((2, 2 * n_gy, 2, cols), F32),
            pltpu.VMEM((4 * n_gy, 2, cols), F32),
            dma((LOADS + 2,)),
            dma((2,)),
            dma((2,)),
            dma((2,)),
            dma((2, 2, PAIRS)),
            dma((2, 2, PAIRS)),
            dma((2, PAIRS)),
            dma((2,)),
            dma((2, CHUNKS + PAIRS)),
            dma((3,)),
            dma((2,)),
            dma((2, 2)),
            dma((2, 2)),
        ],
        compiler_params=pltpu.CompilerParams(
            collective_id=0, has_side_effects=True, vmem_limit_bytes=56 * 1024 * 1024
        ),
        name="analysis",
    )(archive, obs_index.reshape(shape), obs_value.reshape(shape), obs_error.reshape(shape))
    return increment, weights.reshape(n_own)


def solution(mesh):
    n_gx, n_gy = mesh.shape["gx"], mesh.shape["gy"]
    own = P(("gx", "gy", "ma"))
    return jax.shard_map(
        functools.partial(shards, n_gx, n_gy),
        mesh=mesh,
        in_specs=(P("ma", "gx", None, "gy"), own, own, own),
        out_specs=(P("gx", "ma", "gy"), own),
        check_vma=False,
    )
```

```python
import functools
import math

import jax
import jax.numpy as jnp
from jax import lax
from jax.experimental import pallas as pl
from jax.experimental.pallas import tpu as pltpu
from jax.sharding import PartitionSpec as P

M = 512
TAPER_X = 4
TAPER_Y = 8
F32 = jnp.float32
BF16 = jnp.bfloat16
MESH = pl.DeviceIdType.MESH

LOADS = 8
CHUNKS = 4
PAIRS = CHUNKS // 2
STRIP = 16
SOURCE, FILTERED = 0, 1


def course(kind, q):
    return (1 if q % 2 == 0 else -1) * (1 if kind == SOURCE else -1)


def row_weight(distance):
    r = abs(distance) / TAPER_X
    if r <= 1.0:
        return (((-0.25 * r + 0.5) * r + 0.625) * r - 5.0 / 3.0) * r * r + 1.0
    if r < 2.0:
        return (
            ((((r / 12.0 - 0.5) * r + 0.625) * r + 5.0 / 3.0) * r - 5.0) * r
            + 4.0
            - 2.0 / (3.0 * r)
        )
    return 0.0


def taper_weight(distance, half_width):
    ratio = jnp.abs(distance) / half_width
    safe = jnp.maximum(ratio, 1.0)
    inner = (((-0.25 * ratio + 0.5) * ratio + 0.625) * ratio - 5.0 / 3.0) * ratio * ratio + 1.0
    outer = (
        ((((ratio / 12.0 - 0.5) * ratio + 0.625) * ratio + 5.0 / 3.0) * ratio - 5.0) * ratio
        + 4.0
        - 2.0 / (3.0 * safe)
    )
    return jnp.where(ratio <= 1.0, inner, jnp.where(ratio < 2.0, outer, 0.0))


def in_three(x):
    first = x.astype(BF16)
    rest = x - first.astype(F32)
    second = rest.astype(BF16)
    third = (rest - second.astype(F32)).astype(BF16)
    return jnp.concatenate([first, second, third], axis=0)


def sum_of_three(y, rows):
    return (y[2 * rows :] + y[rows : 2 * rows]) + y[:rows]


def kernel(
    n_gx,
    n_gy,
    archive_hbm,
    idx_hbm,
    val_hbm,
    err_hbm,
    inc_ref,
    w_ref,
    arch,
    idx_ref,
    pair_ref,
    meta,
    sums,
    average,
    part,
    s_ref,
    f_ref,
    h_ref,
    t_ref,
    out_ref,
    side_in,
    beside_in,
    count_rows,
    strip_out,
    strip_in,
    wcol,
    pmine,
    ptheirs,
    gsum,
    red1,
    red2,
    count_ref,
    load_sem,
    meta_sem,
    sums_sem,
    block_send,
    block_recv,
    fwd_recv,
    beside_recv,
    strip_send,
    strip_recv,
    p_sem,
    g_sem,
    red_send,
    red_recv,
):
    members = arch.shape[0]
    levels = arch.shape[2]
    half = levels // 2
    cols = arch.shape[3]
    piece = members // CHUNKS
    gx = lax.axis_index("gx")
    gy = lax.axis_index("gy")
    ma = lax.axis_index("ma")
    core = lax.rem(gx, 2)
    other = 1 - ma
    sent_rows = count_rows.at[0 : 15 * CHUNKS]
    plane = gy * 2 + ma
    n_plane = n_gy * 2

    def row_block(k):
        return {"gx": lax.rem(gx + (k + n_gx), n_gx)}

    def col_block(k):
        return {"gy": lax.rem(gy + (k + n_gy), n_gy)}

    def plane_device(k):
        at = lax.rem(plane + k, n_plane)
        return {"gy": at // 2, "ma": lax.rem(at, 2)}

    def remote(src, dst, send_sem, recv_sem, device):
        copy = pltpu.make_async_remote_copy(
            src_ref=src,
            dst_ref=dst,
            send_sem=send_sem,
            recv_sem=recv_sem,
            device_id=device,
            device_id_type=MESH,
        )
        copy.start()
        return copy

    def wait_for(ref, sem):
        pltpu.make_async_copy(ref, ref, sem).wait()

    load = members // LOADS
    loads = []
    for k in range(LOADS):
        copy = pltpu.make_async_copy(
            archive_hbm.at[pl.ds(k * load, load)], arch.at[pl.ds(k * load, load)], load_sem.at[k]
        )
        copy.start()
        loads.append(copy)
    pltpu.make_async_copy(idx_hbm, idx_ref, load_sem.at[LOADS]).start()
    pltpu.make_async_copy(val_hbm, pair_ref.at[0], load_sem.at[LOADS + 1]).start()
    pltpu.make_async_copy(err_hbm, pair_ref.at[1], load_sem.at[LOADS + 1]).start()

    barrier = pltpu.get_barrier_semaphore()
    def far_first(count):
        return sorted(range(1, count), key=lambda k: -min(k, count - k))

    for k in far_first(n_gx):
        pl.semaphore_signal(barrier, inc=1, device_id=row_block(k), device_id_type=MESH)
    for k in far_first(n_plane):
        across = {**plane_device(k), **row_block(1 - 2 * core)}
        for device in (plane_device(k), across):
            pl.semaphore_signal(barrier, inc=1, device_id=device, device_id_type=MESH)

    total = tuple(jnp.zeros((levels, cols), F32) for _ in range(2))
    for k in range(LOADS):
        loads[k].wait()

        def add(m, carry):
            return tuple(carry[x] + arch[m, x].astype(F32) for x in range(2))

        total = lax.fori_loop(k * load, (k + 1) * load, add, total, unroll=8)
    for x in range(2):
        sums[ma, x * levels : (x + 1) * levels, :] = total[x]
    wait_for(idx_ref, load_sem.at[LOADS])
    wait_for(pair_ref, load_sem.at[LOADS + 1])
    meta[ma, 0:2, :] = idx_ref[...].astype(F32)
    meta[ma, 2:4, :] = pair_ref[0]
    meta[ma, 4:6, :] = pair_ref[1]
    meta[ma, 6:8, :] = jnp.zeros((2, cols), F32)

    pl.semaphore_wait(barrier, n_gx - 1 + 2 * (n_plane - 1))

    partner = {"ma": other}
    meta_copy = remote(meta.at[ma], meta.at[ma], meta_sem.at[0], meta_sem.at[1], partner)
    sums_copy = remote(sums.at[ma], sums.at[ma], sums_sem.at[0], sums_sem.at[1], partner)

    source = lax.broadcasted_iota(jnp.int32, (cols, cols), 0)
    target = lax.broadcasted_iota(jnp.int32, (cols, cols), 1)

    def col_weight(shift):
        return taper_weight((source - target + shift).astype(F32), float(TAPER_Y))

    beside = jnp.where(gy > 0, col_weight(-cols), 0.0) + jnp.where(
        gy < n_gy - 1, col_weight(cols), 0.0
    )
    for k, weight in enumerate((col_weight(0), beside)):
        high = weight.astype(BF16)
        low = (weight - high.astype(F32)).astype(BF16)
        wcol[2 * k * cols : (2 * k + 1) * cols, :] = high
        wcol[(2 * k + 1) * cols : (2 * k + 2) * cols, :] = low
        if k == 0:
            wcol[4 * cols : 5 * cols, :] = high

    meta_copy.wait()

    def in_a_row(first):
        rows = [meta[h, first + i : first + i + 1, :] for h in range(2) for i in range(2)]
        return jnp.concatenate(rows, axis=1)

    index = in_a_row(0).astype(jnp.int32)
    target_value = in_a_row(2)
    noise = in_a_row(4)
    n_obs = index.shape[1]
    owner = lax.broadcasted_iota(jnp.int32, (1, n_obs), 1) // (n_obs // 2)
    obs_line = (index >> 11) * levels + owner * half + ((index >> 7) & (half - 1))
    obs_col = index & (cols - 1)
    line_hot = (
        lax.broadcasted_iota(jnp.int32, (2 * levels, n_obs), 0) == obs_line
    ).astype(F32)
    col_hot = (
        (lax.broadcasted_iota(jnp.int32, (cols, n_obs), 0) == obs_col).astype(F32).astype(BF16)
    )

    def gather(grid):
        rows = 2 * levels
        spread = jnp.dot(in_three(grid), col_hot, preferred_element_type=F32)
        return jnp.sum(sum_of_three(spread, rows) * line_hot, axis=0, keepdims=True)

    def scatter(vector):
        rows = 2 * levels
        spread = lax.dot_general(
            in_three(line_hot * vector),
            col_hot,
            (((1,), (1,)), ((), ())),
            preferred_element_type=F32,
        )
        return sum_of_three(spread, rows)

    values = scatter(target_value)
    counts = lax.dot_general(
        line_hot.astype(BF16), col_hot, (((1,), (1,)), ((), ())), preferred_element_type=F32
    )
    sums_copy.wait()
    average[...] = (sums[0] + sums[1]) * (1.0 / M)
    scale = 1.0 / math.sqrt(M - 1.0)

    beside_me = row_block(1 - 2 * core)

    def big(way):
        return core == (1 if way > 0 else 0)

    def send_block(phase, kind, q, field):
        way = course(kind, q)
        row = 1 if way > 0 else 0
        for x in range(2):
            out_ref[phase, kind, q, x] = field[x * piece : (x + 1) * piece].astype(BF16)
        block = out_ref.at[phase, kind, q]
        here = side_in.at[phase, kind, q]
        sems = block_send.at[phase], block_recv.at[phase, kind, q // 2]

        @pl.when(big(way))
        def _():
            remote(block, here.at[2:4], *sems, row_block(4 * way))

        @pl.when(jnp.logical_not(big(way)))
        def _():
            remote(block.at[row], here.at[2], *sems, row_block(4 * way))

        remote(block, here.at[0:2], *sems, row_block(2 * way))

    def pass_on(phase, kind, pair):
        wait_for(count_rows.at[0:7], block_recv.at[phase, kind, pair])
        sems = block_send.at[phase], fwd_recv.at[phase, kind, pair]
        for q in (2 * pair, 2 * pair + 1):
            way = course(kind, q)
            here = side_in.at[phase, kind, q]

            @pl.when(big(way))
            def _(here=here):
                remote(here.at[0:4], here.at[4:8], *sems, beside_me)

            @pl.when(jnp.logical_not(big(way)))
            def _(here=here):
                remote(here.at[0:2], here.at[4:6], *sems, beside_me)

    def passed_in(phase, kind, pair):
        wait_for(count_rows.at[0:6], fwd_recv.at[phase, kind, pair])

    def come_beside(phase):
        for pair in range(PAIRS):
            both = beside_in.at[phase, 2 * pair : 2 * pair + 2]
            wait_for(both, beside_recv.at[phase, pair])

    def weight(k, r, i):
        both = [row_weight(2 * at + r - i) for at in k]
        return both[0] if both[0] == both[1] else jnp.where(core == 0, both[0], both[1])

    def weighed(terms):
        outs = [None, None]
        for k, rows in terms:
            for r in range(2):
                for i in range(2):
                    if any(row_weight(2 * at + r - i) for at in k):
                        term = rows[r] * weight(k, r, i)
                        outs[i] = term if outs[i] is None else outs[i] + term
        return outs

    def halves(field):
        return [field[:piece], field[piece:]]

    def far_row(phase, kind, q):
        way = course(kind, q)
        at = 2 + jnp.where(big(way), 1 if way > 0 else 0, 0)
        value = side_in[phase, kind, q, at].astype(F32) * row_weight(7)
        return value, 0 if way > 0 else 1

    def from_side(phase, kind, q, extra=()):
        way = course(kind, q)
        here = side_in.at[phase, kind, q]
        rows = [here[k].astype(F32) for k in (0, 1, 4, 5)]
        rows += [jnp.where(big(way), 0.0, here[k].astype(F32)) for k in (6, 7)]
        outs = weighed(
            [
                ((-2 * way,) * 2, rows[0:2]),
                ((1 - 2 * way, -1 - 2 * way), rows[2:4]),
                ((-3 * way,) * 2, rows[4:6]),
                *extra,
            ]
        )
        value, i = far_row(phase, kind, q)
        outs[i] = outs[i] + value
        return jnp.concatenate(outs, axis=0)

    strip_rows = 2 * piece * STRIP // cols
    lane = lax.broadcasted_iota(jnp.int32, (strip_rows, cols), 1)

    def send_strips(phase, kind, q, field):
        last = first = jnp.zeros((strip_rows, cols), F32)
        for j in range(cols // STRIP):
            group = field[j * strip_rows : (j + 1) * strip_rows]
            mine = lane // STRIP == j
            last = jnp.where(mine, pltpu.roll(group, ((j + 1) * STRIP) % cols, 1), last)
            first = jnp.where(mine, pltpu.roll(group, j * STRIP, 1), first)
        for side, strip in enumerate((last, first)):
            strip_out[phase, kind, q, side] = strip.astype(BF16)
            remote(
                strip_out.at[phase, kind, q, side],
                strip_in.at[phase, kind, q, side],
                strip_send.at[phase],
                strip_recv.at[phase, q if kind == SOURCE else CHUNKS + q // 2],
                col_block(1 - 2 * side),
            )

    def filter_cols(phase, kind, q, field):
        left = strip_in[phase, kind, q, 0].astype(F32)
        right = strip_in[phase, kind, q, 1].astype(F32)
        strips = []
        for j in range(cols // STRIP):
            strips.append(
                jnp.where(
                    lane < cols // 2,
                    pltpu.roll(right, (cols - j * STRIP) % cols, 1),
                    pltpu.roll(left, cols - (j + 1) * STRIP, 1),
                )
            )
        strips = jnp.concatenate(strips, axis=0).astype(BF16)
        high = field.astype(BF16)
        low = (field - high.astype(F32)).astype(BF16)
        return jnp.dot(
            jnp.concatenate([high, high, strips, strips, low], axis=1),
            wcol[...],
            preferred_element_type=F32,
        )

    def form_sources(phase, q, grid):
        value = [grid[x * levels : (x + 1) * levels] for x in range(2)]

        def one(i, carry):
            m = q * piece + i
            for x in range(2):
                if phase == 0:
                    anomaly = ((arch[m, x].astype(F32) - average[x * levels : (x + 1) * levels, :]) * scale).astype(BF16)
                    arch[m, x] = anomaly
                else:
                    anomaly = arch[m, x]
                product = anomaly.astype(F32) * value[x]
                part[x, pl.ds(pl.multiple_of(i * 8, 8), 8), :] = (
                    product[0:8] + product[8:16]
                ) + (product[16:24] + product[24:32])
            return carry

        lax.fori_loop(0, piece, one, 0, unroll=8)
        for x in range(2):
            for g in range(piece // 8):
                rows = [part[x, pl.ds(g * 64 + k, 8, stride=8), :] for k in range(8)]
                s_ref[q, x * piece + g * 8 : x * piece + g * 8 + 8, :] = (
                    (rows[0] + rows[1]) + (rows[2] + rows[3])
                ) + ((rows[4] + rows[5]) + (rows[6] + rows[7]))

    def member_sum(pieces, carry):
        def one(i, carry):
            for q in pieces:
                carry = tuple(
                    carry[x]
                    + arch[q * piece + i, x].astype(F32) * t_ref[q, pl.ds(x * piece + i, 1), :]
                    for x in range(2)
                )
            return carry

        return lax.fori_loop(0, piece, one, carry, unroll=8)

    def spread(phase, grid, before_last, half_in, near_end):
        for q in range(CHUNKS):
            form_sources(phase, q, grid)
            if phase == 0:
                send_strips(phase, SOURCE, q, s_ref[q])
            send_block(phase, SOURCE, q, s_ref[q])
            if phase == 1:
                send_strips(phase, SOURCE, q, s_ref[q])

        def filter_own(*pieces):
            for q in pieces:
                wait_for(strip_in.at[phase, SOURCE, q], strip_recv.at[phase, q])
                h_ref[phase, q] = filter_cols(phase, SOURCE, q, s_ref[q])
                send_block(phase, FILTERED, q, h_ref[phase, q])
                remote(
                    out_ref.at[phase, FILTERED, q],
                    beside_in.at[phase, q],
                    block_send.at[phase],
                    beside_recv.at[phase, q // 2],
                    beside_me,
                )

        def filter_one_side(pair):
            passed_in(phase, SOURCE, pair)
            for q in (2 * pair, 2 * pair + 1):
                f_ref[q] = from_side(phase, SOURCE, q)
                send_strips(phase, FILTERED, q, f_ref[q])

        def finish(pair, carry):
            pieces = (2 * pair, 2 * pair + 1)
            both = strip_in.at[phase, FILTERED, pieces[0] : pieces[1] + 1]
            wait_for(both, strip_recv.at[phase, CHUNKS + pair])
            for q in pieces:
                t_ref[q] = filter_cols(phase, FILTERED, q, f_ref[q])
            passed_in(phase, FILTERED, pair)
            for q in pieces:
                rest = from_side(
                    phase,
                    FILTERED,
                    q,
                    (
                        ((0, 0), halves(h_ref[phase, q])),
                        ((1, -1), [beside_in[phase, q, r].astype(F32) for r in range(2)]),
                    ),
                )
                t_ref[q] = t_ref[q] + rest
            return member_sum(pieces, carry)

        last = PAIRS - 1
        filter_own(0, 1)
        if phase == 0:
            for pair in range(last):
                pass_on(phase, SOURCE, pair)
                filter_own(2 * pair + 2)
                filter_one_side(pair)
                filter_own(2 * pair + 3)
        else:
            filter_own(*range(2, CHUNKS))
            for pair in range(last):
                pass_on(phase, SOURCE, pair)
        come_beside(phase)
        before_last()
        pass_on(phase, SOURCE, last)
        half_in()
        if phase == 1:
            for pair in range(last):
                filter_one_side(pair)
        filter_one_side(last)

        carry = tuple(jnp.zeros((levels, cols), F32) for _ in range(2))
        if phase == 0:
            for pair in range(PAIRS):
                pass_on(phase, FILTERED, pair)
                carry = finish(pair, carry)
        else:
            for pair in range(PAIRS):
                pass_on(phase, FILTERED, pair)
            for pair in range(PAIRS):
                if pair == PAIRS // 2:
                    near_end()
                carry = finish(pair, carry)
        for x in range(2):
            for h in range(2):
                pmine[phase, h, x] = carry[x][h * half : (h + 1) * half]
        return jnp.concatenate(carry, axis=0)

    def dotted(phase, factor, pieces):
        total = None
        for q in pieces:
            way = course(SOURCE, q)
            here = side_in.at[phase, SOURCE, q]
            own = halves(s_ref[q])
            near = [here[r].astype(F32) * 2.0 for r in range(2)]
            far = [jnp.where(big(way), here[2 + r].astype(F32) * 2.0, 0.0) for r in range(2)]
            mine = weighed([((0, 0), own), ((-2 * way,) * 2, near)])
            value, i = far_row(phase, SOURCE, q)
            mine[i] = mine[i] + value * 2.0
            theirs = weighed(
                [
                    ((-1, 1), own),
                    ((-2 * way - 1, -2 * way + 1), near),
                    ((-3 * way,) * 2, far),
                ]
            )
            field = halves(h_ref[phase, q])
            for i in range(2):
                beside = beside_in[phase, q, i].astype(F32)
                if factor is None:
                    term = mine[i] * field[i] + theirs[i] * beside
                else:
                    term = (mine[i] * factor) * (field[i] * factor) + (theirs[i] * factor) * (
                        beside * factor
                    )
                total = term if total is None else total + term
        return jnp.sum(total, axis=0, keepdims=True)

    def send_increment(phase):
        return remote(
            pmine.at[phase, other], ptheirs.at[phase], p_sem.at[2], p_sem.at[phase], partner
        )

    def folded(vector):
        return (
            sum(vector[:, k * cols : (k + 1) * cols] for k in range(n_obs // cols)) * 0.5
        )

    n_z = n_gx // 2
    hub = core == 1

    def reduce_first(which, rows):
        red1[which, gx, 0:1, :] = rows[0]
        red1[which, gx, 1:2, :] = rows[1]
        mine = red1.at[which, gx]
        sems = red_send.at[which, 0], red_recv.at[which, 0]
        for k in range(1, n_z):
            remote(mine, mine, *sems, {"gx": 2 * lax.rem(gx // 2 + k, n_z) + 1})

        @pl.when(jnp.logical_not(hub))
        def _():
            remote(mine, mine, *sems, {"gx": gx + 1})

    def reduce_second(which):
        @pl.when(hub)
        def _():
            wait_for(red1.at[which, 0 : n_gx - 1], red_recv.at[which, 0])
            red2[which, plane] = jnp.sum(red1[which], axis=0)
            mine = red2.at[which, plane]
            sems = red_send.at[which, 1], red_recv.at[which, 1]
            for k in range(1, n_plane):
                remote(mine, mine, *sems, {**plane_device(k), "gx": gx - 1})
            for k in range(1, n_plane):
                remote(mine, mine, *sems, plane_device(k))
            remote(mine, mine, *sems, {"gx": gx - 1})

    def reduce_last(which):
        @pl.when(hub)
        def _():
            wait_for(red2.at[which, 0 : n_plane - 1], red_recv.at[which, 1])

        @pl.when(jnp.logical_not(hub))
        def _():
            wait_for(red2.at[which, 0:n_plane], red_recv.at[which, 1])

        both = jnp.sum(jnp.sum(red2[which], axis=0), axis=1, keepdims=True)
        return both[0:1], both[1:2]

    def reduce_sent(which):
        @pl.when(hub)
        def _():
            wait_for(count_ref.at[0 : n_z - 1], red_send.at[which, 0])
            wait_for(count_ref.at[0 : 2 * n_plane - 1], red_send.at[which, 1])

        @pl.when(jnp.logical_not(hub))
        def _():
            wait_for(count_ref.at[0:n_z], red_send.at[which, 0])

    state = {}

    def first_half_in():
        innovation = target_value - gather(average[...])
        product = folded(noise * innovation * innovation) + dotted(0, None, range(CHUNKS))
        reduce_first(0, (folded(innovation * innovation), product))
        state["innovation"] = innovation

    grid_b = spread(
        0, values - counts * average[...], lambda: None, first_half_in, lambda: None
    )
    innovation = state["innovation"]
    gsum[ma] = gather(grid_b)
    g_copy = remote(gsum.at[ma], gsum.at[ma], g_sem.at[0], g_sem.at[1], partner)
    send_increment(0)
    reduce_second(0)
    g_copy.wait()
    image = gsum[0] + gsum[1] + noise * innovation

    def before_last():
        norm_now, product = reduce_last(0)
        alpha = norm_now / product
        scaled = alpha * image
        residual = innovation - scaled
        change = folded(scaled * (noise * scaled - 2.0 * image)) + dotted(1, alpha, range(CHUNKS - 2))
        state["step"] = norm_now, product, alpha, residual
        state["sums"] = folded(residual * residual), change

    def half_in():
        norm, change = state["sums"]
        reduce_first(1, (norm, change + dotted(1, state["step"][2], range(CHUNKS - 2, CHUNKS))))

    spread(1, scatter(image), before_last, half_in, lambda: reduce_second(1))
    send_increment(1)
    for phase in range(2):
        wait_for(sent_rows, block_send.at[phase])
        wait_for(strip_in.at[phase], strip_send.at[phase])
    reduce_sent(0)
    wait_for(ptheirs.at[0], p_sem.at[0])

    norm_now, product, alpha, residual = state["step"]
    norm_next, change = reduce_last(1)
    product = product + change
    ratio = norm_next / norm_now
    alpha_next = norm_next / (product - ratio * norm_next / alpha)
    weights = alpha * innovation + alpha_next * (residual + ratio * innovation)
    chosen = jnp.where(ma == 0, weights[:, : n_obs // 2], weights[:, n_obs // 2 :])
    w_ref[0:1, :] = chosen[:, :cols]
    w_ref[1:2, :] = chosen[:, cols:]

    wait_for(ptheirs.at[1], p_sem.at[1])
    first_weight = (alpha + alpha_next * (1.0 + ratio))[None]
    second_weight = (alpha * alpha_next)[None]
    inc_ref[...] = first_weight * (pmine[0, ma] + ptheirs[0]) - second_weight * (
        pmine[1, ma] + ptheirs[1]
    )

    wait_for(ptheirs, p_sem.at[2])
    reduce_sent(1)


def shards(n_gx, n_gy, archive, obs_index, obs_value, obs_error):
    members, rows, levels, cols = archive.shape
    half = levels // 2
    n_own = obs_index.shape[0]
    piece = members // CHUNKS
    strip_rows = rows * piece * STRIP // cols
    shape = (n_own // cols, cols)
    dma = pltpu.SemaphoreType.DMA
    vmem = pl.BlockSpec(memory_space=pltpu.VMEM)
    hbm = pl.BlockSpec(memory_space=pltpu.HBM)
    increment, weights = pl.pallas_call(
        functools.partial(kernel, n_gx, n_gy),
        out_shape=(
            pltpu.VMEM((rows, half, cols), F32),
            pltpu.VMEM(shape, F32),
        ),
        in_specs=[hbm, hbm, hbm, hbm],
        out_specs=(vmem, vmem),
        scratch_shapes=[
            pltpu.VMEM((members, rows, levels, cols), BF16),
            pltpu.VMEM(shape, jnp.int32),
            pltpu.VMEM((2, *shape), F32),
            pltpu.VMEM((2, 8, cols), F32),
            pltpu.VMEM((2, rows * levels, cols), F32),
            pltpu.VMEM((rows * levels, cols), F32),
            pltpu.VMEM((rows, piece * 8, cols), F32),
            pltpu.VMEM((CHUNKS, rows * piece, cols), F32),
            pltpu.VMEM((CHUNKS, rows * piece, cols), F32),
            pltpu.VMEM((2, CHUNKS, rows * piece, cols), F32),
            pltpu.VMEM((CHUNKS, rows * piece, cols), F32),
            pltpu.VMEM((2, 2, CHUNKS, rows, piece, cols), BF16),
            pltpu.VMEM((2, 2, CHUNKS, 8, piece, cols), BF16),
            pltpu.VMEM((2, CHUNKS, rows, piece, cols), BF16),
            pltpu.VMEM((15 * CHUNKS, piece, cols), BF16),
            pltpu.VMEM((2, 2, CHUNKS, 2, strip_rows, cols), BF16),
            pltpu.VMEM((2, 2, CHUNKS, 2, strip_rows, cols), BF16),
            pltpu.VMEM((5 * cols, cols), BF16),
            pltpu.VMEM((2, 2, rows, half, cols), F32),
            pltpu.VMEM((2, rows, half, cols), F32),
            pltpu.VMEM((2, 1, 2 * n_own), F32),
            pltpu.VMEM((2, n_gx, 2, cols), F32),
            pltpu.VMEM((2, 2 * n_gy, 2, cols), F32),
            pltpu.VMEM((4 * n_gy, 2, cols), F32),
            dma((LOADS + 2,)),
            dma((2,)),
            dma((2,)),
            dma((2,)),
            dma((2, 2, PAIRS)),
            dma((2, 2, PAIRS)),
            dma((2, PAIRS)),
            dma((2,)),
            dma((2, CHUNKS + PAIRS)),
            dma((3,)),
            dma((2,)),
            dma((2, 2)),
            dma((2, 2)),
        ],
        compiler_params=pltpu.CompilerParams(
            collective_id=0, has_side_effects=True, vmem_limit_bytes=56 * 1024 * 1024
        ),
        name="analysis",
    )(archive, obs_index.reshape(shape), obs_value.reshape(shape), obs_error.reshape(shape))
    return increment, weights.reshape(n_own)


def solution(mesh):
    n_gx, n_gy = mesh.shape["gx"], mesh.shape["gy"]
    own = P(("gx", "gy", "ma"))
    return jax.shard_map(
        functools.partial(shards, n_gx, n_gy),
        mesh=mesh,
        in_specs=(P("ma", "gx", None, "gy"), own, own, own),
        out_specs=(P("gx", "ma", "gy"), own),
        check_vma=False,
    )
```

```python
import functools
import math

import jax
import jax.numpy as jnp
from jax import lax
from jax.experimental import pallas as pl
from jax.experimental.pallas import tpu as pltpu
from jax.sharding import PartitionSpec as P

M = 512
TAPER_X = 4
TAPER_Y = 8
F32 = jnp.float32
BF16 = jnp.bfloat16
MESH = pl.DeviceIdType.MESH

LOADS = 8
CHUNKS = 4
PAIRS = CHUNKS // 2
STRIP = 16
SOURCE, FILTERED = 0, 1


def course(kind, q):
    return (1 if q % 2 == 0 else -1) * (1 if kind == SOURCE else -1)


def row_weight(distance):
    r = abs(distance) / TAPER_X
    if r <= 1.0:
        return (((-0.25 * r + 0.5) * r + 0.625) * r - 5.0 / 3.0) * r * r + 1.0
    if r < 2.0:
        return (
            ((((r / 12.0 - 0.5) * r + 0.625) * r + 5.0 / 3.0) * r - 5.0) * r
            + 4.0
            - 2.0 / (3.0 * r)
        )
    return 0.0


def taper_weight(distance, half_width):
    ratio = jnp.abs(distance) / half_width
    safe = jnp.maximum(ratio, 1.0)
    inner = (((-0.25 * ratio + 0.5) * ratio + 0.625) * ratio - 5.0 / 3.0) * ratio * ratio + 1.0
    outer = (
        ((((ratio / 12.0 - 0.5) * ratio + 0.625) * ratio + 5.0 / 3.0) * ratio - 5.0) * ratio
        + 4.0
        - 2.0 / (3.0 * safe)
    )
    return jnp.where(ratio <= 1.0, inner, jnp.where(ratio < 2.0, outer, 0.0))


def in_three(x):
    first = x.astype(BF16)
    rest = x - first.astype(F32)
    second = rest.astype(BF16)
    third = (rest - second.astype(F32)).astype(BF16)
    return jnp.concatenate([first, second, third], axis=0)


def sum_of_three(y, rows):
    return (y[2 * rows :] + y[rows : 2 * rows]) + y[:rows]


def kernel(
    n_gx,
    n_gy,
    archive_hbm,
    idx_hbm,
    val_hbm,
    err_hbm,
    inc_ref,
    w_ref,
    arch,
    idx_ref,
    pair_ref,
    meta,
    sums,
    average,
    part,
    s_ref,
    f_ref,
    h_ref,
    t_ref,
    out_ref,
    side_in,
    beside_in,
    count_rows,
    strip_out,
    strip_in,
    wcol,
    pmine,
    ptheirs,
    gsum,
    red1,
    red2,
    count_ref,
    load_sem,
    meta_sem,
    sums_sem,
    block_send,
    block_recv,
    fwd_recv,
    beside_recv,
    strip_send,
    strip_recv,
    p_sem,
    g_sem,
    red_send,
    red_recv,
):
    members = arch.shape[0]
    levels = arch.shape[2]
    half = levels // 2
    cols = arch.shape[3]
    piece = members // CHUNKS
    gx = lax.axis_index("gx")
    gy = lax.axis_index("gy")
    ma = lax.axis_index("ma")
    core = lax.rem(gx, 2)
    other = 1 - ma
    sent_rows = count_rows.at[0 : 15 * CHUNKS]
    plane = gy * 2 + ma
    n_plane = n_gy * 2

    def row_block(k):
        return {"gx": lax.rem(gx + (k + n_gx), n_gx)}

    def col_block(k):
        return {"gy": lax.rem(gy + (k + n_gy), n_gy)}

    def plane_device(k):
        at = lax.rem(plane + k, n_plane)
        return {"gy": at // 2, "ma": lax.rem(at, 2)}

    def remote(src, dst, send_sem, recv_sem, device):
        copy = pltpu.make_async_remote_copy(
            src_ref=src,
            dst_ref=dst,
            send_sem=send_sem,
            recv_sem=recv_sem,
            device_id=device,
            device_id_type=MESH,
        )
        copy.start()
        return copy

    def wait_for(ref, sem):
        pltpu.make_async_copy(ref, ref, sem).wait()

    load = members // LOADS
    loads = []
    for k in range(LOADS):
        copy = pltpu.make_async_copy(
            archive_hbm.at[pl.ds(k * load, load)], arch.at[pl.ds(k * load, load)], load_sem.at[k]
        )
        copy.start()
        loads.append(copy)
    pltpu.make_async_copy(idx_hbm, idx_ref, load_sem.at[LOADS]).start()
    pltpu.make_async_copy(val_hbm, pair_ref.at[0], load_sem.at[LOADS + 1]).start()
    pltpu.make_async_copy(err_hbm, pair_ref.at[1], load_sem.at[LOADS + 1]).start()

    barrier = pltpu.get_barrier_semaphore()
    def far_first(count):
        return sorted(range(1, count), key=lambda k: -min(k, count - k))

    greeted = [row_block(k) for k in far_first(n_gx) if min(k, n_gx - k) <= 4]
    greeted += [col_block(k) for k in (2, -2, 1, -1)] + [{"ma": other}]
    for device in greeted:
        pl.semaphore_signal(barrier, inc=1, device_id=device, device_id_type=MESH)

    total = tuple(jnp.zeros((levels, cols), F32) for _ in range(2))
    for k in range(LOADS):
        loads[k].wait()

        def add(m, carry):
            return tuple(carry[x] + arch[m, x].astype(F32) for x in range(2))

        total = lax.fori_loop(k * load, (k + 1) * load, add, total, unroll=8)
    for x in range(2):
        sums[ma, x * levels : (x + 1) * levels, :] = total[x]
    wait_for(idx_ref, load_sem.at[LOADS])
    wait_for(pair_ref, load_sem.at[LOADS + 1])
    meta[ma, 0:2, :] = idx_ref[...].astype(F32)
    meta[ma, 2:4, :] = pair_ref[0]
    meta[ma, 4:6, :] = pair_ref[1]
    meta[ma, 6:8, :] = jnp.zeros((2, cols), F32)

    pl.semaphore_wait(barrier, len(greeted))

    partner = {"ma": other}
    meta_copy = remote(meta.at[ma], meta.at[ma], meta_sem.at[0], meta_sem.at[1], partner)
    sums_copy = remote(sums.at[ma], sums.at[ma], sums_sem.at[0], sums_sem.at[1], partner)

    source = lax.broadcasted_iota(jnp.int32, (cols, cols), 0)
    target = lax.broadcasted_iota(jnp.int32, (cols, cols), 1)

    def col_weight(shift):
        return taper_weight((source - target + shift).astype(F32), float(TAPER_Y))

    beside = jnp.where(gy > 0, col_weight(-cols), 0.0) + jnp.where(
        gy < n_gy - 1, col_weight(cols), 0.0
    )
    for k, weight in enumerate((col_weight(0), beside)):
        high = weight.astype(BF16)
        low = (weight - high.astype(F32)).astype(BF16)
        wcol[2 * k * cols : (2 * k + 1) * cols, :] = high
        wcol[(2 * k + 1) * cols : (2 * k + 2) * cols, :] = low
        if k == 0:
            wcol[4 * cols : 5 * cols, :] = high

    meta_copy.wait()

    def in_a_row(first):
        rows = [meta[h, first + i : first + i + 1, :] for h in range(2) for i in range(2)]
        return jnp.concatenate(rows, axis=1)

    index = in_a_row(0).astype(jnp.int32)
    target_value = in_a_row(2)
    noise = in_a_row(4)
    n_obs = index.shape[1]
    owner = lax.broadcasted_iota(jnp.int32, (1, n_obs), 1) // (n_obs // 2)
    obs_line = (index >> 11) * levels + owner * half + ((index >> 7) & (half - 1))
    obs_col = index & (cols - 1)
    line_hot = (
        lax.broadcasted_iota(jnp.int32, (2 * levels, n_obs), 0) == obs_line
    ).astype(F32)
    col_hot = (
        (lax.broadcasted_iota(jnp.int32, (cols, n_obs), 0) == obs_col).astype(F32).astype(BF16)
    )

    def gather(grid):
        rows = 2 * levels
        spread = jnp.dot(in_three(grid), col_hot, preferred_element_type=F32)
        return jnp.sum(sum_of_three(spread, rows) * line_hot, axis=0, keepdims=True)

    def scatter(vector):
        rows = 2 * levels
        spread = lax.dot_general(
            in_three(line_hot * vector),
            col_hot,
            (((1,), (1,)), ((), ())),
            preferred_element_type=F32,
        )
        return sum_of_three(spread, rows)

    values = scatter(target_value)
    counts = lax.dot_general(
        line_hot.astype(BF16), col_hot, (((1,), (1,)), ((), ())), preferred_element_type=F32
    )
    sums_copy.wait()
    average[...] = (sums[0] + sums[1]) * (1.0 / M)
    scale = 1.0 / math.sqrt(M - 1.0)

    beside_me = row_block(1 - 2 * core)

    def big(way):
        return core == (1 if way > 0 else 0)

    def send_block(phase, kind, q, field):
        way = course(kind, q)
        row = 1 if way > 0 else 0
        for x in range(2):
            out_ref[phase, kind, q, x] = field[x * piece : (x + 1) * piece].astype(BF16)
        block = out_ref.at[phase, kind, q]
        here = side_in.at[phase, kind, q]
        sems = block_send.at[phase], block_recv.at[phase, kind, q // 2]

        @pl.when(big(way))
        def _():
            remote(block, here.at[2:4], *sems, row_block(4 * way))

        @pl.when(jnp.logical_not(big(way)))
        def _():
            remote(block.at[row], here.at[2], *sems, row_block(4 * way))

        remote(block, here.at[0:2], *sems, row_block(2 * way))

    def pass_on(phase, kind, pair):
        wait_for(count_rows.at[0:7], block_recv.at[phase, kind, pair])
        sems = block_send.at[phase], fwd_recv.at[phase, kind, pair]
        for q in (2 * pair, 2 * pair + 1):
            way = course(kind, q)
            here = side_in.at[phase, kind, q]

            @pl.when(big(way))
            def _(here=here):
                remote(here.at[0:4], here.at[4:8], *sems, beside_me)

            @pl.when(jnp.logical_not(big(way)))
            def _(here=here):
                remote(here.at[0:2], here.at[4:6], *sems, beside_me)

    def passed_in(phase, kind, pair):
        wait_for(count_rows.at[0:6], fwd_recv.at[phase, kind, pair])

    def come_beside(phase):
        for pair in range(PAIRS):
            both = beside_in.at[phase, 2 * pair : 2 * pair + 2]
            wait_for(both, beside_recv.at[phase, pair])

    def weight(k, r, i):
        both = [row_weight(2 * at + r - i) for at in k]
        return both[0] if both[0] == both[1] else jnp.where(core == 0, both[0], both[1])

    def weighed(terms):
        outs = [None, None]
        for k, rows in terms:
            for r in range(2):
                for i in range(2):
                    if any(row_weight(2 * at + r - i) for at in k):
                        term = rows[r] * weight(k, r, i)
                        outs[i] = term if outs[i] is None else outs[i] + term
        return outs

    def halves(field):
        return [field[:piece], field[piece:]]

    def far_row(phase, kind, q):
        way = course(kind, q)
        at = 2 + jnp.where(big(way), 1 if way > 0 else 0, 0)
        value = side_in[phase, kind, q, at].astype(F32) * row_weight(7)
        return value, 0 if way > 0 else 1

    def from_side(phase, kind, q, extra=()):
        way = course(kind, q)
        here = side_in.at[phase, kind, q]
        rows = [here[k].astype(F32) for k in (0, 1, 4, 5)]
        rows += [jnp.where(big(way), 0.0, here[k].astype(F32)) for k in (6, 7)]
        outs = weighed(
            [
                ((-2 * way,) * 2, rows[0:2]),
                ((1 - 2 * way, -1 - 2 * way), rows[2:4]),
                ((-3 * way,) * 2, rows[4:6]),
                *extra,
            ]
        )
        value, i = far_row(phase, kind, q)
        outs[i] = outs[i] + value
        return jnp.concatenate(outs, axis=0)

    strip_rows = 2 * piece * STRIP // cols
    lane = lax.broadcasted_iota(jnp.int32, (strip_rows, cols), 1)

    def send_strips(phase, kind, q, field):
        last = first = jnp.zeros((strip_rows, cols), F32)
        for j in range(cols // STRIP):
            group = field[j * strip_rows : (j + 1) * strip_rows]
            mine = lane // STRIP == j
            last = jnp.where(mine, pltpu.roll(group, ((j + 1) * STRIP) % cols, 1), last)
            first = jnp.where(mine, pltpu.roll(group, j * STRIP, 1), first)
        for side, strip in enumerate((last, first)):
            strip_out[phase, kind, q, side] = strip.astype(BF16)
            remote(
                strip_out.at[phase, kind, q, side],
                strip_in.at[phase, kind, q, side],
                strip_send.at[phase],
                strip_recv.at[phase, q if kind == SOURCE else CHUNKS + q // 2],
                col_block(1 - 2 * side),
            )

    def filter_cols(phase, kind, q, field):
        left = strip_in[phase, kind, q, 0].astype(F32)
        right = strip_in[phase, kind, q, 1].astype(F32)
        strips = []
        for j in range(cols // STRIP):
            strips.append(
                jnp.where(
                    lane < cols // 2,
                    pltpu.roll(right, (cols - j * STRIP) % cols, 1),
                    pltpu.roll(left, cols - (j + 1) * STRIP, 1),
                )
            )
        strips = jnp.concatenate(strips, axis=0).astype(BF16)
        high = field.astype(BF16)
        low = (field - high.astype(F32)).astype(BF16)
        return jnp.dot(
            jnp.concatenate([high, high, strips, strips, low], axis=1),
            wcol[...],
            preferred_element_type=F32,
        )

    def form_sources(phase, q, grid):
        value = [grid[x * levels : (x + 1) * levels] for x in range(2)]

        def one(i, carry):
            m = q * piece + i
            for x in range(2):
                if phase == 0:
                    anomaly = ((arch[m, x].astype(F32) - average[x * levels : (x + 1) * levels, :]) * scale).astype(BF16)
                    arch[m, x] = anomaly
                else:
                    anomaly = arch[m, x]
                product = anomaly.astype(F32) * value[x]
                part[x, pl.ds(pl.multiple_of(i * 8, 8), 8), :] = (
                    product[0:8] + product[8:16]
                ) + (product[16:24] + product[24:32])
            return carry

        lax.fori_loop(0, piece, one, 0, unroll=8)
        for x in range(2):
            for g in range(piece // 8):
                rows = [part[x, pl.ds(g * 64 + k, 8, stride=8), :] for k in range(8)]
                s_ref[q, x * piece + g * 8 : x * piece + g * 8 + 8, :] = (
                    (rows[0] + rows[1]) + (rows[2] + rows[3])
                ) + ((rows[4] + rows[5]) + (rows[6] + rows[7]))

    def member_sum(pieces, carry):
        def one(i, carry):
            for q in pieces:
                carry = tuple(
                    carry[x]
                    + arch[q * piece + i, x].astype(F32) * t_ref[q, pl.ds(x * piece + i, 1), :]
                    for x in range(2)
                )
            return carry

        return lax.fori_loop(0, piece, one, carry, unroll=8)

    def spread(phase, grid, before_last, half_in, near_end):
        for q in range(CHUNKS):
            form_sources(phase, q, grid)
            if phase == 0:
                send_strips(phase, SOURCE, q, s_ref[q])
            send_block(phase, SOURCE, q, s_ref[q])
            if phase == 1:
                send_strips(phase, SOURCE, q, s_ref[q])

        def filter_own(*pieces):
            for q in pieces:
                wait_for(strip_in.at[phase, SOURCE, q], strip_recv.at[phase, q])
                h_ref[phase, q] = filter_cols(phase, SOURCE, q, s_ref[q])
                send_block(phase, FILTERED, q, h_ref[phase, q])
                remote(
                    out_ref.at[phase, FILTERED, q],
                    beside_in.at[phase, q],
                    block_send.at[phase],
                    beside_recv.at[phase, q // 2],
                    beside_me,
                )

        def filter_one_side(pair):
            passed_in(phase, SOURCE, pair)
            for q in (2 * pair, 2 * pair + 1):
                f_ref[q] = from_side(phase, SOURCE, q)
                send_strips(phase, FILTERED, q, f_ref[q])

        def finish(pair, carry):
            pieces = (2 * pair, 2 * pair + 1)
            both = strip_in.at[phase, FILTERED, pieces[0] : pieces[1] + 1]
            wait_for(both, strip_recv.at[phase, CHUNKS + pair])
            for q in pieces:
                t_ref[q] = filter_cols(phase, FILTERED, q, f_ref[q])
            passed_in(phase, FILTERED, pair)
            for q in pieces:
                rest = from_side(
                    phase,
                    FILTERED,
                    q,
                    (
                        ((0, 0), halves(h_ref[phase, q])),
                        ((1, -1), [beside_in[phase, q, r].astype(F32) for r in range(2)]),
                    ),
                )
                t_ref[q] = t_ref[q] + rest
            return member_sum(pieces, carry)

        last = PAIRS - 1
        filter_own(0, 1)
        if phase == 0:
            for pair in range(last):
                pass_on(phase, SOURCE, pair)
                filter_own(2 * pair + 2)
                filter_one_side(pair)
                filter_own(2 * pair + 3)
        else:
            filter_own(*range(2, CHUNKS))
            for pair in range(last):
                pass_on(phase, SOURCE, pair)
        come_beside(phase)
        before_last()
        pass_on(phase, SOURCE, last)
        half_in()
        if phase == 1:
            for pair in range(last):
                filter_one_side(pair)
        filter_one_side(last)

        carry = tuple(jnp.zeros((levels, cols), F32) for _ in range(2))
        if phase == 0:
            for pair in range(PAIRS):
                pass_on(phase, FILTERED, pair)
                carry = finish(pair, carry)
        else:
            for pair in range(PAIRS):
                pass_on(phase, FILTERED, pair)
            for pair in range(PAIRS):
                if pair == PAIRS // 2:
                    near_end()
                carry = finish(pair, carry)
        for x in range(2):
            for h in range(2):
                pmine[phase, h, x] = carry[x][h * half : (h + 1) * half]
        return jnp.concatenate(carry, axis=0)

    def dotted(phase, factor, pieces):
        total = None
        for q in pieces:
            way = course(SOURCE, q)
            here = side_in.at[phase, SOURCE, q]
            own = halves(s_ref[q])
            near = [here[r].astype(F32) * 2.0 for r in range(2)]
            far = [jnp.where(big(way), here[2 + r].astype(F32) * 2.0, 0.0) for r in range(2)]
            mine = weighed([((0, 0), own), ((-2 * way,) * 2, near)])
            value, i = far_row(phase, SOURCE, q)
            mine[i] = mine[i] + value * 2.0
            theirs = weighed(
                [
                    ((-1, 1), own),
                    ((-2 * way - 1, -2 * way + 1), near),
                    ((-3 * way,) * 2, far),
                ]
            )
            field = halves(h_ref[phase, q])
            for i in range(2):
                beside = beside_in[phase, q, i].astype(F32)
                if factor is None:
                    term = mine[i] * field[i] + theirs[i] * beside
                else:
                    term = (mine[i] * factor) * (field[i] * factor) + (theirs[i] * factor) * (
                        beside * factor
                    )
                total = term if total is None else total + term
        return jnp.sum(total, axis=0, keepdims=True)

    def send_increment(phase):
        return remote(
            pmine.at[phase, other], ptheirs.at[phase], p_sem.at[2], p_sem.at[phase], partner
        )

    def folded(vector):
        return (
            sum(vector[:, k * cols : (k + 1) * cols] for k in range(n_obs // cols)) * 0.5
        )

    n_z = n_gx // 2
    hub = core == 1

    def reduce_first(which, rows):
        red1[which, gx, 0:1, :] = rows[0]
        red1[which, gx, 1:2, :] = rows[1]
        mine = red1.at[which, gx]
        sems = red_send.at[which, 0], red_recv.at[which, 0]
        for k in range(1, n_z):
            remote(mine, mine, *sems, {"gx": 2 * lax.rem(gx // 2 + k, n_z) + 1})

        @pl.when(jnp.logical_not(hub))
        def _():
            remote(mine, mine, *sems, {"gx": gx + 1})

    def reduce_second(which):
        @pl.when(hub)
        def _():
            wait_for(red1.at[which, 0 : n_gx - 1], red_recv.at[which, 0])
            red2[which, plane] = jnp.sum(red1[which], axis=0)
            mine = red2.at[which, plane]
            sems = red_send.at[which, 1], red_recv.at[which, 1]
            for k in range(1, n_plane):
                remote(mine, mine, *sems, {**plane_device(k), "gx": gx - 1})
            for k in range(1, n_plane):
                remote(mine, mine, *sems, plane_device(k))
            remote(mine, mine, *sems, {"gx": gx - 1})

    def reduce_last(which):
        @pl.when(hub)
        def _():
            wait_for(red2.at[which, 0 : n_plane - 1], red_recv.at[which, 1])

        @pl.when(jnp.logical_not(hub))
        def _():
            wait_for(red2.at[which, 0:n_plane], red_recv.at[which, 1])

        both = jnp.sum(jnp.sum(red2[which], axis=0), axis=1, keepdims=True)
        return both[0:1], both[1:2]

    def reduce_sent(which):
        @pl.when(hub)
        def _():
            wait_for(count_ref.at[0 : n_z - 1], red_send.at[which, 0])
            wait_for(count_ref.at[0 : 2 * n_plane - 1], red_send.at[which, 1])

        @pl.when(jnp.logical_not(hub))
        def _():
            wait_for(count_ref.at[0:n_z], red_send.at[which, 0])

    state = {}

    def first_half_in():
        innovation = target_value - gather(average[...])
        product = folded(noise * innovation * innovation) + dotted(0, None, range(CHUNKS))
        reduce_first(0, (folded(innovation * innovation), product))
        state["innovation"] = innovation

    grid_b = spread(
        0, values - counts * average[...], lambda: None, first_half_in, lambda: None
    )
    innovation = state["innovation"]
    gsum[ma] = gather(grid_b)
    g_copy = remote(gsum.at[ma], gsum.at[ma], g_sem.at[0], g_sem.at[1], partner)
    send_increment(0)
    g_copy.wait()
    reduce_second(0)
    image = gsum[0] + gsum[1] + noise * innovation

    def before_last():
        norm_now, product = reduce_last(0)
        alpha = norm_now / product
        scaled = alpha * image
        residual = innovation - scaled
        change = folded(scaled * (noise * scaled - 2.0 * image)) + dotted(1, alpha, range(CHUNKS - 2))
        state["step"] = norm_now, product, alpha, residual
        state["sums"] = folded(residual * residual), change

    def half_in():
        norm, change = state["sums"]
        reduce_first(1, (norm, change + dotted(1, state["step"][2], range(CHUNKS - 2, CHUNKS))))

    spread(1, scatter(image), before_last, half_in, lambda: reduce_second(1))
    send_increment(1)
    for phase in range(2):
        wait_for(sent_rows, block_send.at[phase])
        wait_for(strip_in.at[phase], strip_send.at[phase])
    reduce_sent(0)
    wait_for(ptheirs.at[0], p_sem.at[0])

    norm_now, product, alpha, residual = state["step"]
    norm_next, change = reduce_last(1)
    product = product + change
    ratio = norm_next / norm_now
    alpha_next = norm_next / (product - ratio * norm_next / alpha)
    weights = alpha * innovation + alpha_next * (residual + ratio * innovation)
    chosen = jnp.where(ma == 0, weights[:, : n_obs // 2], weights[:, n_obs // 2 :])
    w_ref[0:1, :] = chosen[:, :cols]
    w_ref[1:2, :] = chosen[:, cols:]

    wait_for(ptheirs.at[1], p_sem.at[1])
    first_weight = (alpha + alpha_next * (1.0 + ratio))[None]
    second_weight = (alpha * alpha_next)[None]
    inc_ref[...] = first_weight * (pmine[0, ma] + ptheirs[0]) - second_weight * (
        pmine[1, ma] + ptheirs[1]
    )

    wait_for(ptheirs, p_sem.at[2])
    reduce_sent(1)


def shards(n_gx, n_gy, archive, obs_index, obs_value, obs_error):
    members, rows, levels, cols = archive.shape
    half = levels // 2
    n_own = obs_index.shape[0]
    piece = members // CHUNKS
    strip_rows = rows * piece * STRIP // cols
    shape = (n_own // cols, cols)
    dma = pltpu.SemaphoreType.DMA
    vmem = pl.BlockSpec(memory_space=pltpu.VMEM)
    hbm = pl.BlockSpec(memory_space=pltpu.HBM)
    increment, weights = pl.pallas_call(
        functools.partial(kernel, n_gx, n_gy),
        out_shape=(
            pltpu.VMEM((rows, half, cols), F32),
            pltpu.VMEM(shape, F32),
        ),
        in_specs=[hbm, hbm, hbm, hbm],
        out_specs=(vmem, vmem),
        scratch_shapes=[
            pltpu.VMEM((members, rows, levels, cols), BF16),
            pltpu.VMEM(shape, jnp.int32),
            pltpu.VMEM((2, *shape), F32),
            pltpu.VMEM((2, 8, cols), F32),
            pltpu.VMEM((2, rows * levels, cols), F32),
            pltpu.VMEM((rows * levels, cols), F32),
            pltpu.VMEM((rows, piece * 8, cols), F32),
            pltpu.VMEM((CHUNKS, rows * piece, cols), F32),
            pltpu.VMEM((CHUNKS, rows * piece, cols), F32),
            pltpu.VMEM((2, CHUNKS, rows * piece, cols), F32),
            pltpu.VMEM((CHUNKS, rows * piece, cols), F32),
            pltpu.VMEM((2, 2, CHUNKS, rows, piece, cols), BF16),
            pltpu.VMEM((2, 2, CHUNKS, 8, piece, cols), BF16),
            pltpu.VMEM((2, CHUNKS, rows, piece, cols), BF16),
            pltpu.VMEM((15 * CHUNKS, piece, cols), BF16),
            pltpu.VMEM((2, 2, CHUNKS, 2, strip_rows, cols), BF16),
            pltpu.VMEM((2, 2, CHUNKS, 2, strip_rows, cols), BF16),
            pltpu.VMEM((5 * cols, cols), BF16),
            pltpu.VMEM((2, 2, rows, half, cols), F32),
            pltpu.VMEM((2, rows, half, cols), F32),
            pltpu.VMEM((2, 1, 2 * n_own), F32),
            pltpu.VMEM((2, n_gx, 2, cols), F32),
            pltpu.VMEM((2, 2 * n_gy, 2, cols), F32),
            pltpu.VMEM((4 * n_gy, 2, cols), F32),
            dma((LOADS + 2,)),
            dma((2,)),
            dma((2,)),
            dma((2,)),
            dma((2, 2, PAIRS)),
            dma((2, 2, PAIRS)),
            dma((2, PAIRS)),
            dma((2,)),
            dma((2, CHUNKS + PAIRS)),
            dma((3,)),
            dma((2,)),
            dma((2, 2)),
            dma((2, 2)),
        ],
        compiler_params=pltpu.CompilerParams(
            collective_id=0, has_side_effects=True, vmem_limit_bytes=56 * 1024 * 1024
        ),
        name="analysis",
    )(archive, obs_index.reshape(shape), obs_value.reshape(shape), obs_error.reshape(shape))
    return increment, weights.reshape(n_own)


def solution(mesh):
    n_gx, n_gy = mesh.shape["gx"], mesh.shape["gy"]
    own = P(("gx", "gy", "ma"))
    return jax.shard_map(
        functools.partial(shards, n_gx, n_gy),
        mesh=mesh,
        in_specs=(P("ma", "gx", None, "gy"), own, own, own),
        out_specs=(P("gx", "ma", "gy"), own),
        check_vma=False,
    )
```

```python
import functools
import math

import jax
import jax.numpy as jnp
from jax import lax
from jax.experimental import pallas as pl
from jax.experimental.pallas import tpu as pltpu
from jax.sharding import PartitionSpec as P

M = 512
TAPER_X = 4
TAPER_Y = 8
F32 = jnp.float32
BF16 = jnp.bfloat16
MESH = pl.DeviceIdType.MESH

LOADS = 8
CHUNKS = 4
PAIRS = CHUNKS // 2
STRIP = 16
SOURCE, FILTERED = 0, 1


def course(kind, q):
    return (1 if q % 2 == 0 else -1) * (1 if kind == SOURCE else -1)


def row_weight(distance):
    r = abs(distance) / TAPER_X
    if r <= 1.0:
        return (((-0.25 * r + 0.5) * r + 0.625) * r - 5.0 / 3.0) * r * r + 1.0
    if r < 2.0:
        return (
            ((((r / 12.0 - 0.5) * r + 0.625) * r + 5.0 / 3.0) * r - 5.0) * r
            + 4.0
            - 2.0 / (3.0 * r)
        )
    return 0.0


def taper_weight(distance, half_width):
    ratio = jnp.abs(distance) / half_width
    safe = jnp.maximum(ratio, 1.0)
    inner = (((-0.25 * ratio + 0.5) * ratio + 0.625) * ratio - 5.0 / 3.0) * ratio * ratio + 1.0
    outer = (
        ((((ratio / 12.0 - 0.5) * ratio + 0.625) * ratio + 5.0 / 3.0) * ratio - 5.0) * ratio
        + 4.0
        - 2.0 / (3.0 * safe)
    )
    return jnp.where(ratio <= 1.0, inner, jnp.where(ratio < 2.0, outer, 0.0))


def in_three(x):
    first = x.astype(BF16)
    rest = x - first.astype(F32)
    second = rest.astype(BF16)
    third = (rest - second.astype(F32)).astype(BF16)
    return jnp.concatenate([first, second, third], axis=0)


def sum_of_three(y, rows):
    return (y[2 * rows :] + y[rows : 2 * rows]) + y[:rows]


def kernel(
    n_gx,
    n_gy,
    archive_hbm,
    idx_hbm,
    val_hbm,
    err_hbm,
    inc_ref,
    w_ref,
    arch,
    idx_ref,
    pair_ref,
    meta,
    sums,
    average,
    part,
    s_ref,
    f_ref,
    h_ref,
    t_ref,
    out_ref,
    side_in,
    beside_in,
    count_rows,
    strip_out,
    strip_in,
    wcol,
    pmine,
    ptheirs,
    gsum,
    red1,
    red2,
    count_ref,
    load_sem,
    meta_sem,
    sums_sem,
    block_send,
    block_recv,
    fwd_recv,
    beside_recv,
    strip_send,
    strip_recv,
    p_sem,
    g_sem,
    red_send,
    red_recv,
):
    members = arch.shape[0]
    levels = arch.shape[2]
    half = levels // 2
    cols = arch.shape[3]
    piece = members // CHUNKS
    gx = lax.axis_index("gx")
    gy = lax.axis_index("gy")
    ma = lax.axis_index("ma")
    core = lax.rem(gx, 2)
    other = 1 - ma
    sent_rows = count_rows.at[0 : 15 * CHUNKS]
    plane = gy * 2 + ma
    n_plane = n_gy * 2

    def row_block(k):
        return {"gx": lax.rem(gx + (k + n_gx), n_gx)}

    def col_block(k):
        return {"gy": lax.rem(gy + (k + n_gy), n_gy)}

    def plane_device(k):
        at = lax.rem(plane + k, n_plane)
        return {"gy": at // 2, "ma": lax.rem(at, 2)}

    def remote(src, dst, send_sem, recv_sem, device):
        copy = pltpu.make_async_remote_copy(
            src_ref=src,
            dst_ref=dst,
            send_sem=send_sem,
            recv_sem=recv_sem,
            device_id=device,
            device_id_type=MESH,
        )
        copy.start()
        return copy

    def wait_for(ref, sem):
        pltpu.make_async_copy(ref, ref, sem).wait()

    load = members // LOADS
    loads = []
    for k in range(LOADS):
        copy = pltpu.make_async_copy(
            archive_hbm.at[pl.ds(k * load, load)], arch.at[pl.ds(k * load, load)], load_sem.at[k]
        )
        copy.start()
        loads.append(copy)
    pltpu.make_async_copy(idx_hbm, idx_ref, load_sem.at[LOADS]).start()
    pltpu.make_async_copy(val_hbm, pair_ref.at[0], load_sem.at[LOADS + 1]).start()
    pltpu.make_async_copy(err_hbm, pair_ref.at[1], load_sem.at[LOADS + 1]).start()

    barrier = pltpu.get_barrier_semaphore()
    def far_first(count):
        return sorted(range(1, count), key=lambda k: -min(k, count - k))

    greeted = [row_block(k) for k in far_first(n_gx) if min(k, n_gx - k) <= 4]
    for k in far_first(n_plane):
        greeted += [plane_device(k), {**plane_device(k), **row_block(1 - 2 * core)}]
    for device in greeted:
        pl.semaphore_signal(barrier, inc=1, device_id=device, device_id_type=MESH)

    total = tuple(jnp.zeros((levels, cols), F32) for _ in range(2))
    for k in range(LOADS):
        loads[k].wait()

        def add(m, carry):
            return tuple(carry[x] + arch[m, x].astype(F32) for x in range(2))

        total = lax.fori_loop(k * load, (k + 1) * load, add, total, unroll=8)
    for x in range(2):
        sums[ma, x * levels : (x + 1) * levels, :] = total[x]
    wait_for(idx_ref, load_sem.at[LOADS])
    wait_for(pair_ref, load_sem.at[LOADS + 1])
    meta[ma, 0:2, :] = idx_ref[...].astype(F32)
    meta[ma, 2:4, :] = pair_ref[0]
    meta[ma, 4:6, :] = pair_ref[1]
    meta[ma, 6:8, :] = jnp.zeros((2, cols), F32)

    pl.semaphore_wait(barrier, len(greeted))

    partner = {"ma": other}
    meta_copy = remote(meta.at[ma], meta.at[ma], meta_sem.at[0], meta_sem.at[1], partner)
    sums_copy = remote(sums.at[ma], sums.at[ma], sums_sem.at[0], sums_sem.at[1], partner)

    source = lax.broadcasted_iota(jnp.int32, (cols, cols), 0)
    target = lax.broadcasted_iota(jnp.int32, (cols, cols), 1)

    def col_weight(shift):
        return taper_weight((source - target + shift).astype(F32), float(TAPER_Y))

    beside = jnp.where(gy > 0, col_weight(-cols), 0.0) + jnp.where(
        gy < n_gy - 1, col_weight(cols), 0.0
    )
    for k, weight in enumerate((col_weight(0), beside)):
        high = weight.astype(BF16)
        low = (weight - high.astype(F32)).astype(BF16)
        wcol[2 * k * cols : (2 * k + 1) * cols, :] = high
        wcol[(2 * k + 1) * cols : (2 * k + 2) * cols, :] = low
        if k == 0:
            wcol[4 * cols : 5 * cols, :] = high

    meta_copy.wait()

    def in_a_row(first):
        rows = [meta[h, first + i : first + i + 1, :] for h in range(2) for i in range(2)]
        return jnp.concatenate(rows, axis=1)

    index = in_a_row(0).astype(jnp.int32)
    target_value = in_a_row(2)
    noise = in_a_row(4)
    n_obs = index.shape[1]
    owner = lax.broadcasted_iota(jnp.int32, (1, n_obs), 1) // (n_obs // 2)
    obs_line = (index >> 11) * levels + owner * half + ((index >> 7) & (half - 1))
    obs_col = index & (cols - 1)
    line_hot = (
        lax.broadcasted_iota(jnp.int32, (2 * levels, n_obs), 0) == obs_line
    ).astype(F32)
    col_hot = (
        (lax.broadcasted_iota(jnp.int32, (cols, n_obs), 0) == obs_col).astype(F32).astype(BF16)
    )

    def gather(grid):
        rows = 2 * levels
        spread = jnp.dot(in_three(grid), col_hot, preferred_element_type=F32)
        return jnp.sum(sum_of_three(spread, rows) * line_hot, axis=0, keepdims=True)

    def scatter(vector):
        rows = 2 * levels
        spread = lax.dot_general(
            in_three(line_hot * vector),
            col_hot,
            (((1,), (1,)), ((), ())),
            preferred_element_type=F32,
        )
        return sum_of_three(spread, rows)

    values = scatter(target_value)
    counts = lax.dot_general(
        line_hot.astype(BF16), col_hot, (((1,), (1,)), ((), ())), preferred_element_type=F32
    )
    sums_copy.wait()
    average[...] = (sums[0] + sums[1]) * (1.0 / M)
    scale = 1.0 / math.sqrt(M - 1.0)

    beside_me = row_block(1 - 2 * core)

    def big(way):
        return core == (1 if way > 0 else 0)

    def send_block(phase, kind, q, field):
        way = course(kind, q)
        row = 1 if way > 0 else 0
        for x in range(2):
            out_ref[phase, kind, q, x] = field[x * piece : (x + 1) * piece].astype(BF16)
        block = out_ref.at[phase, kind, q]
        here = side_in.at[phase, kind, q]
        sems = block_send.at[phase], block_recv.at[phase, kind, q // 2]

        @pl.when(big(way))
        def _():
            remote(block, here.at[2:4], *sems, row_block(4 * way))

        @pl.when(jnp.logical_not(big(way)))
        def _():
            remote(block.at[row], here.at[2], *sems, row_block(4 * way))

        remote(block, here.at[0:2], *sems, row_block(2 * way))

    def pass_on(phase, kind, pair):
        wait_for(count_rows.at[0:7], block_recv.at[phase, kind, pair])
        sems = block_send.at[phase], fwd_recv.at[phase, kind, pair]
        for q in (2 * pair, 2 * pair + 1):
            way = course(kind, q)
            here = side_in.at[phase, kind, q]

            @pl.when(big(way))
            def _(here=here):
                remote(here.at[0:4], here.at[4:8], *sems, beside_me)

            @pl.when(jnp.logical_not(big(way)))
            def _(here=here):
                remote(here.at[0:2], here.at[4:6], *sems, beside_me)

    def passed_in(phase, kind, pair):
        wait_for(count_rows.at[0:6], fwd_recv.at[phase, kind, pair])

    def come_beside(phase):
        for pair in range(PAIRS):
            both = beside_in.at[phase, 2 * pair : 2 * pair + 2]
            wait_for(both, beside_recv.at[phase, pair])

    def weight(k, r, i):
        both = [row_weight(2 * at + r - i) for at in k]
        return both[0] if both[0] == both[1] else jnp.where(core == 0, both[0], both[1])

    def weighed(terms):
        outs = [None, None]
        for k, rows in terms:
            for r in range(2):
                for i in range(2):
                    if any(row_weight(2 * at + r - i) for at in k):
                        term = rows[r] * weight(k, r, i)
                        outs[i] = term if outs[i] is None else outs[i] + term
        return outs

    def halves(field):
        return [field[:piece], field[piece:]]

    def far_row(phase, kind, q):
        way = course(kind, q)
        at = 2 + jnp.where(big(way), 1 if way > 0 else 0, 0)
        value = side_in[phase, kind, q, at].astype(F32) * row_weight(7)
        return value, 0 if way > 0 else 1

    def from_side(phase, kind, q, extra=()):
        way = course(kind, q)
        here = side_in.at[phase, kind, q]
        rows = [here[k].astype(F32) for k in (0, 1, 4, 5)]
        rows += [jnp.where(big(way), 0.0, here[k].astype(F32)) for k in (6, 7)]
        outs = weighed(
            [
                ((-2 * way,) * 2, rows[0:2]),
                ((1 - 2 * way, -1 - 2 * way), rows[2:4]),
                ((-3 * way,) * 2, rows[4:6]),
                *extra,
            ]
        )
        value, i = far_row(phase, kind, q)
        outs[i] = outs[i] + value
        return jnp.concatenate(outs, axis=0)

    strip_rows = 2 * piece * STRIP // cols
    lane = lax.broadcasted_iota(jnp.int32, (strip_rows, cols), 1)

    def send_strips(phase, kind, q, field):
        last = first = jnp.zeros((strip_rows, cols), F32)
        for j in range(cols // STRIP):
            group = field[j * strip_rows : (j + 1) * strip_rows]
            mine = lane // STRIP == j
            last = jnp.where(mine, pltpu.roll(group, ((j + 1) * STRIP) % cols, 1), last)
            first = jnp.where(mine, pltpu.roll(group, j * STRIP, 1), first)
        for side, strip in enumerate((last, first)):
            strip_out[phase, kind, q, side] = strip.astype(BF16)
            remote(
                strip_out.at[phase, kind, q, side],
                strip_in.at[phase, kind, q, side],
                strip_send.at[phase],
                strip_recv.at[phase, q if kind == SOURCE else CHUNKS + q // 2],
                col_block(1 - 2 * side),
            )

    def filter_cols(phase, kind, q, field):
        left = strip_in[phase, kind, q, 0].astype(F32)
        right = strip_in[phase, kind, q, 1].astype(F32)
        strips = []
        for j in range(cols // STRIP):
            strips.append(
                jnp.where(
                    lane < cols // 2,
                    pltpu.roll(right, (cols - j * STRIP) % cols, 1),
                    pltpu.roll(left, cols - (j + 1) * STRIP, 1),
                )
            )
        strips = jnp.concatenate(strips, axis=0).astype(BF16)
        high = field.astype(BF16)
        low = (field - high.astype(F32)).astype(BF16)
        return jnp.dot(
            jnp.concatenate([high, high, strips, strips, low], axis=1),
            wcol[...],
            preferred_element_type=F32,
        )

    def form_sources(phase, q, grid):
        value = [grid[x * levels : (x + 1) * levels] for x in range(2)]

        def one(i, carry):
            m = q * piece + i
            for x in range(2):
                if phase == 0:
                    anomaly = ((arch[m, x].astype(F32) - average[x * levels : (x + 1) * levels, :]) * scale).astype(BF16)
                    arch[m, x] = anomaly
                else:
                    anomaly = arch[m, x]
                product = anomaly.astype(F32) * value[x]
                part[x, pl.ds(pl.multiple_of(i * 8, 8), 8), :] = (
                    product[0:8] + product[8:16]
                ) + (product[16:24] + product[24:32])
            return carry

        lax.fori_loop(0, piece, one, 0, unroll=8)
        for x in range(2):
            for g in range(piece // 8):
                rows = [part[x, pl.ds(g * 64 + k, 8, stride=8), :] for k in range(8)]
                s_ref[q, x * piece + g * 8 : x * piece + g * 8 + 8, :] = (
                    (rows[0] + rows[1]) + (rows[2] + rows[3])
                ) + ((rows[4] + rows[5]) + (rows[6] + rows[7]))

    def member_sum(pieces, carry):
        def one(i, carry):
            for q in pieces:
                carry = tuple(
                    carry[x]
                    + arch[q * piece + i, x].astype(F32) * t_ref[q, pl.ds(x * piece + i, 1), :]
                    for x in range(2)
                )
            return carry

        return lax.fori_loop(0, piece, one, carry, unroll=8)

    def spread(phase, grid, before_last, half_in, near_end):
        for q in range(CHUNKS):
            form_sources(phase, q, grid)
            if phase == 0:
                send_strips(phase, SOURCE, q, s_ref[q])
            send_block(phase, SOURCE, q, s_ref[q])
            if phase == 1:
                send_strips(phase, SOURCE, q, s_ref[q])

        def filter_own(*pieces):
            for q in pieces:
                wait_for(strip_in.at[phase, SOURCE, q], strip_recv.at[phase, q])
                h_ref[phase, q] = filter_cols(phase, SOURCE, q, s_ref[q])
                send_block(phase, FILTERED, q, h_ref[phase, q])
                remote(
                    out_ref.at[phase, FILTERED, q],
                    beside_in.at[phase, q],
                    block_send.at[phase],
                    beside_recv.at[phase, q // 2],
                    beside_me,
                )

        def filter_one_side(pair):
            passed_in(phase, SOURCE, pair)
            for q in (2 * pair, 2 * pair + 1):
                f_ref[q] = from_side(phase, SOURCE, q)
                send_strips(phase, FILTERED, q, f_ref[q])

        def finish(pair, carry):
            pieces = (2 * pair, 2 * pair + 1)
            both = strip_in.at[phase, FILTERED, pieces[0] : pieces[1] + 1]
            wait_for(both, strip_recv.at[phase, CHUNKS + pair])
            for q in pieces:
                t_ref[q] = filter_cols(phase, FILTERED, q, f_ref[q])
            passed_in(phase, FILTERED, pair)
            for q in pieces:
                rest = from_side(
                    phase,
                    FILTERED,
                    q,
                    (
                        ((0, 0), halves(h_ref[phase, q])),
                        ((1, -1), [beside_in[phase, q, r].astype(F32) for r in range(2)]),
                    ),
                )
                t_ref[q] = t_ref[q] + rest
            return member_sum(pieces, carry)

        last = PAIRS - 1
        filter_own(0, 1)
        if phase == 0:
            for pair in range(last):
                pass_on(phase, SOURCE, pair)
                filter_own(2 * pair + 2)
                filter_one_side(pair)
                filter_own(2 * pair + 3)
        else:
            filter_own(*range(2, CHUNKS))
            for pair in range(last):
                pass_on(phase, SOURCE, pair)
        come_beside(phase)
        before_last()
        pass_on(phase, SOURCE, last)
        half_in()
        if phase == 1:
            for pair in range(last):
                filter_one_side(pair)
        filter_one_side(last)

        carry = tuple(jnp.zeros((levels, cols), F32) for _ in range(2))
        if phase == 0:
            for pair in range(PAIRS):
                pass_on(phase, FILTERED, pair)
                if pair == last:
                    near_end()
                carry = finish(pair, carry)
        else:
            for pair in range(PAIRS):
                pass_on(phase, FILTERED, pair)
            for pair in range(PAIRS):
                if pair == PAIRS // 2:
                    near_end()
                carry = finish(pair, carry)
        for x in range(2):
            for h in range(2):
                pmine[phase, h, x] = carry[x][h * half : (h + 1) * half]
        return jnp.concatenate(carry, axis=0)

    def dotted(phase, pieces):
        total = None
        for q in pieces:
            way = course(SOURCE, q)
            here = side_in.at[phase, SOURCE, q]
            own = halves(s_ref[q])
            near = [here[r].astype(F32) * 2.0 for r in range(2)]
            far = [jnp.where(big(way), here[2 + r].astype(F32) * 2.0, 0.0) for r in range(2)]
            mine = weighed([((0, 0), own), ((-2 * way,) * 2, near)])
            value, i = far_row(phase, SOURCE, q)
            mine[i] = mine[i] + value * 2.0
            theirs = weighed(
                [
                    ((-1, 1), own),
                    ((-2 * way - 1, -2 * way + 1), near),
                    ((-3 * way,) * 2, far),
                ]
            )
            field = halves(h_ref[phase, q])
            for i in range(2):
                beside = beside_in[phase, q, i].astype(F32)
                term = mine[i] * field[i] + theirs[i] * beside
                total = term if total is None else total + term
        return jnp.sum(total, axis=0, keepdims=True)

    def send_increment(phase):
        return remote(
            pmine.at[phase, other], ptheirs.at[phase], p_sem.at[2], p_sem.at[phase], partner
        )

    def folded(vector):
        return (
            sum(vector[:, k * cols : (k + 1) * cols] for k in range(n_obs // cols)) * 0.5
        )

    n_z = n_gx // 2
    hub = core == 1

    def reduce_first(which, rows):
        red1[which, gx, 0:1, :] = rows[0]
        red1[which, gx, 1:2, :] = rows[1]
        mine = red1.at[which, gx]
        sems = red_send.at[which, 0], red_recv.at[which, 0]
        for k in range(1, n_z):
            remote(mine, mine, *sems, {"gx": 2 * lax.rem(gx // 2 + k, n_z) + 1})

        @pl.when(jnp.logical_not(hub))
        def _():
            remote(mine, mine, *sems, {"gx": gx + 1})

    def reduce_second(which):
        @pl.when(hub)
        def _():
            wait_for(red1.at[which, 0 : n_gx - 1], red_recv.at[which, 0])
            red2[which, plane] = jnp.sum(red1[which], axis=0)
            mine = red2.at[which, plane]
            sems = red_send.at[which, 1], red_recv.at[which, 1]
            for k in range(1, n_plane):
                remote(mine, mine, *sems, {**plane_device(k), "gx": gx - 1})
            for k in range(1, n_plane):
                remote(mine, mine, *sems, plane_device(k))
            remote(mine, mine, *sems, {"gx": gx - 1})

    def reduce_last(which):
        @pl.when(hub)
        def _():
            wait_for(red2.at[which, 0 : n_plane - 1], red_recv.at[which, 1])

        @pl.when(jnp.logical_not(hub))
        def _():
            wait_for(red2.at[which, 0:n_plane], red_recv.at[which, 1])

        both = jnp.sum(jnp.sum(red2[which], axis=0), axis=1, keepdims=True)
        return both[0:1], both[1:2]

    def reduce_sent(which):
        @pl.when(hub)
        def _():
            wait_for(count_ref.at[0 : n_z - 1], red_send.at[which, 0])
            wait_for(count_ref.at[0 : 2 * n_plane - 1], red_send.at[which, 1])

        @pl.when(jnp.logical_not(hub))
        def _():
            wait_for(count_ref.at[0:n_z], red_send.at[which, 0])

    state = {}

    def first_half_in():
        innovation = target_value - gather(average[...])
        product = folded(noise * innovation * innovation) + dotted(0, range(CHUNKS))
        reduce_first(0, (folded(innovation * innovation), product))
        state["innovation"] = innovation

    grid_b = spread(
        0, values - counts * average[...], lambda: None, first_half_in, lambda: reduce_second(0)
    )
    innovation = state["innovation"]
    gsum[ma] = gather(grid_b)
    g_copy = remote(gsum.at[ma], gsum.at[ma], g_sem.at[0], g_sem.at[1], partner)
    send_increment(0)
    g_copy.wait()
    image = gsum[0] + gsum[1] + noise * innovation
    norm_now, product = reduce_last(0)
    alpha = norm_now / product
    residual = innovation - alpha * image

    def before_last():
        product = folded(noise * residual * residual) + dotted(1, range(CHUNKS - 2))
        state["sums"] = folded(residual * residual), product

    def half_in():
        norm, product = state["sums"]
        reduce_first(1, (norm, product + dotted(1, range(CHUNKS - 2, CHUNKS))))

    spread(1, scatter(residual), before_last, half_in, lambda: reduce_second(1))
    send_increment(1)
    for phase in range(2):
        wait_for(sent_rows, block_send.at[phase])
        wait_for(strip_in.at[phase], strip_send.at[phase])
    reduce_sent(0)
    wait_for(ptheirs.at[0], p_sem.at[0])

    norm_next, product = reduce_last(1)
    ratio = norm_next / norm_now
    alpha_next = norm_next / (product - ratio * norm_next / alpha)
    weights = alpha * innovation + alpha_next * (residual + ratio * innovation)
    chosen = jnp.where(ma == 0, weights[:, : n_obs // 2], weights[:, n_obs // 2 :])
    w_ref[0:1, :] = chosen[:, :cols]
    w_ref[1:2, :] = chosen[:, cols:]

    wait_for(ptheirs.at[1], p_sem.at[1])
    first_weight = (alpha + alpha_next * ratio)[None]
    second_weight = alpha_next[None]
    inc_ref[...] = first_weight * (pmine[0, ma] + ptheirs[0]) + second_weight * (
        pmine[1, ma] + ptheirs[1]
    )

    wait_for(ptheirs, p_sem.at[2])
    reduce_sent(1)


def shards(n_gx, n_gy, archive, obs_index, obs_value, obs_error):
    members, rows, levels, cols = archive.shape
    half = levels // 2
    n_own = obs_index.shape[0]
    piece = members // CHUNKS
    strip_rows = rows * piece * STRIP // cols
    shape = (n_own // cols, cols)
    dma = pltpu.SemaphoreType.DMA
    vmem = pl.BlockSpec(memory_space=pltpu.VMEM)
    hbm = pl.BlockSpec(memory_space=pltpu.HBM)
    increment, weights = pl.pallas_call(
        functools.partial(kernel, n_gx, n_gy),
        out_shape=(
            pltpu.VMEM((rows, half, cols), F32),
            pltpu.VMEM(shape, F32),
        ),
        in_specs=[hbm, hbm, hbm, hbm],
        out_specs=(vmem, vmem),
        scratch_shapes=[
            pltpu.VMEM((members, rows, levels, cols), BF16),
            pltpu.VMEM(shape, jnp.int32),
            pltpu.VMEM((2, *shape), F32),
            pltpu.VMEM((2, 8, cols), F32),
            pltpu.VMEM((2, rows * levels, cols), F32),
            pltpu.VMEM((rows * levels, cols), F32),
            pltpu.VMEM((rows, piece * 8, cols), F32),
            pltpu.VMEM((CHUNKS, rows * piece, cols), F32),
            pltpu.VMEM((CHUNKS, rows * piece, cols), F32),
            pltpu.VMEM((2, CHUNKS, rows * piece, cols), F32),
            pltpu.VMEM((CHUNKS, rows * piece, cols), F32),
            pltpu.VMEM((2, 2, CHUNKS, rows, piece, cols), BF16),
            pltpu.VMEM((2, 2, CHUNKS, 8, piece, cols), BF16),
            pltpu.VMEM((2, CHUNKS, rows, piece, cols), BF16),
            pltpu.VMEM((15 * CHUNKS, piece, cols), BF16),
            pltpu.VMEM((2, 2, CHUNKS, 2, strip_rows, cols), BF16),
            pltpu.VMEM((2, 2, CHUNKS, 2, strip_rows, cols), BF16),
            pltpu.VMEM((5 * cols, cols), BF16),
            pltpu.VMEM((2, 2, rows, half, cols), F32),
            pltpu.VMEM((2, rows, half, cols), F32),
            pltpu.VMEM((2, 1, 2 * n_own), F32),
            pltpu.VMEM((2, n_gx, 2, cols), F32),
            pltpu.VMEM((2, 2 * n_gy, 2, cols), F32),
            pltpu.VMEM((4 * n_gy, 2, cols), F32),
            dma((LOADS + 2,)),
            dma((2,)),
            dma((2,)),
            dma((2,)),
            dma((2, 2, PAIRS)),
            dma((2, 2, PAIRS)),
            dma((2, PAIRS)),
            dma((2,)),
            dma((2, CHUNKS + PAIRS)),
            dma((3,)),
            dma((2,)),
            dma((2, 2)),
            dma((2, 2)),
        ],
        compiler_params=pltpu.CompilerParams(
            collective_id=0, has_side_effects=True, vmem_limit_bytes=56 * 1024 * 1024
        ),
        name="analysis",
    )(archive, obs_index.reshape(shape), obs_value.reshape(shape), obs_error.reshape(shape))
    return increment, weights.reshape(n_own)


def solution(mesh):
    n_gx, n_gy = mesh.shape["gx"], mesh.shape["gy"]
    own = P(("gx", "gy", "ma"))
    return jax.shard_map(
        functools.partial(shards, n_gx, n_gy),
        mesh=mesh,
        in_specs=(P("ma", "gx", None, "gy"), own, own, own),
        out_specs=(P("gx", "ma", "gy"), own),
        check_vma=False,
    )
```
